32 devices in a mesh: groups: 2 (over y), block: 4 (over z), seg: 2 (over x), sub: 2 (over core).
Axes of the slice: x: 2, y: 2, z: 4, core: 2. Of those that a mesh axis runs over, the one named last changes fastest.
Arguments:
- old_fields: float32 [2048, 4, 512], P(('groups', 'block', 'seg', 'sub')), parts along dimension 0, may hold values from -6 to 6
- corner_shift: float32 [24, 2048], P(None, ('groups', 'block', 'seg', 'sub')), parts along dimension 1, may hold values from -0.2 to 0.2
- targets: float32 [3, 131072], P(None, ('groups', 'block', 'seg', 'sub')), parts along dimension 1, may hold values from -0.7 to 0.7
- owners: int32 [1024], P(('groups', 'block', 'seg', 'sub')), parts along dimension 0, may hold values from 0 to 1023, as said below
Outputs:
- new_fields: float32 [4, 131072], P(None, ('groups', 'block', 'seg', 'sub')), parts along dimension 1
The draws below stay inside these ranges and needn't reach their ends.
There are 2 independent parts, one for each index of `groups`. The reference program is written for one: setup_inputs(seed, part) draws one part's arguments, and reference() takes and returns one part's arrays. A program takes and returns all parts, laid end to end along the dimension named above; each array names one. Nothing has to cross between parts.
Inputs may be any that keep to these rules, and one draw needn't show every extreme that they name: `owners`: owner e lies on device e // 64. At most 2 of the blocks on the rows of one device are owned by elements of any one device, and in every draw some device owns exactly 2 blocks of every device.
All inputs are finite; a program needn't handle non-finite values.
Results may differ from the reference program's by a relative error of at most 0.00029.
Values sent between devices are 32-bit elements; how exact they have to be, the bound alone decides.
A program may use at most 64 MiB of HBM per device.

```python
import jax
import jax.numpy as jnp
import numpy as np
from jax import lax

NVAR = 4
NODES = 512
NEWTON = 3
CAP = 2
BLK_DEV = 32
E_DEV = 64
ELEMS = 1024
POINTS = 65536


def draw_owners(key, part):
    device_count = ELEMS // E_DEV
    subkeys = jax.random.split(jax.random.fold_in(key, 7), 4)
    popular = jax.random.randint(subkeys[0], (), 0, device_count)
    others = jax.vmap(lambda sub_key: jax.random.permutation(sub_key, device_count - 1))(jax.random.split(subkeys[1], device_count))
    shuffle = jax.vmap(lambda sub_key: jax.random.permutation(sub_key, BLK_DEV))(jax.random.split(subkeys[2], device_count))
    position = jnp.arange(BLK_DEV, dtype=jnp.int32)
    spread_pick = others[:, (position - CAP) % (device_count - 1)]
    spread_dev = (popular + 1 + spread_pick) % device_count
    owner_dev = jnp.where(position[None, :] < CAP, popular, spread_dev)
    owner_dev = jnp.take_along_axis(owner_dev, shuffle, axis=1)
    element = jax.random.randint(subkeys[3], (device_count, BLK_DEV), 0, E_DEV)
    return (owner_dev * E_DEV + element).reshape(-1).astype(jnp.int32)


def block_scale(stream_key, dims, shards, low, largest):
    def one(axis_at, parts):
        heights = jax.random.uniform(jax.random.fold_in(jax.random.fold_in(stream_key, 6), axis_at), (parts,), jnp.float32, low / len(shards), largest / len(shards))
        return jnp.repeat(jnp.exp(heights), dims[axis_at] // parts).reshape((-1,) + (1,) * (len(dims) - axis_at - 1))

    factor_of = one(*shards[0])
    for cut in shards[1:]:
        factor_of = factor_of * one(*cut)
    return factor_of


def noise(stream_key, dims, scale, limit, cuts=(), held_as=jnp.bfloat16):
    values = jax.random.normal(stream_key, dims, jnp.float32) * scale
    if len(cuts) > 0:
        values = block_scale(stream_key, dims, cuts, -0.22, 0.18) * values
    return jnp.clip(values, min=-limit, max=limit).astype(held_as)


def setup_inputs(seed: int = 0, part: int = 0) -> dict:
    streams_of = jax.random.split(jax.random.key(seed), 5)
    part_splits = jax.random.split(jax.random.fold_in(streams_of[4], part), 5)
    return {
        "old_fields": noise(part_splits[0], (ELEMS, NVAR, NODES), 1.0, 6.0, ((0, 16),), jnp.float32),
        "corner_shift": jnp.clip(jax.random.uniform(part_splits[1], (24, ELEMS), jnp.float32, -0.2, 0.2) * block_scale(part_splits[1], (24, ELEMS), ((1, 16),), -0.4, 0.0), -0.2, 0.2),
        "targets": jnp.clip(jax.random.uniform(part_splits[2], (3, POINTS), jnp.float32, -0.7, 0.7) * block_scale(part_splits[2], (3, POINTS), ((1, 16),), -0.4, 0.0), -0.7, 0.7),
        "owners": draw_owners(jax.random.fold_in(jax.random.fold_in(streams_of[4], part), 71), part),
    }


GLL_POINTS = (-1.0, -0.8717401485096066, -0.5917001814331423, -0.2092992179024789, 0.2092992179024789, 0.5917001814331423, 0.8717401485096066, 1.0)
EXACT = lax.Precision.HIGHEST


def lagrange_rows(coords):
    gll_nodes = jnp.array(GLL_POINTS, jnp.float32)
    offsets = coords[None, :] - gll_nodes[:, None]
    spacing = gll_nodes[:, None] - gll_nodes[None, :] + jnp.eye(8, dtype=jnp.float32)
    diag_mask = jnp.eye(8, dtype=bool)
    factors = jnp.where(diag_mask[:, :, None], 1.0, offsets[None, :, :] / spacing[:, :, None])
    return jnp.prod(factors, axis=1)


def corner_signs():
    bit_table = np.array([[(corner >> (2 - coord_dim)) & 1 for corner in range(8)] for coord_dim in range(3)], np.float32)
    return jnp.asarray(2.0 * bit_table - 1.0)


def outer_prod(first, second, third):
    return (first[:, None, None, :] * second[None, :, None, :] * third[None, None, :, :]).reshape(8, -1)


def trilinear(ref_pos):
    shape_list = []
    slope_list = []
    for coord_dim in range(3):
        coordinate = ref_pos[coord_dim]
        shape_list.append(jnp.stack([0.5 - 0.5 * coordinate, 0.5 + 0.5 * coordinate]))
        slope_list.append(jnp.stack([jnp.full_like(coordinate, -0.5), jnp.full_like(coordinate, 0.5)]))
    values = outer_prod(shape_list[0], shape_list[1], shape_list[2])
    slopes = [outer_prod(slope_list[0], shape_list[1], shape_list[2]),
              outer_prod(shape_list[0], slope_list[1], shape_list[2]),
              outer_prod(shape_list[0], shape_list[1], slope_list[2])]
    return values, slopes


def solve_three(matrix, rhs_rows):
    cofactors = []
    for row_id in range(3):
        keep_rows = [remain for remain in range(3) if remain != row_id]
        cof_row = []
        for col_id in range(3):
            keep_cols = [remain for remain in range(3) if remain != col_id]
            sign_factor = 1.0 if (row_id + col_id) % 2 == 0 else -1.0
            cof_row.append(sign_factor * (matrix[keep_rows[0]][keep_cols[0]] * matrix[keep_rows[1]][keep_cols[1]]
                                          - matrix[keep_rows[0]][keep_cols[1]] * matrix[keep_rows[1]][keep_cols[0]]))
        cofactors.append(cof_row)
    determinant = matrix[0][0] * cofactors[0][0] + matrix[0][1] * cofactors[0][1] + matrix[0][2] * cofactors[0][2]
    return [(cofactors[0][col_id] * rhs_rows[0] + cofactors[1][col_id] * rhs_rows[1] + cofactors[2][col_id] * rhs_rows[2]) / determinant for col_id in range(3)]


def invert_map(corners, target):
    ref_pos = jnp.zeros_like(target)
    for iteration in range(NEWTON):
        values, slopes = trilinear(ref_pos)
        mapped = jnp.dot(corners, values, precision=EXACT)
        columns = [jnp.dot(corners, slope_row, precision=EXACT) for slope_row in slopes]
        matrix = [[columns[col_id][row_id] for col_id in range(3)] for row_id in range(3)]
        misfit = mapped - target
        update = solve_three(matrix, [misfit[row_id] for row_id in range(3)])
        ref_pos = jnp.clip(ref_pos - jnp.stack(update), -1.2, 1.2)
    return ref_pos


def interpolate(element_field, corners, target):
    ref_pos = invert_map(corners, target)
    along_x = lagrange_rows(ref_pos[0])
    along_y = lagrange_rows(ref_pos[1])
    along_z = lagrange_rows(ref_pos[2])
    weights = (along_y[:, None, :] * along_z[None, :, :]).reshape(64, -1)
    var_count = element_field.shape[0]
    partial_sum = jnp.dot(element_field.reshape(var_count * 8, 64), weights, precision=EXACT)
    return jnp.sum(partial_sum.reshape(var_count, 8, -1) * along_x[None, :, :], axis=1)


def reference(old_fields, corner_shift, targets, owners):
    block_count = owners.shape[0]
    block_points = targets.reshape(3, block_count, -1).transpose(1, 0, 2)
    cube_signs = corner_signs()

    def per_block(inputs):
        owner_id, target = inputs
        corners = cube_signs + corner_shift[:, owner_id].reshape(3, 8)
        return interpolate(old_fields[owner_id], corners, target)

    result = lax.map(per_block, (owners, block_points), batch_size=64)
    return result.transpose(1, 0, 2).reshape(old_fields.shape[1], -1)
```

```python
import functools

import jax
import jax.numpy as jnp
from jax import lax
from jax.experimental import pallas as pl
from jax.experimental.pallas import tpu as pltpu
from jax.sharding import PartitionSpec as P

NEWTON = 3
CAP = 2
GROUP_PEERS = 4
AXES = ("block", "seg", "sub")

GLL_POINTS = (
    -1.0,
    -0.8717401485096066,
    -0.5917001814331423,
    -0.2092992179024789,
    0.2092992179024789,
    0.5917001814331423,
    0.8717401485096066,
    1.0,
)
WEIGHTS = []
for _n in range(8):
    _w = 1.0
    for _m in range(8):
        if _m != _n:
            _w /= GLL_POINTS[_n] - GLL_POINTS[_m]
    WEIGHTS.append(_w)

F32 = jnp.float32
BF16 = jnp.bfloat16
EXACT = lax.Precision.HIGHEST
NT = (((1,), (1,)), ((), ()))


def iota(shape, dim):
    return lax.broadcasted_iota(jnp.int32, shape, dim)


def flip(index, static):
    bit = 1
    while bit <= static:
        if static & bit:
            index = index + bit * (1 - 2 * ((index // bit) % 2))
        bit *= 2
    return index


def newton(coef, y):
    def update(xi, jac, misfit):
        m = jac
        cof = [
            [m[1][1] * m[2][2] - m[1][2] * m[2][1], m[1][2] * m[2][0] - m[1][0] * m[2][2], m[1][0] * m[2][1] - m[1][1] * m[2][0]],
            [m[0][2] * m[2][1] - m[0][1] * m[2][2], m[0][0] * m[2][2] - m[0][2] * m[2][0], m[0][1] * m[2][0] - m[0][0] * m[2][1]],
            [m[0][1] * m[1][2] - m[0][2] * m[1][1], m[0][2] * m[1][0] - m[0][0] * m[1][2], m[0][0] * m[1][1] - m[0][1] * m[1][0]],
        ]
        inv = 1.0 / (m[0][0] * cof[0][0] + m[0][1] * cof[0][1] + m[0][2] * cof[0][2])
        out = []
        for b in range(3):
            step = (cof[0][b] * misfit[0] + cof[1][b] * misfit[1] + cof[2][b] * misfit[2]) * inv
            new = -step if xi is None else xi[b] - step
            out.append(jnp.clip(new, -1.2, 1.2))
        return out

    xi = update(None, [[c[4], c[2], c[1]] for c in coef], [c[0] - t for c, t in zip(coef, y)])
    for _ in range(NEWTON - 1):
        u, v, w = xi
        uv, uw, vw = u * v, u * w, v * w
        jac, misfit = [], []
        for c, t in zip(coef, y):
            du = c[4] + c[6] * v + c[5] * w + c[7] * vw
            dv = c[2] + c[6] * u + c[3] * w + c[7] * uw
            dw = c[1] + c[5] * u + c[3] * v + c[7] * uv
            jac.append([du, dv, dw])
            misfit.append((c[0] - t) + u * du + v * (c[2] + c[3] * w) + w * c[1])
        xi = update(xi, jac, misfit)
    return xi


def lagrange(x):
    diff = [x - t for t in GLL_POINTS]
    pre = [None, diff[0]]
    for n in range(2, 8):
        pre.append(pre[-1] * diff[n - 1])
    suf = [None] * 8
    suf[6] = diff[7]
    for n in range(5, -1, -1):
        suf[n] = suf[n + 1] * diff[n + 1]
    out = []
    for n in range(8):
        value = suf[n] if n == 0 else pre[n] if n == 7 else pre[n] * suf[n]
        out.append(value * WEIGHTS[n])
    return out


def kernel(sizes, group_peers, owners_hbm, targets_hbm, shift_hbm, fields_hbm, out_ref,
           owners_ref, targets_ref, shift_ref, fbuf, table, send, recv, res, ret, lag, idsend, idrecv, ids, slotv, slots,
           osem, tsem, csem, fsem, idsem, slotsem, s0, r0, s1, r1, s2, r2):
    nb, ns, nc = sizes
    n = nb * ns * nc
    blocks = owners_ref.shape[1]
    elems = shift_ref.shape[1]
    pts = out_ref.shape[2]
    groups = n // group_peers
    lanes = idsend.shape[1]
    wide = idsend.shape[0]
    here = [lax.axis_index(a) for a in AXES]
    me = (here[0] * ns + here[1]) * nc + here[2]

    def peer(k):
        if isinstance(k, int):
            return {
                "block": flip(here[0], k // (ns * nc)),
                "seg": flip(here[1], (k // nc) % ns),
                "sub": flip(here[2], k % nc),
            }
        other = jnp.bitwise_xor(me, k)
        return {"block": other // (ns * nc), "seg": (other // nc) % ns, "sub": other % nc}

    def message(k):
        return pl.ds(8 * k if isinstance(k, int) else pl.multiple_of(8 * k, 8), 3 * CAP)

    def for_wait(first, count, ref, sem):
        part = ref.at[pl.ds(8 * first, 3 * CAP * count), :]
        pltpu.make_async_copy(part, part, sem).wait()

    def send_result(k, g):
        part = pl.ds(CAP * k, CAP)
        return pltpu.make_async_remote_copy(
            src_ref=res.at[part], dst_ref=ret.at[part], send_sem=s2, recv_sem=r2.at[g],
            device_id=peer(k), device_id_type=pl.DeviceIdType.MESH)

    get_owners = pltpu.make_async_copy(owners_hbm, owners_ref, osem)
    get_owners.start()
    get_targets = pltpu.make_async_copy(targets_hbm, targets_ref, tsem)
    get_targets.start()
    get_shift = pltpu.make_async_copy(shift_hbm, shift_ref, csem)
    get_shift.start()
    fetch = pltpu.make_async_copy(fields_hbm, fbuf, fsem)
    fetch.start()
    barrier = pltpu.get_barrier_semaphore()
    unrolled = n <= 32

    def for_peers(first, last, body):
        if unrolled:
            for k in reversed(range(first, last)):
                body(k)
        else:
            lax.fori_loop(first, last, lambda k, c: (body(k), c)[1], 0)

    for_peers(1, n, lambda k: pl.semaphore_signal(
        barrier, inc=1, device_id=peer(k), device_id_type=pl.DeviceIdType.MESH))

    shift_bits = elems.bit_length() - 1
    get_owners.wait()
    own = owners_ref[...]
    owner_dev = jnp.right_shift(own, shift_bits)
    hit = (jnp.bitwise_xor(iota((n, blocks), 0), me) == owner_dev).astype(F32)
    earlier = (iota((blocks, blocks), 0) < iota((blocks, blocks), 1)).astype(F32)
    rank = jnp.dot(hit, earlier, preferred_element_type=F32)
    match = [jnp.where(rank == float(c), hit, 0.0) for c in range(CAP)]
    both = jnp.concatenate(match, axis=0)
    get_targets.wait()
    cat = jnp.concatenate([targets_ref[:, a, :] for a in range(3)], axis=1)
    packed = jnp.dot(both, cat, precision=EXACT, preferred_element_type=F32)
    for c in range(CAP):
        part = slice(c * n, (c + 1) * n)
        for a in range(3):
            send[pl.ds(3 * c + a, n, stride=8), :] = packed[part, a * pts:(a + 1) * pts]
            recv[3 * c + a:3 * c + a + 1, :] = packed[c * n:c * n + 1, a * pts:(a + 1) * pts]
    square = (blocks, blocks)
    diag = iota(square, 0) == iota(square, 1)
    own_rows = jnp.broadcast_to(own, square)
    own_col = jnp.sum(jnp.where(diag, own_rows, 0), axis=1, keepdims=True)
    dev_col = jnp.right_shift(own_col, shift_bits)
    dev_row = jnp.right_shift(own_rows, shift_bits)
    same = jnp.where(dev_col == dev_row, 1, 0)
    rank_row = jnp.sum(jnp.where(iota(square, 0) < iota(square, 1), same, 0), axis=0, keepdims=True)
    rank_col = jnp.sum(jnp.where(iota(square, 1) < iota(square, 0), same, 0), axis=1, keepdims=True)
    place = jnp.minimum(CAP * jnp.bitwise_xor(owner_dev, me) + rank_row, CAP * n - 1)
    place = jnp.concatenate([place, jnp.zeros((1, pts - blocks), jnp.int32)], axis=1)
    elem_col = own_col - dev_col * elems
    lane_of = jnp.where(rank_col < CAP, jnp.bitwise_xor(dev_col, me) + n * rank_col, -1)
    for r in range(wide):
        here_lane = iota((blocks, lanes), 1) + lanes * r == lane_of
        row = jnp.sum(jnp.where(here_lane, elem_col, 0), axis=0, keepdims=True)
        idsend[r:r + 1, :] = row
        idrecv[r:r + 1, :] = row
    slotv[...] = place
    slot_copy = pltpu.make_async_copy(slotv, slots, slotsem)
    slot_copy.start()

    pl.semaphore_wait(barrier, n - 1)
    def send_points(k):
        g = k // group_peers
        pltpu.make_async_remote_copy(
            src_ref=idsend, dst_ref=idrecv.at[pl.ds(wide * k, wide), :], send_sem=s0, recv_sem=r0.at[g],
            device_id=peer(k), device_id_type=pl.DeviceIdType.MESH).start()
        pltpu.make_async_remote_copy(
            src_ref=send.at[message(k), :], dst_ref=recv.at[message(k), :], send_sem=s1, recv_sem=r1.at[g],
            device_id=peer(k), device_id_type=pl.DeviceIdType.MESH).start()

    for_peers(1, n, send_points)

    row, col = iota((24, 24), 0), iota((24, 24), 1)
    both_bits = jnp.bitwise_and(row, col) % 8
    odd = (both_bits + both_bits // 2 + both_bits // 4) % 2
    hada = jnp.where(row // 8 == col // 8, (1 - 2 * odd).astype(F32) * 0.125, 0.0)
    get_shift.wait()
    bits = row % 8
    sign = (1 - 2 * ((bits + bits // 2 + bits // 4) % 2)).astype(F32)
    coefs = jnp.dot(hada * sign, shift_ref[...], precision=EXACT, preferred_element_type=F32)
    c_hi = coefs.astype(BF16)
    rest = coefs - c_hi.astype(F32)
    c_mid = rest.astype(BF16)
    c_lo = (rest - c_mid.astype(F32)).astype(BF16)

    fetch.wait()
    low_sub = iota((8, 128), 0) < 4
    low_lane = iota((8, 128), 1) < 64
    keep = low_sub == low_lane

    def split(e, carry):
        parts = []
        for q in range(4):
            x = fbuf[e, :, q * 128:(q + 1) * 128]
            x = jnp.concatenate([x, x], axis=0)
            hi = x.astype(BF16).astype(F32)
            lo = x - hi
            a = jnp.where(low_sub, hi, lo)
            b = pltpu.roll(jnp.where(low_sub, lo, hi), 64, axis=1)
            parts.append(jnp.where(keep, a, b))
        table[e] = jnp.concatenate(parts, axis=0).astype(BF16)
        return carry

    lax.fori_loop(0, elems, split, 0, unroll=4)

    per = group_peers
    count = CAP * per

    def run_group(g, first):
        base = g * per
        got = per - 1 if first else per
        start = base + 1 if first else base
        for_wait(start, got, recv, r1.at[g])

        def gather(a):
            return jnp.concatenate(
                [recv[pl.ds(8 * base + 3 * c + a, per, stride=8), :] for c in range(CAP)], axis=0)

        y = [gather(a) for a in range(3)]
        taken = idrecv.at[pl.ds(wide * start, wide * got), :]
        pltpu.make_async_copy(taken, taken, r0.at[g]).wait()
        id_copy = pltpu.make_async_copy(idrecv.at[pl.ds(wide * base, wide * per), :], ids.at[pl.ds(wide * base, wide * per), :], idsem)
        id_copy.start()
        id_lane = iota((per, lanes), 1) - iota((per, lanes), 0)
        id_cols = []
        for c in range(CAP):
            at = c * n + base
            id_rows = idrecv[pl.ds(wide * base + at // lanes, per, stride=wide), :]
            id_cols.append(jnp.sum(jnp.where(id_lane == at % lanes, id_rows, 0), axis=1, keepdims=True))
        elem = jnp.concatenate(id_cols, axis=0)
        pick = jnp.where(elem == iota((count, elems), 1), 1.0, 0.0).astype(BF16)
        chosen = sum(lax.dot_general(pick, c, NT, preferred_element_type=F32) for c in (c_hi, c_mid, c_lo))
        coef = []
        for a in range(3):
            line = []
            for m in range(8):
                value = chosen[:, 8 * a + m:8 * a + m + 1]
                if m == 4 >> a:
                    value = value + 1.0
                line.append(jnp.broadcast_to(value, (count, pts)))
            coef.append(line)
        xi = newton(coef, y)
        for a in range(3):
            for i, value in enumerate(lagrange(xi[a])):
                lag[a, pl.ds(i, count, stride=8), :] = value
        id_copy.wait()
        for s in range(count):
            c, p = s // per, s % per
            e = ids[wide * (base + p) + (c * n + base) // lanes, (c * n + base) % lanes + p]
            left = table[e]
            lz = lag[2, 8 * s:8 * s + 8, :]
            w = jnp.concatenate([lag[1, 8 * s + j:8 * s + j + 1, :] * lz for j in range(8)], axis=0)
            w_hi = w.astype(BF16)
            w_lo = (w - w_hi.astype(F32)).astype(BF16)
            prod = jnp.dot(
                jnp.concatenate([left, left], axis=1),
                jnp.concatenate([w_hi, w_hi, w_lo, w_lo], axis=0),
                preferred_element_type=F32)
            total = None
            for q in range(4):
                lx = jnp.where(low_sub, lag[0, 8 * s + 2 * q:8 * s + 2 * q + 1, :],
                               lag[0, 8 * s + 2 * q + 1:8 * s + 2 * q + 2, :])
                term = prod[8 * q:8 * q + 8] * lx
                total = term if total is None else total + term
            total = total[0:4] + total[4:8]
            if first and p == 0:
                ret[c] = total
            else:
                res[CAP * (base + p) + c] = total
        for_peers_in = range(1 if first else 0, per)
        for p in for_peers_in:
            send_result(base + p, g).start()

    run_group(0, True)
    if unrolled:
        for g in range(1, groups):
            run_group(g, False)
    else:
        lax.fori_loop(1, groups, lambda g, c: (run_group(g, False), c)[1], 0)

    slot_copy.wait()
    for g in range(groups):
        start, got = (1, per - 1) if g == 0 else (g * per, per)
        back = ret.at[pl.ds(CAP * start, CAP * got)]
        pltpu.make_async_copy(back, back, r2.at[g]).wait()
    for b in range(blocks):
        out_ref[b] = ret[slots[0, b]]
    rest_ids = idrecv.at[pl.ds(wide, wide * (n - 1)), :]
    pltpu.make_async_copy(rest_ids, rest_ids, s0).wait()
    for_wait(1, n - 1, send, s1)
    left = res.at[pl.ds(CAP, CAP * (n - 1))]
    pltpu.make_async_copy(left, left, s2).wait()


def pair_kernel(sizes, owners_hbm, targets_hbm, shift_hbm, fields_hbm, out_ref,
                owners_ref, targets_ref, shift_ref, fbuf, ctab, send, give, recv, cbuf, lag, res, ret, slots,
                osem, tsem, csem, fsem, s_rel, r_rel, s_fld, r_fld, s_shf, r_shf, s1, r1, s2, r2):
    nb, ns, nc = sizes
    half = nb * ns // 2
    blocks = owners_ref.shape[1]
    elems = shift_ref.shape[2]
    pts = out_ref.shape[2]
    quad = nc * CAP
    rows = 4 * quad
    per = 2 * quad
    b, s, c = [lax.axis_index(a) for a in AXES]
    chip = b * ns + s
    other = 1 - c
    top = nb // 2
    across = b + c * top * (1 - 2 * ((b // top) % 2))

    def peer(j, core):
        return {"block": flip(across, j // ns), "seg": flip(s, j % ns), "sub": core}

    def unless_here(j, body):
        if j == 0:
            pl.when(c == 1)(body)
        else:
            body()

    def remote(src, dst, send_sem, recv_sem, device):
        return pltpu.make_async_remote_copy(
            src_ref=src, dst_ref=dst, send_sem=send_sem, recv_sem=recv_sem,
            device_id=device, device_id_type=pl.DeviceIdType.MESH)

    def wait_for(part, sem):
        pltpu.make_async_copy(part, part, sem).wait()

    get_owners = pltpu.make_async_copy(owners_hbm, owners_ref, osem)
    get_owners.start()
    get_targets = pltpu.make_async_copy(targets_hbm, targets_ref, tsem)
    get_targets.start()
    barrier = pltpu.get_barrier_semaphore()

    def hello(device):
        pl.semaphore_signal(barrier, inc=1, device_id=device, device_id_type=pl.DeviceIdType.MESH)

    for j in reversed(range(half)):
        unless_here(j, lambda: hello(peer(j, c)))
    sibling = {"block": b, "seg": s, "sub": other}
    hello(sibling)
    get_shift = pltpu.make_async_copy(shift_hbm, shift_ref.at[0], csem)
    get_shift.start()
    fetch = pltpu.make_async_copy(fields_hbm, fbuf.at[pl.ds(0, elems)], fsem)
    fetch.start()

    shift_bits = elems.bit_length() - 1
    square = (blocks, blocks)
    get_owners.wait()
    own = owners_ref[...]
    own_rows = jnp.broadcast_to(own, square)
    diag = iota(square, 0) == iota(square, 1)
    own_col = jnp.sum(jnp.where(diag, own_rows, 0), axis=1, keepdims=True)
    dev_col = jnp.right_shift(own_col, shift_bits)
    dev_row = jnp.right_shift(own_rows, shift_bits)
    same = jnp.where(dev_col == dev_row, 1, 0)
    rank_row = jnp.sum(jnp.where(iota(square, 0) < iota(square, 1), same, 0), axis=0, keepdims=True)
    rank_col = jnp.sum(jnp.where(iota(square, 1) < iota(square, 0), same, 0), axis=1, keepdims=True)
    base_chip = jnp.bitwise_xor(chip, c * half)

    def slot_of(dev, rank):
        rel = jnp.bitwise_xor(jnp.right_shift(dev, 1), base_chip)
        return rel, (rel * nc + jnp.bitwise_and(dev, 1)) * CAP + rank

    rel_col, slot_col = slot_of(dev_col, rank_col)
    turned = jnp.where(rel_col >= half, 1, 0)
    side = jnp.bitwise_xor(jnp.bitwise_xor(jnp.bitwise_and(dev_col, 1), c), turned)
    elem_col = own_col - dev_col * elems + elems * side
    _, slot_row = slot_of(jnp.right_shift(own, shift_bits), rank_row)
    count = 2 * half * quad
    pick = jnp.where(iota((count, blocks), 0) == slot_row, 1.0, 0.0)
    id_rows = jnp.broadcast_to(elem_col.astype(F32), (blocks, pts))
    get_targets.wait()
    cat = jnp.concatenate([targets_ref[:, a, :] for a in range(3)] + [id_rows], axis=1)
    packed = jnp.dot(pick, cat, precision=EXACT, preferred_element_type=F32)
    for a in range(4):
        for j in range(half):
            send[j, pl.ds(a, quad, stride=4), :] = packed[quad * j:quad * (j + 1), a * pts:(a + 1) * pts]
            give[j, pl.ds(a, quad, stride=4), :] = packed[quad * (half + j):quad * (half + j + 1), a * pts:(a + 1) * pts]
    slot_safe = jnp.minimum(jnp.maximum(slot_col, 0), count - 1)
    for k in range(blocks):
        slots[0, k] = slot_safe[k, 0]

    low_sub = iota((8, 128), 0) < 4
    low_lane = iota((8, 128), 1) < 64

    def split(e):
        parts = []
        for r in range(0, fbuf.shape[1], 8):
            x = fbuf[e, r:r + 8, :]
            hi = x.astype(BF16).astype(F32)
            lo = x - hi
            turned = pltpu.roll(jnp.where(low_lane, lo, hi), 64, axis=1)
            parts += [jnp.where(low_lane, hi, turned), jnp.where(low_lane, turned, lo)]
        return jnp.concatenate(parts, axis=0).astype(BF16)

    row, col = iota((24, 24), 0), iota((24, 24), 1)
    both_bits = jnp.bitwise_and(row, col) % 8
    odd = (both_bits + both_bits // 2 + both_bits // 4) % 2
    hada = jnp.where(row // 8 == col // 8, (1 - 2 * odd).astype(F32) * 0.125, 0.0)
    bits = row % 8
    sign = (1 - 2 * ((bits + bits // 2 + bits // 4) % 2)).astype(F32)
    line = iota((24, elems), 0)
    unit = jnp.where(line % 8 == jnp.right_shift(4, line // 8), 1.0, 0.0)

    def spread(side):
        coefs = jnp.dot(hada * sign, shift_ref[side], precision=EXACT, preferred_element_type=F32) + unit
        for e in range(elems):
            ctab[side * elems + e] = jnp.broadcast_to(coefs[:, e:e + 1], (24, pts))

    get_shift.wait()
    fetch.wait()
    pl.semaphore_wait(barrier, half + c)
    theirs = send.at[:, pl.ds(rows, rows), :]
    remote(give, theirs, s_rel, r_rel, sibling).start()
    wait_for(theirs, r_rel)
    for j in reversed(range(half)):
        unless_here(j, lambda: remote(
            send.at[j], recv.at[pl.ds(2 * rows * j, 2 * rows), :], s1, r1.at[j], peer(j, c)).start())
    remote(shift_ref.at[0], shift_ref.at[1], s_shf, r_shf, sibling).start()
    remote(fbuf.at[pl.ds(0, elems)], fbuf.at[pl.ds(elems, elems)], s_fld, r_fld, sibling).start()

    @pl.when(c == 0)
    def _():
        recv[0:2 * rows, :] = send[0]

    spread(0)
    wait_for(shift_ref.at[1], r_shf)
    spread(1)
    wait_for(fbuf.at[pl.ds(elems, elems)], r_fld)

    for j in range(half):
        base = 2 * rows * j
        unless_here(j, lambda: wait_for(recv.at[pl.ds(base, 2 * rows), :], r1.at[j]))
        y = [recv[pl.ds(base + a, per, stride=4), :] for a in range(3)]
        ids = recv[pl.ds(base + 3, per, stride=4), :].astype(jnp.int32)
        ids = jnp.minimum(jnp.maximum(ids, 0), 2 * elems - 1)
        elem = [ids[k, 0] for k in range(per)]
        for k in range(per):
            for a in range(3):
                cbuf[a, 8 * k:8 * k + 8, :] = ctab[elem[k], 8 * a:8 * a + 8, :]
        coef = [[cbuf[a, pl.ds(m, per, stride=8), :] for m in range(8)] for a in range(3)]
        xi = newton(coef, y)
        for a in range(3):
            for i, value in enumerate(lagrange(xi[a])):
                lag[a, pl.ds(i, per, stride=8), :] = value
        for k in range(per):
            left = split(elem[k])
            lz = lag[2, 8 * k:8 * k + 8, :]
            w = jnp.concatenate([lag[1, 8 * k + i:8 * k + i + 1, :] * lz for i in range(8)], axis=0)
            w_hi = w.astype(BF16)
            w_lo = (w - w_hi.astype(F32)).astype(BF16)
            prod = jnp.dot(
                jnp.concatenate([left, left], axis=1),
                jnp.concatenate([w_hi, w_hi, w_lo, w_lo], axis=0),
                preferred_element_type=F32)
            total = None
            for q in range(4):
                i = 8 * k + 4 * (q // 2) + q % 2
                lx = jnp.where(low_sub, lag[0, i:i + 1, :], lag[0, i + 2:i + 3, :])
                term = prod[8 * q:8 * q + 8] * lx
                total = term if total is None else total + term
            res[per * j + k] = total[0:4] + total[4:8]

        def result(part, core, slot):
            return remote(res.at[pl.ds(per * j + quad * part, quad)], ret.at[pl.ds(quad * slot, quad)],
                          s2, r2.at[slot], peer(j, core))

        result(1, other, half + j).start()
        unless_here(j, lambda: result(0, c, j).start())
        if j == 0:
            @pl.when(c == 0)
            def _():
                ret[0:quad] = res[0:quad]

    for g in range(2 * half):
        unless_here(g, lambda: wait_for(ret.at[pl.ds(quad * g, quad)], r2.at[g]))
    for k in range(blocks):
        out_ref[k] = ret[slots[0, k]]
    wait_for(theirs, s_rel)
    wait_for(shift_ref.at[1], s_shf)
    wait_for(fbuf.at[pl.ds(elems, elems)], s_fld)

    def finish(skip):
        wait_for(recv.at[pl.ds(2 * rows * skip, 2 * rows * (half - skip)), :], s1)
        wait_for(ret.at[pl.ds(quad * skip, quad * (2 * half - skip))], s2)

    pl.when(c == 0)(lambda: finish(1))
    pl.when(c == 1)(lambda: finish(0))


def paired(sizes, old_fields, corner_shift, points, owners):
    half = sizes[0] * sizes[1] // 2
    elems, nvar, nodes = old_fields.shape
    blocks, _, pts = points.shape
    quad = sizes[2] * CAP
    rows = 4 * quad
    fields = old_fields.reshape(elems, nvar, nodes // 128, 128).transpose(0, 2, 1, 3)
    fields = fields.reshape(elems, nvar * nodes // 128, 128)
    vmem = pl.BlockSpec(memory_space=pltpu.VMEM)
    hbm = pl.BlockSpec(memory_space=pltpu.HBM)
    result = pltpu.VMEM((2 * half * quad, nvar, pts), F32)
    dma = pltpu.SemaphoreType.DMA
    return pl.pallas_call(
        functools.partial(pair_kernel, sizes),
        out_shape=jax.ShapeDtypeStruct((blocks, nvar, pts), F32),
        in_specs=[hbm] * 4,
        out_specs=vmem,
        scratch_shapes=[
            pltpu.VMEM((1, blocks), jnp.int32),
            pltpu.VMEM((blocks, 3, pts), F32),
            pltpu.VMEM((2, 24, elems), F32),
            pltpu.VMEM((2 * elems, nvar * nodes // 128, 128), F32),
            pltpu.VMEM((2 * elems, 24, pts), F32),
            pltpu.VMEM((half, 2 * rows, pts), F32),
            pltpu.VMEM((half, rows, pts), F32),
            pltpu.VMEM((2 * rows * half, pts), F32),
            pltpu.VMEM((3, 16 * quad, pts), F32),
            pltpu.VMEM((3, 16 * quad, pts), F32),
            result, result,
            pltpu.SMEM((1, blocks), jnp.int32),
            *[dma] * 4, *[dma] * 6,
            dma, dma((half,)), dma, dma((2 * half,)),
        ],
        compiler_params=pltpu.CompilerParams(
            collective_id=0, has_side_effects=True, vmem_limit_bytes=24 * 1024 * 1024),
    )(*[pltpu.with_memory_space_constraint(x, pltpu.HBM) for x in (owners.reshape(1, blocks), points, corner_shift, fields)])


def shards(sizes, old_fields, corner_shift, targets, owners):
    n = sizes[0] * sizes[1] * sizes[2]
    elems, nvar, nodes = old_fields.shape
    blocks = owners.shape[0]
    pts = targets.shape[1] // blocks
    assert n & (n - 1) == 0 and elems & (elems - 1) == 0 and nvar == 4 and nodes == 512
    group_peers = min(GROUP_PEERS, n)
    groups = n // group_peers
    wide = (CAP * n + 127) // 128
    points = targets.reshape(3, blocks, pts).transpose(1, 0, 2)
    if n <= 32 and sizes[0] > 1 and sizes[2] == 2:
        out = paired(sizes, old_fields, corner_shift, points, owners)
        return out.transpose(1, 0, 2).reshape(nvar, blocks * pts)
    vmem = pl.BlockSpec(memory_space=pltpu.VMEM)
    hbm = pl.BlockSpec(memory_space=pltpu.HBM)
    message = pltpu.VMEM((8 * n, pts), F32)
    result = pltpu.VMEM((CAP * n, nvar, pts), F32)
    out = pl.pallas_call(
        functools.partial(kernel, sizes, group_peers),
        out_shape=jax.ShapeDtypeStruct((blocks, nvar, pts), F32),
        in_specs=[hbm] * 4,
        out_specs=vmem,
        scratch_shapes=[
            pltpu.VMEM((1, blocks), jnp.int32),
            pltpu.VMEM((blocks, 3, pts), F32),
            pltpu.VMEM((24, elems), F32),
            pltpu.VMEM((elems, nvar, nodes), F32),
            pltpu.VMEM((elems, 32, 128), BF16),
            message, message, result, result,
            pltpu.VMEM((3, 8 * CAP * group_peers, pts), F32),
            pltpu.VMEM((wide, 128), jnp.int32),
            pltpu.VMEM((wide * n, 128), jnp.int32),
            pltpu.SMEM((wide * n, 128), jnp.int32),
            pltpu.VMEM((1, pts), jnp.int32),
            pltpu.SMEM((1, pts), jnp.int32),
            *[pltpu.SemaphoreType.DMA] * 6,
            pltpu.SemaphoreType.DMA, pltpu.SemaphoreType.DMA((groups,)),
            pltpu.SemaphoreType.DMA, pltpu.SemaphoreType.DMA((groups,)),
            pltpu.SemaphoreType.DMA, pltpu.SemaphoreType.DMA((groups,)),
        ],
        compiler_params=pltpu.CompilerParams(
            collective_id=0, has_side_effects=True, vmem_limit_bytes=16 * 1024 * 1024),
    )(*[pltpu.with_memory_space_constraint(x, pltpu.HBM) for x in (owners.reshape(1, blocks), points, corner_shift, old_fields)])
    return out.transpose(1, 0, 2).reshape(nvar, blocks * pts)


def solution(mesh):
    sizes = tuple(mesh.shape[a] for a in AXES)
    in_specs = (
        P(("groups", "block", "seg", "sub"), None, None),
        P(None, ("groups", "block", "seg", "sub")),
        P(None, ("groups", "block", "seg", "sub")),
        P(("groups", "block", "seg", "sub")),
    )
    out_specs = P(None, ("groups", "block", "seg", "sub"))
    return jax.shard_map(functools.partial(shards, sizes), mesh=mesh, in_specs=in_specs,
                         out_specs=out_specs, check_vma=False)
```

```python
import functools

import jax
import jax.numpy as jnp
from jax import lax
from jax.experimental import pallas as pl
from jax.experimental.pallas import tpu as pltpu
from jax.sharding import PartitionSpec as P

NEWTON = 3
CAP = 2
GROUP_PEERS = 4
AXES = ("block", "seg", "sub")

GLL_POINTS = (
    -1.0,
    -0.8717401485096066,
    -0.5917001814331423,
    -0.2092992179024789,
    0.2092992179024789,
    0.5917001814331423,
    0.8717401485096066,
    1.0,
)
WEIGHTS = []
for _n in range(8):
    _w = 1.0
    for _m in range(8):
        if _m != _n:
            _w /= GLL_POINTS[_n] - GLL_POINTS[_m]
    WEIGHTS.append(_w)

F32 = jnp.float32
BF16 = jnp.bfloat16
EXACT = lax.Precision.HIGHEST
NT = (((1,), (1,)), ((), ()))


def iota(shape, dim):
    return lax.broadcasted_iota(jnp.int32, shape, dim)


def flip(index, static):
    bit = 1
    while bit <= static:
        if static & bit:
            index = index + bit * (1 - 2 * ((index // bit) % 2))
        bit *= 2
    return index


def newton(coef, y):
    def update(xi, jac, misfit):
        m = jac
        cof = [
            [m[1][1] * m[2][2] - m[1][2] * m[2][1], m[1][2] * m[2][0] - m[1][0] * m[2][2], m[1][0] * m[2][1] - m[1][1] * m[2][0]],
            [m[0][2] * m[2][1] - m[0][1] * m[2][2], m[0][0] * m[2][2] - m[0][2] * m[2][0], m[0][1] * m[2][0] - m[0][0] * m[2][1]],
            [m[0][1] * m[1][2] - m[0][2] * m[1][1], m[0][2] * m[1][0] - m[0][0] * m[1][2], m[0][0] * m[1][1] - m[0][1] * m[1][0]],
        ]
        inv = 1.0 / (m[0][0] * cof[0][0] + m[0][1] * cof[0][1] + m[0][2] * cof[0][2])
        out = []
        for b in range(3):
            step = (cof[0][b] * misfit[0] + cof[1][b] * misfit[1] + cof[2][b] * misfit[2]) * inv
            new = -step if xi is None else xi[b] - step
            out.append(jnp.clip(new, -1.2, 1.2))
        return out

    xi = update(None, [[c[4], c[2], c[1]] for c in coef], [c[0] - t for c, t in zip(coef, y)])
    for _ in range(NEWTON - 1):
        u, v, w = xi
        uv, uw, vw = u * v, u * w, v * w
        jac, misfit = [], []
        for c, t in zip(coef, y):
            du = c[4] + c[6] * v + c[5] * w + c[7] * vw
            dv = c[2] + c[6] * u + c[3] * w + c[7] * uw
            dw = c[1] + c[5] * u + c[3] * v + c[7] * uv
            jac.append([du, dv, dw])
            misfit.append((c[0] - t) + u * du + v * (c[2] + c[3] * w) + w * c[1])
        xi = update(xi, jac, misfit)
    return xi


def lagrange(x):
    diff = [x - t for t in GLL_POINTS]
    pre = [None, diff[0]]
    for n in range(2, 8):
        pre.append(pre[-1] * diff[n - 1])
    suf = [None] * 8
    suf[6] = diff[7]
    for n in range(5, -1, -1):
        suf[n] = suf[n + 1] * diff[n + 1]
    out = []
    for n in range(8):
        value = suf[n] if n == 0 else pre[n] if n == 7 else pre[n] * suf[n]
        out.append(value * WEIGHTS[n])
    return out


def kernel(sizes, group_peers, owners_hbm, targets_hbm, shift_hbm, fields_hbm, out_ref,
           owners_ref, targets_ref, shift_ref, fbuf, table, send, recv, res, ret, lag, idsend, idrecv, ids, slotv, slots,
           osem, tsem, csem, fsem, idsem, slotsem, s0, r0, s1, r1, s2, r2):
    nb, ns, nc = sizes
    n = nb * ns * nc
    blocks = owners_ref.shape[1]
    elems = shift_ref.shape[1]
    pts = out_ref.shape[2]
    groups = n // group_peers
    lanes = idsend.shape[1]
    wide = idsend.shape[0]
    here = [lax.axis_index(a) for a in AXES]
    me = (here[0] * ns + here[1]) * nc + here[2]

    def peer(k):
        if isinstance(k, int):
            return {
                "block": flip(here[0], k // (ns * nc)),
                "seg": flip(here[1], (k // nc) % ns),
                "sub": flip(here[2], k % nc),
            }
        other = jnp.bitwise_xor(me, k)
        return {"block": other // (ns * nc), "seg": (other // nc) % ns, "sub": other % nc}

    def message(k):
        return pl.ds(8 * k if isinstance(k, int) else pl.multiple_of(8 * k, 8), 3 * CAP)

    def for_wait(first, count, ref, sem):
        part = ref.at[pl.ds(8 * first, 3 * CAP * count), :]
        pltpu.make_async_copy(part, part, sem).wait()

    def send_result(k, g):
        part = pl.ds(CAP * k, CAP)
        return pltpu.make_async_remote_copy(
            src_ref=res.at[part], dst_ref=ret.at[part], send_sem=s2, recv_sem=r2.at[g],
            device_id=peer(k), device_id_type=pl.DeviceIdType.MESH)

    get_owners = pltpu.make_async_copy(owners_hbm, owners_ref, osem)
    get_owners.start()
    get_targets = pltpu.make_async_copy(targets_hbm, targets_ref, tsem)
    get_targets.start()
    get_shift = pltpu.make_async_copy(shift_hbm, shift_ref, csem)
    get_shift.start()
    fetch = pltpu.make_async_copy(fields_hbm, fbuf, fsem)
    fetch.start()
    barrier = pltpu.get_barrier_semaphore()
    unrolled = n <= 32

    def for_peers(first, last, body):
        if unrolled:
            for k in reversed(range(first, last)):
                body(k)
        else:
            lax.fori_loop(first, last, lambda k, c: (body(k), c)[1], 0)

    for_peers(1, n, lambda k: pl.semaphore_signal(
        barrier, inc=1, device_id=peer(k), device_id_type=pl.DeviceIdType.MESH))

    shift_bits = elems.bit_length() - 1
    get_owners.wait()
    own = owners_ref[...]
    owner_dev = jnp.right_shift(own, shift_bits)
    hit = (jnp.bitwise_xor(iota((n, blocks), 0), me) == owner_dev).astype(F32)
    earlier = (iota((blocks, blocks), 0) < iota((blocks, blocks), 1)).astype(F32)
    rank = jnp.dot(hit, earlier, preferred_element_type=F32)
    match = [jnp.where(rank == float(c), hit, 0.0) for c in range(CAP)]
    both = jnp.concatenate(match, axis=0)
    get_targets.wait()
    cat = jnp.concatenate([targets_ref[:, a, :] for a in range(3)], axis=1)
    packed = jnp.dot(both, cat, precision=EXACT, preferred_element_type=F32)
    for c in range(CAP):
        part = slice(c * n, (c + 1) * n)
        for a in range(3):
            send[pl.ds(3 * c + a, n, stride=8), :] = packed[part, a * pts:(a + 1) * pts]
            recv[3 * c + a:3 * c + a + 1, :] = packed[c * n:c * n + 1, a * pts:(a + 1) * pts]
    square = (blocks, blocks)
    diag = iota(square, 0) == iota(square, 1)
    own_rows = jnp.broadcast_to(own, square)
    own_col = jnp.sum(jnp.where(diag, own_rows, 0), axis=1, keepdims=True)
    dev_col = jnp.right_shift(own_col, shift_bits)
    dev_row = jnp.right_shift(own_rows, shift_bits)
    same = jnp.where(dev_col == dev_row, 1, 0)
    rank_row = jnp.sum(jnp.where(iota(square, 0) < iota(square, 1), same, 0), axis=0, keepdims=True)
    rank_col = jnp.sum(jnp.where(iota(square, 1) < iota(square, 0), same, 0), axis=1, keepdims=True)
    place = jnp.minimum(CAP * jnp.bitwise_xor(owner_dev, me) + rank_row, CAP * n - 1)
    place = jnp.concatenate([place, jnp.zeros((1, pts - blocks), jnp.int32)], axis=1)
    elem_col = own_col - dev_col * elems
    lane_of = jnp.where(rank_col < CAP, jnp.bitwise_xor(dev_col, me) + n * rank_col, -1)
    for r in range(wide):
        here_lane = iota((blocks, lanes), 1) + lanes * r == lane_of
        row = jnp.sum(jnp.where(here_lane, elem_col, 0), axis=0, keepdims=True)
        idsend[r:r + 1, :] = row
        idrecv[r:r + 1, :] = row
    slotv[...] = place
    slot_copy = pltpu.make_async_copy(slotv, slots, slotsem)
    slot_copy.start()

    pl.semaphore_wait(barrier, n - 1)
    def send_points(k):
        g = k // group_peers
        pltpu.make_async_remote_copy(
            src_ref=idsend, dst_ref=idrecv.at[pl.ds(wide * k, wide), :], send_sem=s0, recv_sem=r0.at[g],
            device_id=peer(k), device_id_type=pl.DeviceIdType.MESH).start()
        pltpu.make_async_remote_copy(
            src_ref=send.at[message(k), :], dst_ref=recv.at[message(k), :], send_sem=s1, recv_sem=r1.at[g],
            device_id=peer(k), device_id_type=pl.DeviceIdType.MESH).start()

    for_peers(1, n, send_points)

    row, col = iota((24, 24), 0), iota((24, 24), 1)
    both_bits = jnp.bitwise_and(row, col) % 8
    odd = (both_bits + both_bits // 2 + both_bits // 4) % 2
    hada = jnp.where(row // 8 == col // 8, (1 - 2 * odd).astype(F32) * 0.125, 0.0)
    get_shift.wait()
    bits = row % 8
    sign = (1 - 2 * ((bits + bits // 2 + bits // 4) % 2)).astype(F32)
    coefs = jnp.dot(hada * sign, shift_ref[...], precision=EXACT, preferred_element_type=F32)
    c_hi = coefs.astype(BF16)
    rest = coefs - c_hi.astype(F32)
    c_mid = rest.astype(BF16)
    c_lo = (rest - c_mid.astype(F32)).astype(BF16)

    fetch.wait()
    low_sub = iota((8, 128), 0) < 4
    low_lane = iota((8, 128), 1) < 64
    keep = low_sub == low_lane

    def split(e, carry):
        parts = []
        for q in range(4):
            x = fbuf[e, :, q * 128:(q + 1) * 128]
            x = jnp.concatenate([x, x], axis=0)
            hi = x.astype(BF16).astype(F32)
            lo = x - hi
            a = jnp.where(low_sub, hi, lo)
            b = pltpu.roll(jnp.where(low_sub, lo, hi), 64, axis=1)
            parts.append(jnp.where(keep, a, b))
        table[e] = jnp.concatenate(parts, axis=0).astype(BF16)
        return carry

    lax.fori_loop(0, elems, split, 0, unroll=4)

    per = group_peers
    count = CAP * per

    def run_group(g, first):
        base = g * per
        got = per - 1 if first else per
        start = base + 1 if first else base
        for_wait(start, got, recv, r1.at[g])

        def gather(a):
            return jnp.concatenate(
                [recv[pl.ds(8 * base + 3 * c + a, per, stride=8), :] for c in range(CAP)], axis=0)

        y = [gather(a) for a in range(3)]
        taken = idrecv.at[pl.ds(wide * start, wide * got), :]
        pltpu.make_async_copy(taken, taken, r0.at[g]).wait()
        id_copy = pltpu.make_async_copy(idrecv.at[pl.ds(wide * base, wide * per), :], ids.at[pl.ds(wide * base, wide * per), :], idsem)
        id_copy.start()
        id_lane = iota((per, lanes), 1) - iota((per, lanes), 0)
        id_cols = []
        for c in range(CAP):
            at = c * n + base
            id_rows = idrecv[pl.ds(wide * base + at // lanes, per, stride=wide), :]
            id_cols.append(jnp.sum(jnp.where(id_lane == at % lanes, id_rows, 0), axis=1, keepdims=True))
        elem = jnp.concatenate(id_cols, axis=0)
        pick = jnp.where(elem == iota((count, elems), 1), 1.0, 0.0).astype(BF16)
        chosen = sum(lax.dot_general(pick, c, NT, preferred_element_type=F32) for c in (c_hi, c_mid, c_lo))
        coef = []
        for a in range(3):
            line = []
            for m in range(8):
                value = chosen[:, 8 * a + m:8 * a + m + 1]
                if m == 4 >> a:
                    value = value + 1.0
                line.append(jnp.broadcast_to(value, (count, pts)))
            coef.append(line)
        xi = newton(coef, y)
        for a in range(3):
            for i, value in enumerate(lagrange(xi[a])):
                lag[a, pl.ds(i, count, stride=8), :] = value
        id_copy.wait()
        for s in range(count):
            c, p = s // per, s % per
            e = ids[wide * (base + p) + (c * n + base) // lanes, (c * n + base) % lanes + p]
            left = table[e]
            lz = lag[2, 8 * s:8 * s + 8, :]
            w = jnp.concatenate([lag[1, 8 * s + j:8 * s + j + 1, :] * lz for j in range(8)], axis=0)
            w_hi = w.astype(BF16)
            w_lo = (w - w_hi.astype(F32)).astype(BF16)
            prod = jnp.dot(
                jnp.concatenate([left, left], axis=1),
                jnp.concatenate([w_hi, w_hi, w_lo, w_lo], axis=0),
                preferred_element_type=F32)
            total = None
            for q in range(4):
                lx = jnp.where(low_sub, lag[0, 8 * s + 2 * q:8 * s + 2 * q + 1, :],
                               lag[0, 8 * s + 2 * q + 1:8 * s + 2 * q + 2, :])
                term = prod[8 * q:8 * q + 8] * lx
                total = term if total is None else total + term
            total = total[0:4] + total[4:8]
            if first and p == 0:
                ret[c] = total
            else:
                res[CAP * (base + p) + c] = total
        for_peers_in = range(1 if first else 0, per)
        for p in for_peers_in:
            send_result(base + p, g).start()

    run_group(0, True)
    if unrolled:
        for g in range(1, groups):
            run_group(g, False)
    else:
        lax.fori_loop(1, groups, lambda g, c: (run_group(g, False), c)[1], 0)

    slot_copy.wait()
    for g in range(groups):
        start, got = (1, per - 1) if g == 0 else (g * per, per)
        back = ret.at[pl.ds(CAP * start, CAP * got)]
        pltpu.make_async_copy(back, back, r2.at[g]).wait()
    for b in range(blocks):
        out_ref[b] = ret[slots[0, b]]
    rest_ids = idrecv.at[pl.ds(wide, wide * (n - 1)), :]
    pltpu.make_async_copy(rest_ids, rest_ids, s0).wait()
    for_wait(1, n - 1, send, s1)
    left = res.at[pl.ds(CAP, CAP * (n - 1))]
    pltpu.make_async_copy(left, left, s2).wait()


def pair_kernel(sizes, owners_hbm, targets_hbm, shift_hbm, fields_hbm, out_ref,
                owners_ref, targets_ref, shift_ref, fbuf, ctab, send, give, recv, cbuf, lag, res, ret, slots,
                osem, tsem, csem, fsem, s_rel, r_rel, s_fld, r_fld, s_shf, r_shf, s1, r1, s2, r2):
    nb, ns, nc = sizes
    half = nb * ns // 2
    blocks = owners_ref.shape[1]
    elems = shift_ref.shape[2]
    pts = out_ref.shape[2]
    quad = nc * CAP
    rows = 4 * quad
    per = 2 * quad
    b, s, c = [lax.axis_index(a) for a in AXES]
    chip = b * ns + s
    other = 1 - c
    top = nb // 2
    across = b + c * top * (1 - 2 * ((b // top) % 2))

    def peer(j, core):
        return {"block": flip(across, j // ns), "seg": flip(s, j % ns), "sub": core}

    def near(j, core):
        return {"block": flip(b, j // ns), "seg": flip(s, j % ns), "sub": core}

    def unless_here(j, body):
        if j == 0:
            pl.when(c == 1)(body)
        else:
            body()

    def remote(src, dst, send_sem, recv_sem, device):
        return pltpu.make_async_remote_copy(
            src_ref=src, dst_ref=dst, send_sem=send_sem, recv_sem=recv_sem,
            device_id=device, device_id_type=pl.DeviceIdType.MESH)

    def wait_for(part, sem):
        pltpu.make_async_copy(part, part, sem).wait()

    get_owners = pltpu.make_async_copy(owners_hbm, owners_ref, osem)
    get_owners.start()
    get_targets = pltpu.make_async_copy(targets_hbm, targets_ref, tsem)
    get_targets.start()
    barrier = pltpu.get_barrier_semaphore()

    def hello(device):
        pl.semaphore_signal(barrier, inc=1, device_id=device, device_id_type=pl.DeviceIdType.MESH)

    for j in reversed(range(half)):
        unless_here(j, lambda: hello(peer(j, c)))
    sibling = {"block": b, "seg": s, "sub": other}
    hello(sibling)

    @pl.when(c == 0)
    def _():
        for j in range(1, half):
            hello(near(j, 1))

    get_shift = pltpu.make_async_copy(shift_hbm, shift_ref.at[0], csem)
    get_shift.start()
    fetch = pltpu.make_async_copy(fields_hbm, fbuf.at[pl.ds(0, elems)], fsem)
    fetch.start()

    shift_bits = elems.bit_length() - 1
    square = (blocks, blocks)
    get_owners.wait()
    own = owners_ref[...]
    own_rows = jnp.broadcast_to(own, square)
    diag = iota(square, 0) == iota(square, 1)
    own_col = jnp.sum(jnp.where(diag, own_rows, 0), axis=1, keepdims=True)
    dev_col = jnp.right_shift(own_col, shift_bits)
    dev_row = jnp.right_shift(own_rows, shift_bits)
    same = jnp.where(dev_col == dev_row, 1, 0)
    rank_row = jnp.sum(jnp.where(iota(square, 0) < iota(square, 1), same, 0), axis=0, keepdims=True)
    rank_col = jnp.sum(jnp.where(iota(square, 1) < iota(square, 0), same, 0), axis=1, keepdims=True)
    base_chip = jnp.bitwise_xor(chip, c * half)

    def slot_of(dev, rank):
        rel = jnp.bitwise_xor(jnp.right_shift(dev, 1), base_chip)
        return rel, (rel * nc + jnp.bitwise_and(dev, 1)) * CAP + rank

    rel_col, slot_col = slot_of(dev_col, rank_col)
    turned = jnp.where(rel_col >= half, 1, 0)
    side = jnp.bitwise_xor(jnp.bitwise_xor(jnp.bitwise_and(dev_col, 1), c), turned)
    elem_col = own_col - dev_col * elems + elems * side
    _, slot_row = slot_of(jnp.right_shift(own, shift_bits), rank_row)
    count = 2 * half * quad
    pick = jnp.where(iota((count, blocks), 0) == slot_row, 1.0, 0.0)
    id_rows = jnp.broadcast_to(elem_col.astype(F32), (blocks, pts))
    get_targets.wait()
    cat = jnp.concatenate([targets_ref[:, a, :] for a in range(3)] + [id_rows], axis=1)
    packed = jnp.dot(pick, cat, precision=EXACT, preferred_element_type=F32)
    for a in range(4):
        for j in range(half):
            send[j, pl.ds(a, quad, stride=4), :] = packed[quad * j:quad * (j + 1), a * pts:(a + 1) * pts]
            give[j, pl.ds(a, quad, stride=4), :] = packed[quad * (half + j):quad * (half + j + 1), a * pts:(a + 1) * pts]
    slot_safe = jnp.minimum(jnp.maximum(slot_col, 0), count - 1)
    for k in range(blocks):
        slots[0, k] = slot_safe[k, 0]

    low_sub = iota((8, 128), 0) < 4
    low_lane = iota((8, 128), 1) < 64

    def split(e):
        parts = []
        for r in range(0, fbuf.shape[1], 8):
            x = fbuf[e, r:r + 8, :]
            hi = x.astype(BF16).astype(F32)
            lo = x - hi
            turned = pltpu.roll(jnp.where(low_lane, lo, hi), 64, axis=1)
            parts += [jnp.where(low_lane, hi, turned), jnp.where(low_lane, turned, lo)]
        return jnp.concatenate(parts, axis=0).astype(BF16)

    row, col = iota((24, 24), 0), iota((24, 24), 1)
    both_bits = jnp.bitwise_and(row, col) % 8
    odd = (both_bits + both_bits // 2 + both_bits // 4) % 2
    hada = jnp.where(row // 8 == col // 8, (1 - 2 * odd).astype(F32) * 0.125, 0.0)
    bits = row % 8
    sign = (1 - 2 * ((bits + bits // 2 + bits // 4) % 2)).astype(F32)
    line = iota((24, elems), 0)
    unit = jnp.where(line % 8 == jnp.right_shift(4, line // 8), 1.0, 0.0)

    def spread(side):
        coefs = jnp.dot(hada * sign, shift_ref[side], precision=EXACT, preferred_element_type=F32) + unit
        for e in range(elems):
            ctab[side * elems + e] = jnp.broadcast_to(coefs[:, e:e + 1], (24, pts))

    get_shift.wait()
    fetch.wait()
    pl.semaphore_wait(barrier, half + c * half)
    theirs = send.at[:, pl.ds(rows, rows), :]

    @pl.when(c == 0)
    def _():
        remote(give, theirs, s_rel, r_rel, sibling).start()
        for j in reversed(range(1, half)):
            remote(send.at[j, pl.ds(0, rows), :], recv.at[pl.ds(2 * rows * j, rows), :], s1, r1.at[j], near(j, 0)).start()

    @pl.when(c == 1)
    def _():
        def far(j):
            remote(send.at[j], recv.at[pl.ds(2 * rows * j, 2 * rows), :], s1, r1.at[j], peer(j, 1)).start()

        wait_for(theirs, r_rel)
        for j in reversed(range(half // 2, half)):
            far(j)
        for j in reversed(range(half)):
            remote(give.at[j], recv.at[pl.ds(2 * rows * j + rows, rows), :], s_rel, r1.at[j], near(j, 0)).start()
        for j in reversed(range(half // 2)):
            far(j)

    remote(shift_ref.at[0], shift_ref.at[1], s_shf, r_shf, sibling).start()
    remote(fbuf.at[pl.ds(0, elems)], fbuf.at[pl.ds(elems, elems)], s_fld, r_fld, sibling).start()

    @pl.when(c == 0)
    def _():
        recv[0:rows, :] = send[0, 0:rows, :]

    spread(0)
    wait_for(shift_ref.at[1], r_shf)
    spread(1)
    wait_for(fbuf.at[pl.ds(elems, elems)], r_fld)

    order = list(range(half - 2)) + [half - 1, half - 2] if half > 1 else [0]
    for j in order:
        base = 2 * rows * j
        unless_here(j, lambda: wait_for(recv.at[pl.ds(base, 2 * rows), :], r1.at[j]))
        if j == 0:
            pl.when(c == 0)(lambda: wait_for(recv.at[pl.ds(base + rows, rows), :], r1.at[j]))
        y = [recv[pl.ds(base + a, per, stride=4), :] for a in range(3)]
        ids = recv[pl.ds(base + 3, per, stride=4), :].astype(jnp.int32)
        ids = jnp.minimum(jnp.maximum(ids, 0), 2 * elems - 1)
        elem = [ids[k, 0] for k in range(per)]
        for k in range(per):
            for a in range(3):
                cbuf[a, 8 * k:8 * k + 8, :] = ctab[elem[k], 8 * a:8 * a + 8, :]
        coef = [[cbuf[a, pl.ds(m, per, stride=8), :] for m in range(8)] for a in range(3)]
        xi = newton(coef, y)
        for a in range(3):
            for i, value in enumerate(lagrange(xi[a])):
                lag[a, pl.ds(i, per, stride=8), :] = value
        for k in range(per):
            left = split(elem[k])
            lz = lag[2, 8 * k:8 * k + 8, :]
            w = jnp.concatenate([lag[1, 8 * k + i:8 * k + i + 1, :] * lz for i in range(8)], axis=0)
            w_hi = w.astype(BF16)
            w_lo = (w - w_hi.astype(F32)).astype(BF16)
            prod = jnp.dot(
                jnp.concatenate([left, left], axis=1),
                jnp.concatenate([w_hi, w_hi, w_lo, w_lo], axis=0),
                preferred_element_type=F32)
            total = None
            for q in range(4):
                i = 8 * k + 4 * (q // 2) + q % 2
                lx = jnp.where(low_sub, lag[0, i:i + 1, :], lag[0, i + 2:i + 3, :])
                term = prod[8 * q:8 * q + 8] * lx
                total = term if total is None else total + term
            res[per * j + k] = total[0:4] + total[4:8]

        def result(part, core, slot):
            return remote(res.at[pl.ds(per * j + quad * part, quad)], ret.at[pl.ds(quad * slot, quad)],
                          s2, r2.at[slot], peer(j, core))

        result(1, other, half + j).start()
        unless_here(j, lambda: result(0, c, j).start())
        if j == 0:
            @pl.when(c == 0)
            def _():
                ret[0:quad] = res[0:quad]

    for g in range(2 * half):
        unless_here(g, lambda: wait_for(ret.at[pl.ds(quad * g, quad)], r2.at[g]))
    for k in range(blocks):
        out_ref[k] = ret[slots[0, k]]
    wait_for(give, s_rel)
    wait_for(shift_ref.at[1], s_shf)
    wait_for(fbuf.at[pl.ds(elems, elems)], s_fld)

    def finish(skip):
        wait_for(recv.at[pl.ds(0, (half - 1 if skip else 2 * half) * rows), :], s1)
        wait_for(ret.at[pl.ds(quad * skip, quad * (2 * half - skip))], s2)

    pl.when(c == 0)(lambda: finish(1))
    pl.when(c == 1)(lambda: finish(0))


def paired(sizes, old_fields, corner_shift, points, owners):
    half = sizes[0] * sizes[1] // 2
    elems, nvar, nodes = old_fields.shape
    blocks, _, pts = points.shape
    quad = sizes[2] * CAP
    rows = 4 * quad
    fields = old_fields.reshape(elems, nvar, nodes // 128, 128).transpose(0, 2, 1, 3)
    fields = fields.reshape(elems, nvar * nodes // 128, 128)
    vmem = pl.BlockSpec(memory_space=pltpu.VMEM)
    hbm = pl.BlockSpec(memory_space=pltpu.HBM)
    result = pltpu.VMEM((2 * half * quad, nvar, pts), F32)
    dma = pltpu.SemaphoreType.DMA
    return pl.pallas_call(
        functools.partial(pair_kernel, sizes),
        out_shape=jax.ShapeDtypeStruct((blocks, nvar, pts), F32),
        in_specs=[hbm] * 4,
        out_specs=vmem,
        scratch_shapes=[
            pltpu.VMEM((1, blocks), jnp.int32),
            pltpu.VMEM((blocks, 3, pts), F32),
            pltpu.VMEM((2, 24, elems), F32),
            pltpu.VMEM((2 * elems, nvar * nodes // 128, 128), F32),
            pltpu.VMEM((2 * elems, 24, pts), F32),
            pltpu.VMEM((half, 2 * rows, pts), F32),
            pltpu.VMEM((half, rows, pts), F32),
            pltpu.VMEM((2 * rows * half, pts), F32),
            pltpu.VMEM((3, 16 * quad, pts), F32),
            pltpu.VMEM((3, 16 * quad, pts), F32),
            result, result,
            pltpu.SMEM((1, blocks), jnp.int32),
            *[dma] * 4, *[dma] * 6,
            dma, dma((half,)), dma, dma((2 * half,)),
        ],
        compiler_params=pltpu.CompilerParams(
            collective_id=0, has_side_effects=True, vmem_limit_bytes=24 * 1024 * 1024),
    )(*[pltpu.with_memory_space_constraint(x, pltpu.HBM) for x in (owners.reshape(1, blocks), points, corner_shift, fields)])


def shards(sizes, old_fields, corner_shift, targets, owners):
    n = sizes[0] * sizes[1] * sizes[2]
    elems, nvar, nodes = old_fields.shape
    blocks = owners.shape[0]
    pts = targets.shape[1] // blocks
    assert n & (n - 1) == 0 and elems & (elems - 1) == 0 and nvar == 4 and nodes == 512
    group_peers = min(GROUP_PEERS, n)
    groups = n // group_peers
    wide = (CAP * n + 127) // 128
    points = targets.reshape(3, blocks, pts).transpose(1, 0, 2)
    if n <= 32 and sizes[0] > 1 and sizes[2] == 2:
        out = paired(sizes, old_fields, corner_shift, points, owners)
        return out.transpose(1, 0, 2).reshape(nvar, blocks * pts)
    vmem = pl.BlockSpec(memory_space=pltpu.VMEM)
    hbm = pl.BlockSpec(memory_space=pltpu.HBM)
    message = pltpu.VMEM((8 * n, pts), F32)
    result = pltpu.VMEM((CAP * n, nvar, pts), F32)
    out = pl.pallas_call(
        functools.partial(kernel, sizes, group_peers),
        out_shape=jax.ShapeDtypeStruct((blocks, nvar, pts), F32),
        in_specs=[hbm] * 4,
        out_specs=vmem,
        scratch_shapes=[
            pltpu.VMEM((1, blocks), jnp.int32),
            pltpu.VMEM((blocks, 3, pts), F32),
            pltpu.VMEM((24, elems), F32),
            pltpu.VMEM((elems, nvar, nodes), F32),
            pltpu.VMEM((elems, 32, 128), BF16),
            message, message, result, result,
            pltpu.VMEM((3, 8 * CAP * group_peers, pts), F32),
            pltpu.VMEM((wide, 128), jnp.int32),
            pltpu.VMEM((wide * n, 128), jnp.int32),
            pltpu.SMEM((wide * n, 128), jnp.int32),
            pltpu.VMEM((1, pts), jnp.int32),
            pltpu.SMEM((1, pts), jnp.int32),
            *[pltpu.SemaphoreType.DMA] * 6,
            pltpu.SemaphoreType.DMA, pltpu.SemaphoreType.DMA((groups,)),
            pltpu.SemaphoreType.DMA, pltpu.SemaphoreType.DMA((groups,)),
            pltpu.SemaphoreType.DMA, pltpu.SemaphoreType.DMA((groups,)),
        ],
        compiler_params=pltpu.CompilerParams(
            collective_id=0, has_side_effects=True, vmem_limit_bytes=16 * 1024 * 1024),
    )(*[pltpu.with_memory_space_constraint(x, pltpu.HBM) for x in (owners.reshape(1, blocks), points, corner_shift, old_fields)])
    return out.transpose(1, 0, 2).reshape(nvar, blocks * pts)


def solution(mesh):
    sizes = tuple(mesh.shape[a] for a in AXES)
    in_specs = (
        P(("groups", "block", "seg", "sub"), None, None),
        P(None, ("groups", "block", "seg", "sub")),
        P(None, ("groups", "block", "seg", "sub")),
        P(("groups", "block", "seg", "sub")),
    )
    out_specs = P(None, ("groups", "block", "seg", "sub"))
    return jax.shard_map(functools.partial(shards, sizes), mesh=mesh, in_specs=in_specs,
                         out_specs=out_specs, check_vma=False)
```

```python
import functools

import jax
import jax.numpy as jnp
from jax import lax
from jax.experimental import pallas as pl
from jax.experimental.pallas import tpu as pltpu
from jax.sharding import PartitionSpec as P

NEWTON = 3
CAP = 2
GROUP_PEERS = 4
AXES = ("block", "seg", "sub")

GLL_POINTS = (
    -1.0,
    -0.8717401485096066,
    -0.5917001814331423,
    -0.2092992179024789,
    0.2092992179024789,
    0.5917001814331423,
    0.8717401485096066,
    1.0,
)
WEIGHTS = []
for _n in range(8):
    _w = 1.0
    for _m in range(8):
        if _m != _n:
            _w /= GLL_POINTS[_n] - GLL_POINTS[_m]
    WEIGHTS.append(_w)

F32 = jnp.float32
BF16 = jnp.bfloat16
EXACT = lax.Precision.HIGHEST
NT = (((1,), (1,)), ((), ()))


def iota(shape, dim):
    return lax.broadcasted_iota(jnp.int32, shape, dim)


def flip(index, static):
    bit = 1
    while bit <= static:
        if static & bit:
            index = index + bit * (1 - 2 * ((index // bit) % 2))
        bit *= 2
    return index


def newton(coef, y):
    def update(xi, jac, misfit):
        m = jac
        cof = [
            [m[1][1] * m[2][2] - m[1][2] * m[2][1], m[1][2] * m[2][0] - m[1][0] * m[2][2], m[1][0] * m[2][1] - m[1][1] * m[2][0]],
            [m[0][2] * m[2][1] - m[0][1] * m[2][2], m[0][0] * m[2][2] - m[0][2] * m[2][0], m[0][1] * m[2][0] - m[0][0] * m[2][1]],
            [m[0][1] * m[1][2] - m[0][2] * m[1][1], m[0][2] * m[1][0] - m[0][0] * m[1][2], m[0][0] * m[1][1] - m[0][1] * m[1][0]],
        ]
        inv = 1.0 / (m[0][0] * cof[0][0] + m[0][1] * cof[0][1] + m[0][2] * cof[0][2])
        out = []
        for b in range(3):
            step = (cof[0][b] * misfit[0] + cof[1][b] * misfit[1] + cof[2][b] * misfit[2]) * inv
            new = -step if xi is None else xi[b] - step
            out.append(jnp.clip(new, -1.2, 1.2))
        return out

    xi = update(None, [[c[4], c[2], c[1]] for c in coef], [c[0] - t for c, t in zip(coef, y)])
    for _ in range(NEWTON - 1):
        u, v, w = xi
        uv, uw, vw = u * v, u * w, v * w
        jac, misfit = [], []
        for c, t in zip(coef, y):
            du = c[4] + c[6] * v + c[5] * w + c[7] * vw
            dv = c[2] + c[6] * u + c[3] * w + c[7] * uw
            dw = c[1] + c[5] * u + c[3] * v + c[7] * uv
            jac.append([du, dv, dw])
            misfit.append((c[0] - t) + u * du + v * (c[2] + c[3] * w) + w * c[1])
        xi = update(xi, jac, misfit)
    return xi


def lagrange(x):
    diff = [x - t for t in GLL_POINTS]
    pre = [None, diff[0]]
    for n in range(2, 8):
        pre.append(pre[-1] * diff[n - 1])
    suf = [None] * 8
    suf[6] = diff[7]
    for n in range(5, -1, -1):
        suf[n] = suf[n + 1] * diff[n + 1]
    out = []
    for n in range(8):
        value = suf[n] if n == 0 else pre[n] if n == 7 else pre[n] * suf[n]
        out.append(value * WEIGHTS[n])
    return out


def kernel(sizes, group_peers, owners_hbm, targets_hbm, shift_hbm, fields_hbm, out_ref,
           owners_ref, targets_ref, shift_ref, fbuf, table, send, recv, res, ret, lag, idsend, idrecv, ids, slotv, slots,
           osem, tsem, csem, fsem, idsem, slotsem, s0, r0, s1, r1, s2, r2):
    nb, ns, nc = sizes
    n = nb * ns * nc
    blocks = owners_ref.shape[1]
    elems = shift_ref.shape[1]
    pts = out_ref.shape[2]
    groups = n // group_peers
    lanes = idsend.shape[1]
    wide = idsend.shape[0]
    here = [lax.axis_index(a) for a in AXES]
    me = (here[0] * ns + here[1]) * nc + here[2]

    def peer(k):
        if isinstance(k, int):
            return {
                "block": flip(here[0], k // (ns * nc)),
                "seg": flip(here[1], (k // nc) % ns),
                "sub": flip(here[2], k % nc),
            }
        other = jnp.bitwise_xor(me, k)
        return {"block": other // (ns * nc), "seg": (other // nc) % ns, "sub": other % nc}

    def message(k):
        return pl.ds(8 * k if isinstance(k, int) else pl.multiple_of(8 * k, 8), 3 * CAP)

    def for_wait(first, count, ref, sem):
        part = ref.at[pl.ds(8 * first, 3 * CAP * count), :]
        pltpu.make_async_copy(part, part, sem).wait()

    def send_result(k, g):
        part = pl.ds(CAP * k, CAP)
        return pltpu.make_async_remote_copy(
            src_ref=res.at[part], dst_ref=ret.at[part], send_sem=s2, recv_sem=r2.at[g],
            device_id=peer(k), device_id_type=pl.DeviceIdType.MESH)

    get_owners = pltpu.make_async_copy(owners_hbm, owners_ref, osem)
    get_owners.start()
    get_targets = pltpu.make_async_copy(targets_hbm, targets_ref, tsem)
    get_targets.start()
    get_shift = pltpu.make_async_copy(shift_hbm, shift_ref, csem)
    get_shift.start()
    fetch = pltpu.make_async_copy(fields_hbm, fbuf, fsem)
    fetch.start()
    barrier = pltpu.get_barrier_semaphore()
    unrolled = n <= 32

    def for_peers(first, last, body):
        if unrolled:
            for k in reversed(range(first, last)):
                body(k)
        else:
            lax.fori_loop(first, last, lambda k, c: (body(k), c)[1], 0)

    for_peers(1, n, lambda k: pl.semaphore_signal(
        barrier, inc=1, device_id=peer(k), device_id_type=pl.DeviceIdType.MESH))

    shift_bits = elems.bit_length() - 1
    get_owners.wait()
    own = owners_ref[...]
    owner_dev = jnp.right_shift(own, shift_bits)
    hit = (jnp.bitwise_xor(iota((n, blocks), 0), me) == owner_dev).astype(F32)
    earlier = (iota((blocks, blocks), 0) < iota((blocks, blocks), 1)).astype(F32)
    rank = jnp.dot(hit, earlier, preferred_element_type=F32)
    match = [jnp.where(rank == float(c), hit, 0.0) for c in range(CAP)]
    both = jnp.concatenate(match, axis=0)
    get_targets.wait()
    cat = jnp.concatenate([targets_ref[:, a, :] for a in range(3)], axis=1)
    packed = jnp.dot(both, cat, precision=EXACT, preferred_element_type=F32)
    for c in range(CAP):
        part = slice(c * n, (c + 1) * n)
        for a in range(3):
            send[pl.ds(3 * c + a, n, stride=8), :] = packed[part, a * pts:(a + 1) * pts]
            recv[3 * c + a:3 * c + a + 1, :] = packed[c * n:c * n + 1, a * pts:(a + 1) * pts]
    square = (blocks, blocks)
    diag = iota(square, 0) == iota(square, 1)
    own_rows = jnp.broadcast_to(own, square)
    own_col = jnp.sum(jnp.where(diag, own_rows, 0), axis=1, keepdims=True)
    dev_col = jnp.right_shift(own_col, shift_bits)
    dev_row = jnp.right_shift(own_rows, shift_bits)
    same = jnp.where(dev_col == dev_row, 1, 0)
    rank_row = jnp.sum(jnp.where(iota(square, 0) < iota(square, 1), same, 0), axis=0, keepdims=True)
    rank_col = jnp.sum(jnp.where(iota(square, 1) < iota(square, 0), same, 0), axis=1, keepdims=True)
    place = jnp.minimum(CAP * jnp.bitwise_xor(owner_dev, me) + rank_row, CAP * n - 1)
    place = jnp.concatenate([place, jnp.zeros((1, pts - blocks), jnp.int32)], axis=1)
    elem_col = own_col - dev_col * elems
    lane_of = jnp.where(rank_col < CAP, jnp.bitwise_xor(dev_col, me) + n * rank_col, -1)
    for r in range(wide):
        here_lane = iota((blocks, lanes), 1) + lanes * r == lane_of
        row = jnp.sum(jnp.where(here_lane, elem_col, 0), axis=0, keepdims=True)
        idsend[r:r + 1, :] = row
        idrecv[r:r + 1, :] = row
    slotv[...] = place
    slot_copy = pltpu.make_async_copy(slotv, slots, slotsem)
    slot_copy.start()

    pl.semaphore_wait(barrier, n - 1)
    def send_points(k):
        g = k // group_peers
        pltpu.make_async_remote_copy(
            src_ref=idsend, dst_ref=idrecv.at[pl.ds(wide * k, wide), :], send_sem=s0, recv_sem=r0.at[g],
            device_id=peer(k), device_id_type=pl.DeviceIdType.MESH).start()
        pltpu.make_async_remote_copy(
            src_ref=send.at[message(k), :], dst_ref=recv.at[message(k), :], send_sem=s1, recv_sem=r1.at[g],
            device_id=peer(k), device_id_type=pl.DeviceIdType.MESH).start()

    for_peers(1, n, send_points)

    row, col = iota((24, 24), 0), iota((24, 24), 1)
    both_bits = jnp.bitwise_and(row, col) % 8
    odd = (both_bits + both_bits // 2 + both_bits // 4) % 2
    hada = jnp.where(row // 8 == col // 8, (1 - 2 * odd).astype(F32) * 0.125, 0.0)
    get_shift.wait()
    bits = row % 8
    sign = (1 - 2 * ((bits + bits // 2 + bits // 4) % 2)).astype(F32)
    coefs = jnp.dot(hada * sign, shift_ref[...], precision=EXACT, preferred_element_type=F32)
    c_hi = coefs.astype(BF16)
    rest = coefs - c_hi.astype(F32)
    c_mid = rest.astype(BF16)
    c_lo = (rest - c_mid.astype(F32)).astype(BF16)

    fetch.wait()
    low_sub = iota((8, 128), 0) < 4
    low_lane = iota((8, 128), 1) < 64
    keep = low_sub == low_lane

    def split(e, carry):
        parts = []
        for q in range(4):
            x = fbuf[e, :, q * 128:(q + 1) * 128]
            x = jnp.concatenate([x, x], axis=0)
            hi = x.astype(BF16).astype(F32)
            lo = x - hi
            a = jnp.where(low_sub, hi, lo)
            b = pltpu.roll(jnp.where(low_sub, lo, hi), 64, axis=1)
            parts.append(jnp.where(keep, a, b))
        table[e] = jnp.concatenate(parts, axis=0).astype(BF16)
        return carry

    lax.fori_loop(0, elems, split, 0, unroll=4)

    per = group_peers
    count = CAP * per

    def run_group(g, first):
        base = g * per
        got = per - 1 if first else per
        start = base + 1 if first else base
        for_wait(start, got, recv, r1.at[g])

        def gather(a):
            return jnp.concatenate(
                [recv[pl.ds(8 * base + 3 * c + a, per, stride=8), :] for c in range(CAP)], axis=0)

        y = [gather(a) for a in range(3)]
        taken = idrecv.at[pl.ds(wide * start, wide * got), :]
        pltpu.make_async_copy(taken, taken, r0.at[g]).wait()
        id_copy = pltpu.make_async_copy(idrecv.at[pl.ds(wide * base, wide * per), :], ids.at[pl.ds(wide * base, wide * per), :], idsem)
        id_copy.start()
        id_lane = iota((per, lanes), 1) - iota((per, lanes), 0)
        id_cols = []
        for c in range(CAP):
            at = c * n + base
            id_rows = idrecv[pl.ds(wide * base + at // lanes, per, stride=wide), :]
            id_cols.append(jnp.sum(jnp.where(id_lane == at % lanes, id_rows, 0), axis=1, keepdims=True))
        elem = jnp.concatenate(id_cols, axis=0)
        pick = jnp.where(elem == iota((count, elems), 1), 1.0, 0.0).astype(BF16)
        chosen = sum(lax.dot_general(pick, c, NT, preferred_element_type=F32) for c in (c_hi, c_mid, c_lo))
        coef = []
        for a in range(3):
            line = []
            for m in range(8):
                value = chosen[:, 8 * a + m:8 * a + m + 1]
                if m == 4 >> a:
                    value = value + 1.0
                line.append(jnp.broadcast_to(value, (count, pts)))
            coef.append(line)
        xi = newton(coef, y)
        for a in range(3):
            for i, value in enumerate(lagrange(xi[a])):
                lag[a, pl.ds(i, count, stride=8), :] = value
        id_copy.wait()
        for s in range(count):
            c, p = s // per, s % per
            e = ids[wide * (base + p) + (c * n + base) // lanes, (c * n + base) % lanes + p]
            left = table[e]
            lz = lag[2, 8 * s:8 * s + 8, :]
            w = jnp.concatenate([lag[1, 8 * s + j:8 * s + j + 1, :] * lz for j in range(8)], axis=0)
            w_hi = w.astype(BF16)
            w_lo = (w - w_hi.astype(F32)).astype(BF16)
            prod = jnp.dot(
                jnp.concatenate([left, left], axis=1),
                jnp.concatenate([w_hi, w_hi, w_lo, w_lo], axis=0),
                preferred_element_type=F32)
            total = None
            for q in range(4):
                lx = jnp.where(low_sub, lag[0, 8 * s + 2 * q:8 * s + 2 * q + 1, :],
                               lag[0, 8 * s + 2 * q + 1:8 * s + 2 * q + 2, :])
                term = prod[8 * q:8 * q + 8] * lx
                total = term if total is None else total + term
            total = total[0:4] + total[4:8]
            if first and p == 0:
                ret[c] = total
            else:
                res[CAP * (base + p) + c] = total
        for_peers_in = range(1 if first else 0, per)
        for p in for_peers_in:
            send_result(base + p, g).start()

    run_group(0, True)
    if unrolled:
        for g in range(1, groups):
            run_group(g, False)
    else:
        lax.fori_loop(1, groups, lambda g, c: (run_group(g, False), c)[1], 0)

    slot_copy.wait()
    for g in range(groups):
        start, got = (1, per - 1) if g == 0 else (g * per, per)
        back = ret.at[pl.ds(CAP * start, CAP * got)]
        pltpu.make_async_copy(back, back, r2.at[g]).wait()
    for b in range(blocks):
        out_ref[b] = ret[slots[0, b]]
    rest_ids = idrecv.at[pl.ds(wide, wide * (n - 1)), :]
    pltpu.make_async_copy(rest_ids, rest_ids, s0).wait()
    for_wait(1, n - 1, send, s1)
    left = res.at[pl.ds(CAP, CAP * (n - 1))]
    pltpu.make_async_copy(left, left, s2).wait()


def pair_kernel(sizes, owners_hbm, targets_hbm, shift_hbm, fields_hbm, out_ref,
                owners_ref, targets_ref, shift_ref, fbuf, ctab, send, give, via, recv, cbuf, lag, res, ret, slots,
                osem, tsem, csem, fsem, s_rel, r_rel, s_fld, r_fld, s_shf, r_shf, s1, r1, s2, r2, r_via, here):
    nb, ns, nc = sizes
    half = nb * ns // 2
    blocks = owners_ref.shape[1]
    elems = shift_ref.shape[2]
    pts = out_ref.shape[2]
    quad = nc * CAP
    rows = 4 * quad
    per = 2 * quad
    b, s, c = [lax.axis_index(a) for a in AXES]
    chip = b * ns + s
    other = 1 - c
    top = nb // 2
    across = b + c * top * (1 - 2 * ((b // top) % 2))

    def peer(j, core):
        return {"block": flip(across, j // ns), "seg": flip(s, j % ns), "sub": core}

    def near(j, core):
        return {"block": flip(b, j // ns), "seg": flip(s, j % ns), "sub": core}

    def unless_here(j, body):
        if j == 0:
            pl.when(c == 1)(body)
        else:
            body()

    def remote(src, dst, send_sem, recv_sem, device):
        return pltpu.make_async_remote_copy(
            src_ref=src, dst_ref=dst, send_sem=send_sem, recv_sem=recv_sem,
            device_id=device, device_id_type=pl.DeviceIdType.MESH)

    def wait_for(part, sem):
        pltpu.make_async_copy(part, part, sem).wait()

    get_owners = pltpu.make_async_copy(owners_hbm, owners_ref, osem)
    get_owners.start()
    get_targets = pltpu.make_async_copy(targets_hbm, targets_ref, tsem)
    get_targets.start()
    barrier = pltpu.get_barrier_semaphore()

    def hello(device):
        pl.semaphore_signal(barrier, inc=1, device_id=device, device_id_type=pl.DeviceIdType.MESH)

    sibling = {"block": b, "seg": s, "sub": other}
    partner = {"block": b, "seg": flip(s, 1), "sub": 1}
    first = jnp.logical_and(c == 1, b == 0)
    high = jnp.logical_and(c == 1, b >= top)

    def above(j):
        return b % 2 == 0 if j // ns else s == 0

    def below(j):
        return b % 2 == 1 if j // ns else s == 1

    @pl.when(c == 1)
    def _():
        @pl.when(b < top)
        def _():
            for j in reversed(range(half)):
                hello(peer(j, 1))

        pl.when(b == 0)(lambda: hello(partner))
        hello(sibling)

    @pl.when(c == 0)
    def _():
        for j in reversed(range(1, half)):
            pl.when(above(j))(lambda: hello(near(j, 0)))

    get_shift = pltpu.make_async_copy(shift_hbm, shift_ref.at[0], csem)
    get_shift.start()
    fetch = pltpu.make_async_copy(fields_hbm, fbuf.at[pl.ds(0, elems)], fsem)
    fetch.start()

    pl.when(c == 0)(lambda: pl.semaphore_wait(barrier, 1 + (b % 2) * ns + s))
    pl.when(high)(lambda: pl.semaphore_wait(barrier, half))

    def answer(j, device):
        pl.semaphore_signal(here.at[j], inc=1, device_id=device, device_id_type=pl.DeviceIdType.MESH)

    @pl.when(high)
    def _():
        for j in reversed(range(half)):
            if j % ns:
                pl.when(flip(across, j // ns) != 0)(lambda: answer(j, peer(j, 1)))
            else:
                answer(j, peer(j, 1))

    @pl.when(c == 0)
    def _():
        for j in reversed(range(1, half)):
            pl.when(below(j))(lambda: answer(j, near(j, 0)))

    shift_bits = elems.bit_length() - 1
    square = (blocks, blocks)
    get_owners.wait()
    own = owners_ref[...]
    own_rows = jnp.broadcast_to(own, square)
    diag = iota(square, 0) == iota(square, 1)
    own_col = jnp.sum(jnp.where(diag, own_rows, 0), axis=1, keepdims=True)
    dev_col = jnp.right_shift(own_col, shift_bits)
    dev_row = jnp.right_shift(own_rows, shift_bits)
    same = jnp.where(dev_col == dev_row, 1, 0)
    rank_row = jnp.sum(jnp.where(iota(square, 0) < iota(square, 1), same, 0), axis=0, keepdims=True)
    rank_col = jnp.sum(jnp.where(iota(square, 1) < iota(square, 0), same, 0), axis=1, keepdims=True)
    base_chip = jnp.bitwise_xor(chip, c * half)

    def slot_of(dev, rank):
        rel = jnp.bitwise_xor(jnp.right_shift(dev, 1), base_chip)
        return rel, (rel * nc + jnp.bitwise_and(dev, 1)) * CAP + rank

    rel_col, slot_col = slot_of(dev_col, rank_col)
    turned = jnp.where(rel_col >= half, 1, 0)
    side = jnp.bitwise_xor(jnp.bitwise_xor(jnp.bitwise_and(dev_col, 1), c), turned)
    elem_col = own_col - dev_col * elems + elems * side
    _, slot_row = slot_of(jnp.right_shift(own, shift_bits), rank_row)
    count = 2 * half * quad
    pick = jnp.where(iota((count, blocks), 0) == slot_row, 1.0, 0.0)
    id_rows = jnp.broadcast_to(elem_col.astype(F32), (blocks, pts))
    get_targets.wait()
    cat = jnp.concatenate([targets_ref[:, a, :] for a in range(3)] + [id_rows], axis=1)
    packed = jnp.dot(pick, cat, precision=EXACT, preferred_element_type=F32)
    for a in range(4):
        for j in range(half):
            send[j, pl.ds(a, quad, stride=4), :] = packed[quad * j:quad * (j + 1), a * pts:(a + 1) * pts]
            give[j, pl.ds(a, quad, stride=4), :] = packed[quad * (half + j):quad * (half + j + 1), a * pts:(a + 1) * pts]
    slot_safe = jnp.minimum(jnp.maximum(slot_col, 0), count - 1)
    for k in range(blocks):
        slots[0, k] = slot_safe[k, 0]

    low_sub = iota((8, 128), 0) < 4
    low_lane = iota((8, 128), 1) < 64

    def split(e):
        parts = []
        for r in range(0, fbuf.shape[1], 8):
            x = fbuf[e, r:r + 8, :]
            hi = x.astype(BF16).astype(F32)
            lo = x - hi
            turned = pltpu.roll(jnp.where(low_lane, lo, hi), 64, axis=1)
            parts += [jnp.where(low_lane, hi, turned), jnp.where(low_lane, turned, lo)]
        return jnp.concatenate(parts, axis=0).astype(BF16)

    row, col = iota((24, 24), 0), iota((24, 24), 1)
    both_bits = jnp.bitwise_and(row, col) % 8
    odd = (both_bits + both_bits // 2 + both_bits // 4) % 2
    hada = jnp.where(row // 8 == col // 8, (1 - 2 * odd).astype(F32) * 0.125, 0.0)
    bits = row % 8
    sign = (1 - 2 * ((bits + bits // 2 + bits // 4) % 2)).astype(F32)
    line = iota((24, elems), 0)
    unit = jnp.where(line % 8 == jnp.right_shift(4, line // 8), 1.0, 0.0)

    def spread(side):
        coefs = jnp.dot(hada * sign, shift_ref[side], precision=EXACT, preferred_element_type=F32) + unit
        for e in range(elems):
            ctab[side * elems + e] = jnp.broadcast_to(coefs[:, e:e + 1], (24, pts))

    get_shift.wait()
    fetch.wait()
    pl.when(first)(lambda: pl.semaphore_wait(barrier, 1))
    theirs = send.at[:, pl.ds(rows, rows), :]

    def heard(j):
        pl.semaphore_wait(here.at[j], 1)

    def share():
        remote(shift_ref.at[0], shift_ref.at[1], s_shf, r_shf, sibling).start()
        remote(fbuf.at[pl.ds(0, elems)], fbuf.at[pl.ds(elems, elems)], s_fld, r_fld, sibling).start()

    corner = (b % 2) * ns + s

    def request(src, group, device):
        at = pl.multiple_of(2 * rows * group, 2 * rows)
        remote(src, recv.at[pl.ds(at, 2 * rows), :], s1, r1.at[group], device).start()

    @pl.when(c == 0)
    def _():
        remote(give, theirs, s_rel, r_rel, sibling).start()
        share()
        wait_for(theirs, r_rel)
        for j in reversed(range(1, half)):
            pl.when(above(j))(lambda: heard(j))
            request(send.at[j], corner, near(j, 0))
        recv[pl.ds(pl.multiple_of(2 * rows * corner, 2 * rows), 2 * rows), :] = send[0]

    @pl.when(c == 1)
    def _():
        wait_for(theirs, r_rel)

        @pl.when(b == 0)
        def _():
            for j in reversed(range(1, half, ns)):
                remote(send.at[j], via.at[j // ns], s1, r_via.at[j // ns], partner).start()

        remote(give, theirs, s_rel, r_rel, sibling).start()

        def pass_on(i):
            wait_for(via.at[i], r_via.at[i])
            request(via.at[i], flip(s, 1), peer(ns * i, 1))

        def own(i):
            request(send.at[ns * i], corner, peer(ns * i, 1))

        columns = list(reversed(range(half // ns)))

        @pl.when(jnp.logical_and(b == 0, s == 0))
        def _():
            for i in columns:
                heard(ns * i)
                own(i)
            share()
            for i in columns:
                pass_on(i)

        @pl.when(jnp.logical_and(b == 0, s == 1))
        def _():
            for i in columns:
                heard(ns * i)
                pass_on(i)
                own(i)
            share()

        @pl.when(b > 0)
        def _():
            for j in reversed(range(half)):
                pl.when(b < top)(lambda: heard(j))
                request(send.at[j], corner, peer(j, 1))
            share()

    spread(0)
    wait_for(shift_ref.at[1], r_shf)
    spread(1)
    wait_for(fbuf.at[pl.ds(elems, elems)], r_fld)

    for g in range(half):
        base = 2 * rows * g
        z, x = g // ns, g % ns
        local = jnp.logical_and(c == 0, corner == g)

        def unless_local(body):
            pl.when(jnp.logical_not(local))(body)

        unless_local(lambda: wait_for(recv.at[pl.ds(base, 2 * rows), :], r1.at[g]))
        y = [recv[pl.ds(base + a, per, stride=4), :] for a in range(3)]
        ids = recv[pl.ds(base + 3, per, stride=4), :].astype(jnp.int32)
        ids = jnp.minimum(jnp.maximum(ids, 0), 2 * elems - 1)
        elem = [ids[k, 0] for k in range(per)]
        for k in range(per):
            for a in range(3):
                cbuf[a, 8 * k:8 * k + 8, :] = ctab[elem[k], 8 * a:8 * a + 8, :]
        coef = [[cbuf[a, pl.ds(m, per, stride=8), :] for m in range(8)] for a in range(3)]
        xi = newton(coef, y)
        for a in range(3):
            for i, value in enumerate(lagrange(xi[a])):
                lag[a, pl.ds(i, per, stride=8), :] = value
        for k in range(per):
            left = split(elem[k])
            lz = lag[2, 8 * k:8 * k + 8, :]
            w = jnp.concatenate([lag[1, 8 * k + i:8 * k + i + 1, :] * lz for i in range(8)], axis=0)
            w_hi = w.astype(BF16)
            w_lo = (w - w_hi.astype(F32)).astype(BF16)
            prod = jnp.dot(
                jnp.concatenate([left, left], axis=1),
                jnp.concatenate([w_hi, w_hi, w_lo, w_lo], axis=0),
                preferred_element_type=F32)
            total = None
            for q in range(4):
                i = 8 * k + 4 * (q // 2) + q % 2
                lx = jnp.where(low_sub, lag[0, i:i + 1, :], lag[0, i + 2:i + 3, :])
                term = prod[8 * q:8 * q + 8] * lx
                total = term if total is None else total + term
            res[per * g + k] = total[0:4] + total[4:8]

        slot = ns * flip(b % 2, z) + flip(s, x)

        def result(part, core, to):
            return remote(res.at[pl.ds(per * g + quad * part, quad)], ret.at[pl.ds(quad * to, quad)],
                          s2, r2.at[to], {"block": 2 * (across // 2) + z, "seg": x, "sub": core})

        result(1, other, half + slot).start()
        unless_local(lambda: result(0, c, slot).start())

        @pl.when(local)
        def _():
            ret[0:quad] = res[per * g:per * g + quad]

    for g in range(2 * half):
        unless_here(g, lambda: wait_for(ret.at[pl.ds(quad * g, quad)], r2.at[g]))
    for k in range(blocks):
        out_ref[k] = ret[slots[0, k]]
    wait_for(give, s_rel)
    wait_for(shift_ref.at[1], s_shf)
    wait_for(fbuf.at[pl.ds(elems, elems)], s_fld)

    def finish(skip):
        wait_for(recv.at[pl.ds(2 * rows * skip, 2 * rows * (half - skip)), :], s1)
        wait_for(ret.at[pl.ds(quad * skip, quad * (2 * half - skip))], s2)

    pl.when(c == 0)(lambda: finish(1))
    pl.when(c == 1)(lambda: finish(0))
    pl.when(first)(lambda: wait_for(via, s1))


def paired(sizes, old_fields, corner_shift, points, owners):
    half = sizes[0] * sizes[1] // 2
    elems, nvar, nodes = old_fields.shape
    blocks, _, pts = points.shape
    quad = sizes[2] * CAP
    rows = 4 * quad
    fields = old_fields.reshape(elems, nvar, nodes // 128, 128).transpose(0, 2, 1, 3)
    fields = fields.reshape(elems, nvar * nodes // 128, 128)
    vmem = pl.BlockSpec(memory_space=pltpu.VMEM)
    hbm = pl.BlockSpec(memory_space=pltpu.HBM)
    result = pltpu.VMEM((2 * half * quad, nvar, pts), F32)
    dma = pltpu.SemaphoreType.DMA
    return pl.pallas_call(
        functools.partial(pair_kernel, sizes),
        out_shape=jax.ShapeDtypeStruct((blocks, nvar, pts), F32),
        in_specs=[hbm] * 4,
        out_specs=vmem,
        scratch_shapes=[
            pltpu.VMEM((1, blocks), jnp.int32),
            pltpu.VMEM((blocks, 3, pts), F32),
            pltpu.VMEM((2, 24, elems), F32),
            pltpu.VMEM((2 * elems, nvar * nodes // 128, 128), F32),
            pltpu.VMEM((2 * elems, 24, pts), F32),
            pltpu.VMEM((half, 2 * rows, pts), F32),
            pltpu.VMEM((half, rows, pts), F32),
            pltpu.VMEM((half // sizes[1], 2 * rows, pts), F32),
            pltpu.VMEM((2 * rows * half, pts), F32),
            pltpu.VMEM((3, 16 * quad, pts), F32),
            pltpu.VMEM((3, 16 * quad, pts), F32),
            result, result,
            pltpu.SMEM((1, blocks), jnp.int32),
            *[dma] * 4, *[dma] * 6,
            dma, dma((half,)), dma, dma((2 * half,)),
            dma((half // sizes[1],)), pltpu.SemaphoreType.REGULAR((half,)),
        ],
        compiler_params=pltpu.CompilerParams(
            collective_id=0, has_side_effects=True, vmem_limit_bytes=24 * 1024 * 1024),
    )(*[pltpu.with_memory_space_constraint(x, pltpu.HBM) for x in (owners.reshape(1, blocks), points, corner_shift, fields)])


def shards(sizes, old_fields, corner_shift, targets, owners):
    n = sizes[0] * sizes[1] * sizes[2]
    elems, nvar, nodes = old_fields.shape
    blocks = owners.shape[0]
    pts = targets.shape[1] // blocks
    assert n & (n - 1) == 0 and elems & (elems - 1) == 0 and nvar == 4 and nodes == 512
    group_peers = min(GROUP_PEERS, n)
    groups = n // group_peers
    wide = (CAP * n + 127) // 128
    points = targets.reshape(3, blocks, pts).transpose(1, 0, 2)
    if sizes[0] == 4 and sizes[1] == 2 and sizes[2] == 2:
        out = paired(sizes, old_fields, corner_shift, points, owners)
        return out.transpose(1, 0, 2).reshape(nvar, blocks * pts)
    vmem = pl.BlockSpec(memory_space=pltpu.VMEM)
    hbm = pl.BlockSpec(memory_space=pltpu.HBM)
    message = pltpu.VMEM((8 * n, pts), F32)
    result = pltpu.VMEM((CAP * n, nvar, pts), F32)
    out = pl.pallas_call(
        functools.partial(kernel, sizes, group_peers),
        out_shape=jax.ShapeDtypeStruct((blocks, nvar, pts), F32),
        in_specs=[hbm] * 4,
        out_specs=vmem,
        scratch_shapes=[
            pltpu.VMEM((1, blocks), jnp.int32),
            pltpu.VMEM((blocks, 3, pts), F32),
            pltpu.VMEM((24, elems), F32),
            pltpu.VMEM((elems, nvar, nodes), F32),
            pltpu.VMEM((elems, 32, 128), BF16),
            message, message, result, result,
            pltpu.VMEM((3, 8 * CAP * group_peers, pts), F32),
            pltpu.VMEM((wide, 128), jnp.int32),
            pltpu.VMEM((wide * n, 128), jnp.int32),
            pltpu.SMEM((wide * n, 128), jnp.int32),
            pltpu.VMEM((1, pts), jnp.int32),
            pltpu.SMEM((1, pts), jnp.int32),
            *[pltpu.SemaphoreType.DMA] * 6,
            pltpu.SemaphoreType.DMA, pltpu.SemaphoreType.DMA((groups,)),
            pltpu.SemaphoreType.DMA, pltpu.SemaphoreType.DMA((groups,)),
            pltpu.SemaphoreType.DMA, pltpu.SemaphoreType.DMA((groups,)),
        ],
        compiler_params=pltpu.CompilerParams(
            collective_id=0, has_side_effects=True, vmem_limit_bytes=16 * 1024 * 1024),
    )(*[pltpu.with_memory_space_constraint(x, pltpu.HBM) for x in (owners.reshape(1, blocks), points, corner_shift, old_fields)])
    return out.transpose(1, 0, 2).reshape(nvar, blocks * pts)


def solution(mesh):
    sizes = tuple(mesh.shape[a] for a in AXES)
    in_specs = (
        P(("groups", "block", "seg", "sub"), None, None),
        P(None, ("groups", "block", "seg", "sub")),
        P(None, ("groups", "block", "seg", "sub")),
        P(("groups", "block", "seg", "sub")),
    )
    out_specs = P(None, ("groups", "block", "seg", "sub"))
    return jax.shard_map(functools.partial(shards, sizes), mesh=mesh, in_specs=in_specs,
                         out_specs=out_specs, check_vma=False)
```

```python
import functools

import jax
import jax.numpy as jnp
from jax import lax
from jax.experimental import pallas as pl
from jax.experimental.pallas import tpu as pltpu
from jax.sharding import PartitionSpec as P

NEWTON = 3
CAP = 2
GROUP_PEERS = 4
AXES = ("block", "seg", "sub")

GLL_POINTS = (
    -1.0,
    -0.8717401485096066,
    -0.5917001814331423,
    -0.2092992179024789,
    0.2092992179024789,
    0.5917001814331423,
    0.8717401485096066,
    1.0,
)
WEIGHTS = []
for _n in range(8):
    _w = 1.0
    for _m in range(8):
        if _m != _n:
            _w /= GLL_POINTS[_n] - GLL_POINTS[_m]
    WEIGHTS.append(_w)

F32 = jnp.float32
BF16 = jnp.bfloat16
EXACT = lax.Precision.HIGHEST
NT = (((1,), (1,)), ((), ()))


def iota(shape, dim):
    return lax.broadcasted_iota(jnp.int32, shape, dim)


def flip(index, static):
    bit = 1
    while bit <= static:
        if static & bit:
            index = index + bit * (1 - 2 * ((index // bit) % 2))
        bit *= 2
    return index


def newton(coef, y):
    def update(xi, jac, misfit):
        m = jac
        cof = [
            [m[1][1] * m[2][2] - m[1][2] * m[2][1], m[1][2] * m[2][0] - m[1][0] * m[2][2], m[1][0] * m[2][1] - m[1][1] * m[2][0]],
            [m[0][2] * m[2][1] - m[0][1] * m[2][2], m[0][0] * m[2][2] - m[0][2] * m[2][0], m[0][1] * m[2][0] - m[0][0] * m[2][1]],
            [m[0][1] * m[1][2] - m[0][2] * m[1][1], m[0][2] * m[1][0] - m[0][0] * m[1][2], m[0][0] * m[1][1] - m[0][1] * m[1][0]],
        ]
        inv = 1.0 / (m[0][0] * cof[0][0] + m[0][1] * cof[0][1] + m[0][2] * cof[0][2])
        out = []
        for b in range(3):
            step = (cof[0][b] * misfit[0] + cof[1][b] * misfit[1] + cof[2][b] * misfit[2]) * inv
            new = -step if xi is None else xi[b] - step
            out.append(jnp.clip(new, -1.2, 1.2))
        return out

    xi = update(None, [[c[4], c[2], c[1]] for c in coef], [c[0] - t for c, t in zip(coef, y)])
    for _ in range(NEWTON - 1):
        u, v, w = xi
        uv, uw, vw = u * v, u * w, v * w
        jac, misfit = [], []
        for c, t in zip(coef, y):
            du = c[4] + c[6] * v + c[5] * w + c[7] * vw
            dv = c[2] + c[6] * u + c[3] * w + c[7] * uw
            dw = c[1] + c[5] * u + c[3] * v + c[7] * uv
            jac.append([du, dv, dw])
            misfit.append((c[0] - t) + u * du + v * (c[2] + c[3] * w) + w * c[1])
        xi = update(xi, jac, misfit)
    return xi


def lagrange(x):
    diff = [x - t for t in GLL_POINTS]
    pre = [None, diff[0]]
    for n in range(2, 8):
        pre.append(pre[-1] * diff[n - 1])
    suf = [None] * 8
    suf[6] = diff[7]
    for n in range(5, -1, -1):
        suf[n] = suf[n + 1] * diff[n + 1]
    out = []
    for n in range(8):
        value = suf[n] if n == 0 else pre[n] if n == 7 else pre[n] * suf[n]
        out.append(value * WEIGHTS[n])
    return out


def kernel(sizes, group_peers, owners_hbm, targets_hbm, shift_hbm, fields_hbm, out_ref,
           owners_ref, targets_ref, shift_ref, fbuf, table, send, recv, res, ret, lag, idsend, idrecv, ids, slotv, slots,
           osem, tsem, csem, fsem, idsem, slotsem, s0, r0, s1, r1, s2, r2):
    nb, ns, nc = sizes
    n = nb * ns * nc
    blocks = owners_ref.shape[1]
    elems = shift_ref.shape[1]
    pts = out_ref.shape[2]
    groups = n // group_peers
    lanes = idsend.shape[1]
    wide = idsend.shape[0]
    here = [lax.axis_index(a) for a in AXES]
    me = (here[0] * ns + here[1]) * nc + here[2]

    def peer(k):
        if isinstance(k, int):
            return {
                "block": flip(here[0], k // (ns * nc)),
                "seg": flip(here[1], (k // nc) % ns),
                "sub": flip(here[2], k % nc),
            }
        other = jnp.bitwise_xor(me, k)
        return {"block": other // (ns * nc), "seg": (other // nc) % ns, "sub": other % nc}

    def message(k):
        return pl.ds(8 * k if isinstance(k, int) else pl.multiple_of(8 * k, 8), 3 * CAP)

    def for_wait(first, count, ref, sem):
        part = ref.at[pl.ds(8 * first, 3 * CAP * count), :]
        pltpu.make_async_copy(part, part, sem).wait()

    def send_result(k, g):
        part = pl.ds(CAP * k, CAP)
        return pltpu.make_async_remote_copy(
            src_ref=res.at[part], dst_ref=ret.at[part], send_sem=s2, recv_sem=r2.at[g],
            device_id=peer(k), device_id_type=pl.DeviceIdType.MESH)

    get_owners = pltpu.make_async_copy(owners_hbm, owners_ref, osem)
    get_owners.start()
    get_targets = pltpu.make_async_copy(targets_hbm, targets_ref, tsem)
    get_targets.start()
    get_shift = pltpu.make_async_copy(shift_hbm, shift_ref, csem)
    get_shift.start()
    fetch = pltpu.make_async_copy(fields_hbm, fbuf, fsem)
    fetch.start()
    barrier = pltpu.get_barrier_semaphore()
    unrolled = n <= 32

    def for_peers(first, last, body):
        if unrolled:
            for k in reversed(range(first, last)):
                body(k)
        else:
            lax.fori_loop(first, last, lambda k, c: (body(k), c)[1], 0)

    for_peers(1, n, lambda k: pl.semaphore_signal(
        barrier, inc=1, device_id=peer(k), device_id_type=pl.DeviceIdType.MESH))

    shift_bits = elems.bit_length() - 1
    get_owners.wait()
    own = owners_ref[...]
    owner_dev = jnp.right_shift(own, shift_bits)
    hit = (jnp.bitwise_xor(iota((n, blocks), 0), me) == owner_dev).astype(F32)
    earlier = (iota((blocks, blocks), 0) < iota((blocks, blocks), 1)).astype(F32)
    rank = jnp.dot(hit, earlier, preferred_element_type=F32)
    match = [jnp.where(rank == float(c), hit, 0.0) for c in range(CAP)]
    both = jnp.concatenate(match, axis=0)
    get_targets.wait()
    cat = jnp.concatenate([targets_ref[:, a, :] for a in range(3)], axis=1)
    packed = jnp.dot(both, cat, precision=EXACT, preferred_element_type=F32)
    for c in range(CAP):
        part = slice(c * n, (c + 1) * n)
        for a in range(3):
            send[pl.ds(3 * c + a, n, stride=8), :] = packed[part, a * pts:(a + 1) * pts]
            recv[3 * c + a:3 * c + a + 1, :] = packed[c * n:c * n + 1, a * pts:(a + 1) * pts]
    square = (blocks, blocks)
    diag = iota(square, 0) == iota(square, 1)
    own_rows = jnp.broadcast_to(own, square)
    own_col = jnp.sum(jnp.where(diag, own_rows, 0), axis=1, keepdims=True)
    dev_col = jnp.right_shift(own_col, shift_bits)
    dev_row = jnp.right_shift(own_rows, shift_bits)
    same = jnp.where(dev_col == dev_row, 1, 0)
    rank_row = jnp.sum(jnp.where(iota(square, 0) < iota(square, 1), same, 0), axis=0, keepdims=True)
    rank_col = jnp.sum(jnp.where(iota(square, 1) < iota(square, 0), same, 0), axis=1, keepdims=True)
    place = jnp.minimum(CAP * jnp.bitwise_xor(owner_dev, me) + rank_row, CAP * n - 1)
    place = jnp.concatenate([place, jnp.zeros((1, pts - blocks), jnp.int32)], axis=1)
    elem_col = own_col - dev_col * elems
    lane_of = jnp.where(rank_col < CAP, jnp.bitwise_xor(dev_col, me) + n * rank_col, -1)
    for r in range(wide):
        here_lane = iota((blocks, lanes), 1) + lanes * r == lane_of
        row = jnp.sum(jnp.where(here_lane, elem_col, 0), axis=0, keepdims=True)
        idsend[r:r + 1, :] = row
        idrecv[r:r + 1, :] = row
    slotv[...] = place
    slot_copy = pltpu.make_async_copy(slotv, slots, slotsem)
    slot_copy.start()

    pl.semaphore_wait(barrier, n - 1)
    def send_points(k):
        g = k // group_peers
        pltpu.make_async_remote_copy(
            src_ref=idsend, dst_ref=idrecv.at[pl.ds(wide * k, wide), :], send_sem=s0, recv_sem=r0.at[g],
            device_id=peer(k), device_id_type=pl.DeviceIdType.MESH).start()
        pltpu.make_async_remote_copy(
            src_ref=send.at[message(k), :], dst_ref=recv.at[message(k), :], send_sem=s1, recv_sem=r1.at[g],
            device_id=peer(k), device_id_type=pl.DeviceIdType.MESH).start()

    for_peers(1, n, send_points)

    row, col = iota((24, 24), 0), iota((24, 24), 1)
    both_bits = jnp.bitwise_and(row, col) % 8
    odd = (both_bits + both_bits // 2 + both_bits // 4) % 2
    hada = jnp.where(row // 8 == col // 8, (1 - 2 * odd).astype(F32) * 0.125, 0.0)
    get_shift.wait()
    bits = row % 8
    sign = (1 - 2 * ((bits + bits // 2 + bits // 4) % 2)).astype(F32)
    coefs = jnp.dot(hada * sign, shift_ref[...], precision=EXACT, preferred_element_type=F32)
    c_hi = coefs.astype(BF16)
    rest = coefs - c_hi.astype(F32)
    c_mid = rest.astype(BF16)
    c_lo = (rest - c_mid.astype(F32)).astype(BF16)

    fetch.wait()
    low_sub = iota((8, 128), 0) < 4
    low_lane = iota((8, 128), 1) < 64
    keep = low_sub == low_lane

    def split(e, carry):
        parts = []
        for q in range(4):
            x = fbuf[e, :, q * 128:(q + 1) * 128]
            x = jnp.concatenate([x, x], axis=0)
            hi = x.astype(BF16).astype(F32)
            lo = x - hi
            a = jnp.where(low_sub, hi, lo)
            b = pltpu.roll(jnp.where(low_sub, lo, hi), 64, axis=1)
            parts.append(jnp.where(keep, a, b))
        table[e] = jnp.concatenate(parts, axis=0).astype(BF16)
        return carry

    lax.fori_loop(0, elems, split, 0, unroll=4)

    per = group_peers
    count = CAP * per

    def run_group(g, first):
        base = g * per
        got = per - 1 if first else per
        start = base + 1 if first else base
        for_wait(start, got, recv, r1.at[g])

        def gather(a):
            return jnp.concatenate(
                [recv[pl.ds(8 * base + 3 * c + a, per, stride=8), :] for c in range(CAP)], axis=0)

        y = [gather(a) for a in range(3)]
        taken = idrecv.at[pl.ds(wide * start, wide * got), :]
        pltpu.make_async_copy(taken, taken, r0.at[g]).wait()
        id_copy = pltpu.make_async_copy(idrecv.at[pl.ds(wide * base, wide * per), :], ids.at[pl.ds(wide * base, wide * per), :], idsem)
        id_copy.start()
        id_lane = iota((per, lanes), 1) - iota((per, lanes), 0)
        id_cols = []
        for c in range(CAP):
            at = c * n + base
            id_rows = idrecv[pl.ds(wide * base + at // lanes, per, stride=wide), :]
            id_cols.append(jnp.sum(jnp.where(id_lane == at % lanes, id_rows, 0), axis=1, keepdims=True))
        elem = jnp.concatenate(id_cols, axis=0)
        pick = jnp.where(elem == iota((count, elems), 1), 1.0, 0.0).astype(BF16)
        chosen = sum(lax.dot_general(pick, c, NT, preferred_element_type=F32) for c in (c_hi, c_mid, c_lo))
        coef = []
        for a in range(3):
            line = []
            for m in range(8):
                value = chosen[:, 8 * a + m:8 * a + m + 1]
                if m == 4 >> a:
                    value = value + 1.0
                line.append(jnp.broadcast_to(value, (count, pts)))
            coef.append(line)
        xi = newton(coef, y)
        for a in range(3):
            for i, value in enumerate(lagrange(xi[a])):
                lag[a, pl.ds(i, count, stride=8), :] = value
        id_copy.wait()
        for s in range(count):
            c, p = s // per, s % per
            e = ids[wide * (base + p) + (c * n + base) // lanes, (c * n + base) % lanes + p]
            left = table[e]
            lz = lag[2, 8 * s:8 * s + 8, :]
            w = jnp.concatenate([lag[1, 8 * s + j:8 * s + j + 1, :] * lz for j in range(8)], axis=0)
            w_hi = w.astype(BF16)
            w_lo = (w - w_hi.astype(F32)).astype(BF16)
            prod = jnp.dot(
                jnp.concatenate([left, left], axis=1),
                jnp.concatenate([w_hi, w_hi, w_lo, w_lo], axis=0),
                preferred_element_type=F32)
            total = None
            for q in range(4):
                lx = jnp.where(low_sub, lag[0, 8 * s + 2 * q:8 * s + 2 * q + 1, :],
                               lag[0, 8 * s + 2 * q + 1:8 * s + 2 * q + 2, :])
                term = prod[8 * q:8 * q + 8] * lx
                total = term if total is None else total + term
            total = total[0:4] + total[4:8]
            if first and p == 0:
                ret[c] = total
            else:
                res[CAP * (base + p) + c] = total
        for_peers_in = range(1 if first else 0, per)
        for p in for_peers_in:
            send_result(base + p, g).start()

    run_group(0, True)
    if unrolled:
        for g in range(1, groups):
            run_group(g, False)
    else:
        lax.fori_loop(1, groups, lambda g, c: (run_group(g, False), c)[1], 0)

    slot_copy.wait()
    for g in range(groups):
        start, got = (1, per - 1) if g == 0 else (g * per, per)
        back = ret.at[pl.ds(CAP * start, CAP * got)]
        pltpu.make_async_copy(back, back, r2.at[g]).wait()
    for b in range(blocks):
        out_ref[b] = ret[slots[0, b]]
    rest_ids = idrecv.at[pl.ds(wide, wide * (n - 1)), :]
    pltpu.make_async_copy(rest_ids, rest_ids, s0).wait()
    for_wait(1, n - 1, send, s1)
    left = res.at[pl.ds(CAP, CAP * (n - 1))]
    pltpu.make_async_copy(left, left, s2).wait()


def pair_kernel(sizes, owners_hbm, targets_hbm, shift_hbm, fields_hbm, out_ref,
                owners_ref, targets_ref, shift_ref, fbuf, ctab, send, give, via, recv, cbuf, lag, res, ret, slots,
                csem, fsem, sent, r_rel, r_shf, r_fld, r1, r2, r_via, here):
    nb, ns, nc = sizes
    half = nb * ns // 2
    blocks = owners_ref.shape[1]
    elems = shift_ref.shape[2]
    pts = out_ref.shape[2]
    quad = nc * CAP
    rows = 4 * quad
    per = 2 * quad
    b, s, c = [lax.axis_index(a) for a in AXES]
    chip = b * ns + s
    other = 1 - c
    top = nb // 2
    across = b + c * top * (1 - 2 * ((b // top) % 2))

    def peer(j, core):
        return {"block": flip(across, j // ns), "seg": flip(s, j % ns), "sub": core}

    def near(j, core):
        return {"block": flip(b, j // ns), "seg": flip(s, j % ns), "sub": core}

    def unless_here(j, body):
        if j == 0:
            pl.when(c == 1)(body)
        else:
            body()

    def remote(src, dst, send_sem, recv_sem, device):
        return pltpu.make_async_remote_copy(
            src_ref=src, dst_ref=dst, send_sem=send_sem, recv_sem=recv_sem,
            device_id=device, device_id_type=pl.DeviceIdType.MESH)

    def wait_for(part, sem):
        pltpu.make_async_copy(part, part, sem).wait()

    get_owners = pltpu.make_async_copy(owners_hbm, owners_ref, r2)
    get_owners.start()
    get_targets = pltpu.make_async_copy(targets_hbm, targets_ref, sent)
    get_targets.start()
    barrier = pltpu.get_barrier_semaphore()

    def hello(device):
        pl.semaphore_signal(barrier, inc=1, device_id=device, device_id_type=pl.DeviceIdType.MESH)

    sibling = {"block": b, "seg": s, "sub": other}
    partner = {"block": b, "seg": flip(s, 1), "sub": 1}
    first = jnp.logical_and(c == 1, b == 0)
    high = jnp.logical_and(c == 1, b >= top)

    def above(j):
        return b % 2 == 0 if j // ns else s == 0

    def below(j):
        return b % 2 == 1 if j // ns else s == 1

    @pl.when(c == 1)
    def _():
        @pl.when(b < top)
        def _():
            for j in reversed(range(half)):
                hello(peer(j, 1))

        pl.when(b == 0)(lambda: hello(partner))
        hello(sibling)

    @pl.when(c == 0)
    def _():
        for j in reversed(range(1, half)):
            pl.when(above(j))(lambda: hello(near(j, 0)))

    get_shift = pltpu.make_async_copy(shift_hbm, shift_ref.at[0], csem)
    get_shift.start()
    fetch = pltpu.make_async_copy(fields_hbm, fbuf.at[pl.ds(0, elems)], fsem)
    fetch.start()

    pl.when(c == 0)(lambda: pl.semaphore_wait(barrier, 1 + (b % 2) * ns + s))
    pl.when(high)(lambda: pl.semaphore_wait(barrier, half))

    def answer(j, device):
        pl.semaphore_signal(here.at[j], inc=1, device_id=device, device_id_type=pl.DeviceIdType.MESH)

    @pl.when(high)
    def _():
        for j in reversed(range(half)):
            if j % ns:
                pl.when(flip(across, j // ns) != 0)(lambda: answer(j, peer(j, 1)))
            else:
                answer(j, peer(j, 1))

    @pl.when(c == 0)
    def _():
        for j in reversed(range(1, half)):
            pl.when(below(j))(lambda: answer(j, near(j, 0)))

    shift_bits = elems.bit_length() - 1
    square = (blocks, blocks)
    get_owners.wait()
    own = owners_ref[...]
    own_rows = jnp.broadcast_to(own, square)
    diag = iota(square, 0) == iota(square, 1)
    own_col = jnp.sum(jnp.where(diag, own_rows, 0), axis=1, keepdims=True)
    dev_col = jnp.right_shift(own_col, shift_bits)
    dev_row = jnp.right_shift(own_rows, shift_bits)
    same = jnp.where(dev_col == dev_row, 1, 0)
    rank_row = jnp.sum(jnp.where(iota(square, 0) < iota(square, 1), same, 0), axis=0, keepdims=True)
    rank_col = jnp.sum(jnp.where(iota(square, 1) < iota(square, 0), same, 0), axis=1, keepdims=True)
    base_chip = jnp.bitwise_xor(chip, c * half)

    def slot_of(dev, rank):
        rel = jnp.bitwise_xor(jnp.right_shift(dev, 1), base_chip)
        return rel, (rel * nc + jnp.bitwise_and(dev, 1)) * CAP + rank

    rel_col, slot_col = slot_of(dev_col, rank_col)
    turned = jnp.where(rel_col >= half, 1, 0)
    side = jnp.bitwise_xor(jnp.bitwise_xor(jnp.bitwise_and(dev_col, 1), c), turned)
    elem_col = own_col - dev_col * elems + elems * side
    _, slot_row = slot_of(jnp.right_shift(own, shift_bits), rank_row)
    count = 2 * half * quad
    pick = jnp.where(iota((count, blocks), 0) == slot_row, 1.0, 0.0)
    id_rows = jnp.broadcast_to(elem_col.astype(F32), (blocks, pts))
    get_targets.wait()
    cat = jnp.concatenate([targets_ref[:, a, :] for a in range(3)] + [id_rows], axis=1)
    packed = jnp.dot(pick, cat, precision=EXACT, preferred_element_type=F32)
    for a in range(4):
        for j in range(half):
            send[j, pl.ds(a, quad, stride=4), :] = packed[quad * j:quad * (j + 1), a * pts:(a + 1) * pts]
            give[j, pl.ds(a, quad, stride=4), :] = packed[quad * (half + j):quad * (half + j + 1), a * pts:(a + 1) * pts]
    slot_safe = jnp.minimum(jnp.maximum(slot_col, 0), count - 1)
    for k in range(blocks):
        slots[0, k] = slot_safe[k, 0]

    low_sub = iota((8, 128), 0) < 4
    low_lane = iota((8, 128), 1) < 64

    def split(e):
        parts = []
        for r in range(0, fbuf.shape[1], 8):
            x = fbuf[e, r:r + 8, :]
            hi = x.astype(BF16).astype(F32)
            lo = x - hi
            turned = pltpu.roll(jnp.where(low_lane, lo, hi), 64, axis=1)
            parts += [jnp.where(low_lane, hi, turned), jnp.where(low_lane, turned, lo)]
        return jnp.concatenate(parts, axis=0).astype(BF16)

    row, col = iota((24, 24), 0), iota((24, 24), 1)
    both_bits = jnp.bitwise_and(row, col) % 8
    odd = (both_bits + both_bits // 2 + both_bits // 4) % 2
    hada = jnp.where(row // 8 == col // 8, (1 - 2 * odd).astype(F32) * 0.125, 0.0)
    bits = row % 8
    sign = (1 - 2 * ((bits + bits // 2 + bits // 4) % 2)).astype(F32)
    line = iota((24, elems), 0)
    unit = jnp.where(line % 8 == jnp.right_shift(4, line // 8), 1.0, 0.0)

    def spread(side):
        coefs = jnp.dot(hada * sign, shift_ref[side], precision=EXACT, preferred_element_type=F32) + unit
        for e in range(elems):
            ctab[side * elems + e] = jnp.broadcast_to(coefs[:, e:e + 1], (24, pts))

    get_shift.wait()
    fetch.wait()
    pl.when(first)(lambda: pl.semaphore_wait(barrier, 1))
    theirs = send.at[:, pl.ds(rows, rows), :]

    def heard(j):
        pl.semaphore_wait(here.at[j], 1)

    def share():
        remote(fbuf.at[pl.ds(0, elems)], fbuf.at[pl.ds(elems, elems)], sent, r_fld, sibling).start()

    corner = (b % 2) * ns + s

    def request(src, group, device):
        at = pl.multiple_of(2 * rows * group, 2 * rows)
        remote(src, recv.at[pl.ds(at, 2 * rows), :], sent, r1.at[group], device).start()

    @pl.when(c == 0)
    def _():
        remote(give, theirs, sent, r_rel, sibling).start()
        remote(shift_ref.at[0], shift_ref.at[1], sent, r_shf, sibling).start()
        share()
        wait_for(theirs, r_rel)
        for j in reversed(range(1, half)):
            pl.when(above(j))(lambda: heard(j))
            request(send.at[j], corner, near(j, 0))
        recv[pl.ds(pl.multiple_of(2 * rows * corner, 2 * rows), 2 * rows), :] = send[0]

    @pl.when(c == 1)
    def _():
        wait_for(theirs, r_rel)

        @pl.when(b == 0)
        def _():
            for j in reversed(range(1, half, ns)):
                remote(send.at[j], via.at[j // ns], sent, r_via.at[j // ns], partner).start()

        remote(give, theirs, sent, r_rel, sibling).start()
        remote(shift_ref.at[0], shift_ref.at[1], sent, r_shf, sibling).start()

        def pass_on(i):
            wait_for(via.at[i], r_via.at[i])
            request(via.at[i], flip(s, 1), peer(ns * i, 1))

        def own(i):
            request(send.at[ns * i], corner, peer(ns * i, 1))

        columns = list(reversed(range(half // ns)))

        @pl.when(jnp.logical_and(b == 0, s == 0))
        def _():
            for i in columns:
                heard(ns * i)
                own(i)
            share()
            for i in columns:
                pass_on(i)

        @pl.when(jnp.logical_and(b == 0, s == 1))
        def _():
            for i in columns:
                heard(ns * i)
                pass_on(i)
                own(i)
            share()

        @pl.when(b > 0)
        def _():
            for j in reversed(range(half)):
                pl.when(b < top)(lambda: heard(j))
                request(send.at[j], corner, peer(j, 1))
            share()

    spread(0)
    wait_for(shift_ref.at[1], r_shf)
    spread(1)
    wait_for(fbuf.at[pl.ds(elems, elems)], r_fld)

    for g in range(half):
        base = 2 * rows * g
        z, x = g // ns, g % ns
        local = jnp.logical_and(c == 0, corner == g)

        def unless_local(body):
            pl.when(jnp.logical_not(local))(body)

        unless_local(lambda: wait_for(recv.at[pl.ds(base, 2 * rows), :], r1.at[g]))
        y = [recv[pl.ds(base + a, per, stride=4), :] for a in range(3)]
        ids = recv[pl.ds(base + 3, per, stride=4), :].astype(jnp.int32)
        ids = jnp.minimum(jnp.maximum(ids, 0), 2 * elems - 1)
        elem = [ids[k, 0] for k in range(per)]
        for k in range(per):
            for a in range(3):
                cbuf[a, 8 * k:8 * k + 8, :] = ctab[elem[k], 8 * a:8 * a + 8, :]
        coef = [[cbuf[a, pl.ds(m, per, stride=8), :] for m in range(8)] for a in range(3)]
        xi = newton(coef, y)
        for a in range(3):
            for i, value in enumerate(lagrange(xi[a])):
                lag[a, pl.ds(i, per, stride=8), :] = value
        for k in range(per):
            left = split(elem[k])
            lz = lag[2, 8 * k:8 * k + 8, :]
            w = jnp.concatenate([lag[1, 8 * k + i:8 * k + i + 1, :] * lz for i in range(8)], axis=0)
            w_hi = w.astype(BF16)
            w_lo = (w - w_hi.astype(F32)).astype(BF16)
            prod = jnp.dot(
                jnp.concatenate([left, left], axis=1),
                jnp.concatenate([w_hi, w_hi, w_lo, w_lo], axis=0),
                preferred_element_type=F32)
            total = None
            for q in range(4):
                i = 8 * k + 4 * (q // 2) + q % 2
                lx = jnp.where(low_sub, lag[0, i:i + 1, :], lag[0, i + 2:i + 3, :])
                term = prod[8 * q:8 * q + 8] * lx
                total = term if total is None else total + term
            res[per * g + k] = total[0:4] + total[4:8]

        slot = ns * flip(b % 2, z) + flip(s, x)

        def result(part, core, to):
            return remote(res.at[pl.ds(per * g + quad * part, quad)], ret.at[pl.ds(quad * to, quad)],
                          sent, r2, {"block": 2 * (across // 2) + z, "seg": x, "sub": core})

        result(1, other, half + slot).start()
        unless_local(lambda: result(0, c, slot).start())

        @pl.when(local)
        def _():
            ret[0:quad] = res[per * g:per * g + quad]

    pl.when(c == 0)(lambda: wait_for(ret.at[pl.ds(quad, quad * (2 * half - 1))], r2))
    pl.when(c == 1)(lambda: wait_for(ret, r2))
    for k in range(blocks):
        out_ref[k] = ret[slots[0, k]]
    wait_for(give, sent)
    wait_for(shift_ref.at[1], sent)
    wait_for(fbuf.at[pl.ds(elems, elems)], sent)

    def finish(skip):
        wait_for(recv.at[pl.ds(2 * rows * skip, 2 * rows * (half - skip)), :], sent)
        wait_for(ret.at[pl.ds(quad * skip, quad * (2 * half - skip))], sent)

    pl.when(c == 0)(lambda: finish(1))
    pl.when(c == 1)(lambda: finish(0))
    pl.when(first)(lambda: wait_for(via, sent))


def paired(sizes, old_fields, corner_shift, points, owners):
    half = sizes[0] * sizes[1] // 2
    elems, nvar, nodes = old_fields.shape
    blocks, _, pts = points.shape
    quad = sizes[2] * CAP
    rows = 4 * quad
    fields = old_fields.reshape(elems, nvar, nodes // 128, 128).transpose(0, 2, 1, 3)
    fields = fields.reshape(elems, nvar * nodes // 128, 128)
    vmem = pl.BlockSpec(memory_space=pltpu.VMEM)
    hbm = pl.BlockSpec(memory_space=pltpu.HBM)
    result = pltpu.VMEM((2 * half * quad, nvar, pts), F32)
    dma = pltpu.SemaphoreType.DMA
    return pl.pallas_call(
        functools.partial(pair_kernel, sizes),
        out_shape=jax.ShapeDtypeStruct((blocks, nvar, pts), F32),
        in_specs=[hbm] * 4,
        out_specs=vmem,
        scratch_shapes=[
            pltpu.VMEM((1, blocks), jnp.int32),
            pltpu.VMEM((blocks, 3, pts), F32),
            pltpu.VMEM((2, 24, elems), F32),
            pltpu.VMEM((2 * elems, nvar * nodes // 128, 128), F32),
            pltpu.VMEM((2 * elems, 24, pts), F32),
            pltpu.VMEM((half, 2 * rows, pts), F32),
            pltpu.VMEM((half, rows, pts), F32),
            pltpu.VMEM((half // sizes[1], 2 * rows, pts), F32),
            pltpu.VMEM((2 * rows * half, pts), F32),
            pltpu.VMEM((3, 16 * quad, pts), F32),
            pltpu.VMEM((3, 16 * quad, pts), F32),
            result, result,
            pltpu.SMEM((1, blocks), jnp.int32),
            *[dma] * 6, dma((half,)), dma,
            dma((half // sizes[1],)), pltpu.SemaphoreType.REGULAR((half,)),
        ],
        compiler_params=pltpu.CompilerParams(
            collective_id=0, has_side_effects=True, vmem_limit_bytes=24 * 1024 * 1024),
    )(*[pltpu.with_memory_space_constraint(x, pltpu.HBM) for x in (owners.reshape(1, blocks), points, corner_shift, fields)])


def shards(sizes, old_fields, corner_shift, targets, owners):
    n = sizes[0] * sizes[1] * sizes[2]
    elems, nvar, nodes = old_fields.shape
    blocks = owners.shape[0]
    pts = targets.shape[1] // blocks
    assert n & (n - 1) == 0 and elems & (elems - 1) == 0 and nvar == 4 and nodes == 512
    group_peers = min(GROUP_PEERS, n)
    groups = n // group_peers
    wide = (CAP * n + 127) // 128
    points = targets.reshape(3, blocks, pts).transpose(1, 0, 2)
    if sizes[0] == 4 and sizes[1] == 2 and sizes[2] == 2:
        out = paired(sizes, old_fields, corner_shift, points, owners)
        return out.transpose(1, 0, 2).reshape(nvar, blocks * pts)
    vmem = pl.BlockSpec(memory_space=pltpu.VMEM)
    hbm = pl.BlockSpec(memory_space=pltpu.HBM)
    message = pltpu.VMEM((8 * n, pts), F32)
    result = pltpu.VMEM((CAP * n, nvar, pts), F32)
    out = pl.pallas_call(
        functools.partial(kernel, sizes, group_peers),
        out_shape=jax.ShapeDtypeStruct((blocks, nvar, pts), F32),
        in_specs=[hbm] * 4,
        out_specs=vmem,
        scratch_shapes=[
            pltpu.VMEM((1, blocks), jnp.int32),
            pltpu.VMEM((blocks, 3, pts), F32),
            pltpu.VMEM((24, elems), F32),
            pltpu.VMEM((elems, nvar, nodes), F32),
            pltpu.VMEM((elems, 32, 128), BF16),
            message, message, result, result,
            pltpu.VMEM((3, 8 * CAP * group_peers, pts), F32),
            pltpu.VMEM((wide, 128), jnp.int32),
            pltpu.VMEM((wide * n, 128), jnp.int32),
            pltpu.SMEM((wide * n, 128), jnp.int32),
            pltpu.VMEM((1, pts), jnp.int32),
            pltpu.SMEM((1, pts), jnp.int32),
            *[pltpu.SemaphoreType.DMA] * 6,
            pltpu.SemaphoreType.DMA, pltpu.SemaphoreType.DMA((groups,)),
            pltpu.SemaphoreType.DMA, pltpu.SemaphoreType.DMA((groups,)),
            pltpu.SemaphoreType.DMA, pltpu.SemaphoreType.DMA((groups,)),
        ],
        compiler_params=pltpu.CompilerParams(
            collective_id=0, has_side_effects=True, vmem_limit_bytes=16 * 1024 * 1024),
    )(*[pltpu.with_memory_space_constraint(x, pltpu.HBM) for x in (owners.reshape(1, blocks), points, corner_shift, old_fields)])
    return out.transpose(1, 0, 2).reshape(nvar, blocks * pts)


def solution(mesh):
    sizes = tuple(mesh.shape[a] for a in AXES)
    in_specs = (
        P(("groups", "block", "seg", "sub"), None, None),
        P(None, ("groups", "block", "seg", "sub")),
        P(None, ("groups", "block", "seg", "sub")),
        P(("groups", "block", "seg", "sub")),
    )
    out_specs = P(None, ("groups", "block", "seg", "sub"))
    return jax.shard_map(functools.partial(shards, sizes), mesh=mesh, in_specs=in_specs,
                         out_specs=out_specs, check_vma=False)
```

```python
import functools

import jax
import jax.numpy as jnp
from jax import lax
from jax.experimental import pallas as pl
from jax.experimental.pallas import tpu as pltpu
from jax.sharding import PartitionSpec as P

NEWTON = 3
CAP = 2
GROUP_PEERS = 4
AXES = ("block", "seg", "sub")

GLL_POINTS = (
    -1.0,
    -0.8717401485096066,
    -0.5917001814331423,
    -0.2092992179024789,
    0.2092992179024789,
    0.5917001814331423,
    0.8717401485096066,
    1.0,
)
WEIGHTS = []
for _n in range(8):
    _w = 1.0
    for _m in range(8):
        if _m != _n:
            _w /= GLL_POINTS[_n] - GLL_POINTS[_m]
    WEIGHTS.append(_w)

F32 = jnp.float32
BF16 = jnp.bfloat16
EXACT = lax.Precision.HIGHEST
NT = (((1,), (1,)), ((), ()))


def iota(shape, dim):
    return lax.broadcasted_iota(jnp.int32, shape, dim)


def flip(index, static):
    bit = 1
    while bit <= static:
        if static & bit:
            index = index + bit * (1 - 2 * ((index // bit) % 2))
        bit *= 2
    return index


def newton(coef, y):
    def update(xi, jac, misfit):
        m = jac
        cof = [
            [m[1][1] * m[2][2] - m[1][2] * m[2][1], m[1][2] * m[2][0] - m[1][0] * m[2][2], m[1][0] * m[2][1] - m[1][1] * m[2][0]],
            [m[0][2] * m[2][1] - m[0][1] * m[2][2], m[0][0] * m[2][2] - m[0][2] * m[2][0], m[0][1] * m[2][0] - m[0][0] * m[2][1]],
            [m[0][1] * m[1][2] - m[0][2] * m[1][1], m[0][2] * m[1][0] - m[0][0] * m[1][2], m[0][0] * m[1][1] - m[0][1] * m[1][0]],
        ]
        inv = 1.0 / (m[0][0] * cof[0][0] + m[0][1] * cof[0][1] + m[0][2] * cof[0][2])
        out = []
        for b in range(3):
            step = (cof[0][b] * misfit[0] + cof[1][b] * misfit[1] + cof[2][b] * misfit[2]) * inv
            new = -step if xi is None else xi[b] - step
            out.append(jnp.clip(new, -1.2, 1.2))
        return out

    xi = update(None, [[c[4], c[2], c[1]] for c in coef], [c[0] - t for c, t in zip(coef, y)])
    for _ in range(NEWTON - 1):
        u, v, w = xi
        uv, uw, vw = u * v, u * w, v * w
        jac, misfit = [], []
        for c, t in zip(coef, y):
            du = c[4] + c[6] * v + c[5] * w + c[7] * vw
            dv = c[2] + c[6] * u + c[3] * w + c[7] * uw
            dw = c[1] + c[5] * u + c[3] * v + c[7] * uv
            jac.append([du, dv, dw])
            misfit.append((c[0] - t) + u * du + v * (c[2] + c[3] * w) + w * c[1])
        xi = update(xi, jac, misfit)
    return xi


def lagrange(x):
    diff = [x - t for t in GLL_POINTS]
    pre = [None, diff[0]]
    for n in range(2, 8):
        pre.append(pre[-1] * diff[n - 1])
    suf = [None] * 8
    suf[6] = diff[7]
    for n in range(5, -1, -1):
        suf[n] = suf[n + 1] * diff[n + 1]
    out = []
    for n in range(8):
        value = suf[n] if n == 0 else pre[n] if n == 7 else pre[n] * suf[n]
        out.append(value * WEIGHTS[n])
    return out


def kernel(sizes, group_peers, owners_hbm, targets_hbm, shift_hbm, fields_hbm, out_ref,
           owners_ref, targets_ref, shift_ref, fbuf, table, send, recv, res, ret, lag, idsend, idrecv, ids, slotv, slots,
           osem, tsem, csem, fsem, idsem, slotsem, s0, r0, s1, r1, s2, r2):
    nb, ns, nc = sizes
    n = nb * ns * nc
    blocks = owners_ref.shape[1]
    elems = shift_ref.shape[1]
    pts = out_ref.shape[2]
    groups = n // group_peers
    lanes = idsend.shape[1]
    wide = idsend.shape[0]
    here = [lax.axis_index(a) for a in AXES]
    me = (here[0] * ns + here[1]) * nc + here[2]

    def peer(k):
        if isinstance(k, int):
            return {
                "block": flip(here[0], k // (ns * nc)),
                "seg": flip(here[1], (k // nc) % ns),
                "sub": flip(here[2], k % nc),
            }
        other = jnp.bitwise_xor(me, k)
        return {"block": other // (ns * nc), "seg": (other // nc) % ns, "sub": other % nc}

    def message(k):
        return pl.ds(8 * k if isinstance(k, int) else pl.multiple_of(8 * k, 8), 3 * CAP)

    def for_wait(first, count, ref, sem):
        part = ref.at[pl.ds(8 * first, 3 * CAP * count), :]
        pltpu.make_async_copy(part, part, sem).wait()

    def send_result(k, g):
        part = pl.ds(CAP * k, CAP)
        return pltpu.make_async_remote_copy(
            src_ref=res.at[part], dst_ref=ret.at[part], send_sem=s2, recv_sem=r2.at[g],
            device_id=peer(k), device_id_type=pl.DeviceIdType.MESH)

    get_owners = pltpu.make_async_copy(owners_hbm, owners_ref, osem)
    get_owners.start()
    get_targets = pltpu.make_async_copy(targets_hbm, targets_ref, tsem)
    get_targets.start()
    get_shift = pltpu.make_async_copy(shift_hbm, shift_ref, csem)
    get_shift.start()
    fetch = pltpu.make_async_copy(fields_hbm, fbuf, fsem)
    fetch.start()
    barrier = pltpu.get_barrier_semaphore()
    unrolled = n <= 32

    def for_peers(first, last, body):
        if unrolled:
            for k in reversed(range(first, last)):
                body(k)
        else:
            lax.fori_loop(first, last, lambda k, c: (body(k), c)[1], 0)

    for_peers(1, n, lambda k: pl.semaphore_signal(
        barrier, inc=1, device_id=peer(k), device_id_type=pl.DeviceIdType.MESH))

    shift_bits = elems.bit_length() - 1
    get_owners.wait()
    own = owners_ref[...]
    owner_dev = jnp.right_shift(own, shift_bits)
    hit = (jnp.bitwise_xor(iota((n, blocks), 0), me) == owner_dev).astype(F32)
    earlier = (iota((blocks, blocks), 0) < iota((blocks, blocks), 1)).astype(F32)
    rank = jnp.dot(hit, earlier, preferred_element_type=F32)
    match = [jnp.where(rank == float(c), hit, 0.0) for c in range(CAP)]
    both = jnp.concatenate(match, axis=0)
    get_targets.wait()
    cat = jnp.concatenate([targets_ref[:, a, :] for a in range(3)], axis=1)
    packed = jnp.dot(both, cat, precision=EXACT, preferred_element_type=F32)
    for c in range(CAP):
        part = slice(c * n, (c + 1) * n)
        for a in range(3):
            send[pl.ds(3 * c + a, n, stride=8), :] = packed[part, a * pts:(a + 1) * pts]
            recv[3 * c + a:3 * c + a + 1, :] = packed[c * n:c * n + 1, a * pts:(a + 1) * pts]
    square = (blocks, blocks)
    diag = iota(square, 0) == iota(square, 1)
    own_rows = jnp.broadcast_to(own, square)
    own_col = jnp.sum(jnp.where(diag, own_rows, 0), axis=1, keepdims=True)
    dev_col = jnp.right_shift(own_col, shift_bits)
    dev_row = jnp.right_shift(own_rows, shift_bits)
    same = jnp.where(dev_col == dev_row, 1, 0)
    rank_row = jnp.sum(jnp.where(iota(square, 0) < iota(square, 1), same, 0), axis=0, keepdims=True)
    rank_col = jnp.sum(jnp.where(iota(square, 1) < iota(square, 0), same, 0), axis=1, keepdims=True)
    place = jnp.minimum(CAP * jnp.bitwise_xor(owner_dev, me) + rank_row, CAP * n - 1)
    place = jnp.concatenate([place, jnp.zeros((1, pts - blocks), jnp.int32)], axis=1)
    elem_col = own_col - dev_col * elems
    lane_of = jnp.where(rank_col < CAP, jnp.bitwise_xor(dev_col, me) + n * rank_col, -1)
    for r in range(wide):
        here_lane = iota((blocks, lanes), 1) + lanes * r == lane_of
        row = jnp.sum(jnp.where(here_lane, elem_col, 0), axis=0, keepdims=True)
        idsend[r:r + 1, :] = row
        idrecv[r:r + 1, :] = row
    slotv[...] = place
    slot_copy = pltpu.make_async_copy(slotv, slots, slotsem)
    slot_copy.start()

    pl.semaphore_wait(barrier, n - 1)
    def send_points(k):
        g = k // group_peers
        pltpu.make_async_remote_copy(
            src_ref=idsend, dst_ref=idrecv.at[pl.ds(wide * k, wide), :], send_sem=s0, recv_sem=r0.at[g],
            device_id=peer(k), device_id_type=pl.DeviceIdType.MESH).start()
        pltpu.make_async_remote_copy(
            src_ref=send.at[message(k), :], dst_ref=recv.at[message(k), :], send_sem=s1, recv_sem=r1.at[g],
            device_id=peer(k), device_id_type=pl.DeviceIdType.MESH).start()

    for_peers(1, n, send_points)

    row, col = iota((24, 24), 0), iota((24, 24), 1)
    both_bits = jnp.bitwise_and(row, col) % 8
    odd = (both_bits + both_bits // 2 + both_bits // 4) % 2
    hada = jnp.where(row // 8 == col // 8, (1 - 2 * odd).astype(F32) * 0.125, 0.0)
    get_shift.wait()
    bits = row % 8
    sign = (1 - 2 * ((bits + bits // 2 + bits // 4) % 2)).astype(F32)
    coefs = jnp.dot(hada * sign, shift_ref[...], precision=EXACT, preferred_element_type=F32)
    c_hi = coefs.astype(BF16)
    rest = coefs - c_hi.astype(F32)
    c_mid = rest.astype(BF16)
    c_lo = (rest - c_mid.astype(F32)).astype(BF16)

    fetch.wait()
    low_sub = iota((8, 128), 0) < 4
    low_lane = iota((8, 128), 1) < 64
    keep = low_sub == low_lane

    def split(e, carry):
        parts = []
        for q in range(4):
            x = fbuf[e, :, q * 128:(q + 1) * 128]
            x = jnp.concatenate([x, x], axis=0)
            hi = x.astype(BF16).astype(F32)
            lo = x - hi
            a = jnp.where(low_sub, hi, lo)
            b = pltpu.roll(jnp.where(low_sub, lo, hi), 64, axis=1)
            parts.append(jnp.where(keep, a, b))
        table[e] = jnp.concatenate(parts, axis=0).astype(BF16)
        return carry

    lax.fori_loop(0, elems, split, 0, unroll=4)

    per = group_peers
    count = CAP * per

    def run_group(g, first):
        base = g * per
        got = per - 1 if first else per
        start = base + 1 if first else base
        for_wait(start, got, recv, r1.at[g])

        def gather(a):
            return jnp.concatenate(
                [recv[pl.ds(8 * base + 3 * c + a, per, stride=8), :] for c in range(CAP)], axis=0)

        y = [gather(a) for a in range(3)]
        taken = idrecv.at[pl.ds(wide * start, wide * got), :]
        pltpu.make_async_copy(taken, taken, r0.at[g]).wait()
        id_copy = pltpu.make_async_copy(idrecv.at[pl.ds(wide * base, wide * per), :], ids.at[pl.ds(wide * base, wide * per), :], idsem)
        id_copy.start()
        id_lane = iota((per, lanes), 1) - iota((per, lanes), 0)
        id_cols = []
        for c in range(CAP):
            at = c * n + base
            id_rows = idrecv[pl.ds(wide * base + at // lanes, per, stride=wide), :]
            id_cols.append(jnp.sum(jnp.where(id_lane == at % lanes, id_rows, 0), axis=1, keepdims=True))
        elem = jnp.concatenate(id_cols, axis=0)
        pick = jnp.where(elem == iota((count, elems), 1), 1.0, 0.0).astype(BF16)
        chosen = sum(lax.dot_general(pick, c, NT, preferred_element_type=F32) for c in (c_hi, c_mid, c_lo))
        coef = []
        for a in range(3):
            line = []
            for m in range(8):
                value = chosen[:, 8 * a + m:8 * a + m + 1]
                if m == 4 >> a:
                    value = value + 1.0
                line.append(jnp.broadcast_to(value, (count, pts)))
            coef.append(line)
        xi = newton(coef, y)
        for a in range(3):
            for i, value in enumerate(lagrange(xi[a])):
                lag[a, pl.ds(i, count, stride=8), :] = value
        id_copy.wait()
        for s in range(count):
            c, p = s // per, s % per
            e = ids[wide * (base + p) + (c * n + base) // lanes, (c * n + base) % lanes + p]
            left = table[e]
            lz = lag[2, 8 * s:8 * s + 8, :]
            w = jnp.concatenate([lag[1, 8 * s + j:8 * s + j + 1, :] * lz for j in range(8)], axis=0)
            w_hi = w.astype(BF16)
            w_lo = (w - w_hi.astype(F32)).astype(BF16)
            prod = jnp.dot(
                jnp.concatenate([left, left], axis=1),
                jnp.concatenate([w_hi, w_hi, w_lo, w_lo], axis=0),
                preferred_element_type=F32)
            total = None
            for q in range(4):
                lx = jnp.where(low_sub, lag[0, 8 * s + 2 * q:8 * s + 2 * q + 1, :],
                               lag[0, 8 * s + 2 * q + 1:8 * s + 2 * q + 2, :])
                term = prod[8 * q:8 * q + 8] * lx
                total = term if total is None else total + term
            total = total[0:4] + total[4:8]
            if first and p == 0:
                ret[c] = total
            else:
                res[CAP * (base + p) + c] = total
        for_peers_in = range(1 if first else 0, per)
        for p in for_peers_in:
            send_result(base + p, g).start()

    run_group(0, True)
    if unrolled:
        for g in range(1, groups):
            run_group(g, False)
    else:
        lax.fori_loop(1, groups, lambda g, c: (run_group(g, False), c)[1], 0)

    slot_copy.wait()
    for g in range(groups):
        start, got = (1, per - 1) if g == 0 else (g * per, per)
        back = ret.at[pl.ds(CAP * start, CAP * got)]
        pltpu.make_async_copy(back, back, r2.at[g]).wait()
    for b in range(blocks):
        out_ref[b] = ret[slots[0, b]]
    rest_ids = idrecv.at[pl.ds(wide, wide * (n - 1)), :]
    pltpu.make_async_copy(rest_ids, rest_ids, s0).wait()
    for_wait(1, n - 1, send, s1)
    left = res.at[pl.ds(CAP, CAP * (n - 1))]
    pltpu.make_async_copy(left, left, s2).wait()


def pair_kernel(sizes, owners_hbm, targets_hbm, shift_hbm, fields_hbm, out_ref,
                owners_ref, targets_ref, shift_ref, fbuf, ctab, send, give, via, recv, cbuf, lag, res, ret, slots,
                csem, fsem, sent, r_rel, r_fld, r1, r2, r_via, here):
    nb, ns, nc = sizes
    half = nb * ns // 2
    blocks = owners_ref.shape[1]
    elems = shift_ref.shape[1]
    pts = out_ref.shape[2]
    quad = nc * CAP
    rows = 4 * quad
    per = 2 * quad
    b, s, c = [lax.axis_index(a) for a in AXES]
    chip = b * ns + s
    other = 1 - c
    top = nb // 2
    across = b + c * top * (1 - 2 * ((b // top) % 2))

    def peer(j, core):
        return {"block": flip(across, j // ns), "seg": flip(s, j % ns), "sub": core}

    def near(j, core):
        return {"block": flip(b, j // ns), "seg": flip(s, j % ns), "sub": core}

    def unless_here(j, body):
        if j == 0:
            pl.when(c == 1)(body)
        else:
            body()

    def remote(src, dst, send_sem, recv_sem, device):
        return pltpu.make_async_remote_copy(
            src_ref=src, dst_ref=dst, send_sem=send_sem, recv_sem=recv_sem,
            device_id=device, device_id_type=pl.DeviceIdType.MESH)

    def wait_for(part, sem):
        pltpu.make_async_copy(part, part, sem).wait()

    get_owners = pltpu.make_async_copy(owners_hbm, owners_ref, r2)
    get_owners.start()
    get_targets = pltpu.make_async_copy(targets_hbm, targets_ref, sent)
    get_targets.start()
    barrier = pltpu.get_barrier_semaphore()

    def hello(device):
        pl.semaphore_signal(barrier, inc=1, device_id=device, device_id_type=pl.DeviceIdType.MESH)

    sibling = {"block": b, "seg": s, "sub": other}
    partner = {"block": b, "seg": flip(s, 1), "sub": 1}
    first = jnp.logical_and(c == 1, b == 0)
    high = jnp.logical_and(c == 1, b >= top)

    def above(j):
        return b % 2 == 0 if j // ns else s == 0

    def below(j):
        return b % 2 == 1 if j // ns else s == 1

    @pl.when(c == 1)
    def _():
        @pl.when(b < top)
        def _():
            for j in reversed(range(half)):
                hello(peer(j, 1))

        pl.when(b == 0)(lambda: hello(partner))
        hello(sibling)

    @pl.when(c == 0)
    def _():
        for j in reversed(range(1, half)):
            pl.when(above(j))(lambda: hello(near(j, 0)))

    get_shift = pltpu.make_async_copy(shift_hbm, shift_ref, csem)
    get_shift.start()
    fetch = pltpu.make_async_copy(fields_hbm, fbuf.at[pl.ds(0, elems)], fsem)
    fetch.start()

    pl.when(c == 0)(lambda: pl.semaphore_wait(barrier, 1 + (b % 2) * ns + s))
    pl.when(high)(lambda: pl.semaphore_wait(barrier, half))

    def answer(device):
        pl.semaphore_signal(here, inc=1, device_id=device, device_id_type=pl.DeviceIdType.MESH)

    @pl.when(high)
    def _():
        for j in reversed(range(half)):
            if j % ns:
                pl.when(flip(across, j // ns) != 0)(lambda: answer(peer(j, 1)))
            else:
                answer(peer(j, 1))

    @pl.when(c == 0)
    def _():
        for j in reversed(range(1, half)):
            pl.when(below(j))(lambda: answer(near(j, 0)))

    shift_bits = elems.bit_length() - 1
    square = (blocks, blocks)
    get_owners.wait()
    own = owners_ref[...]
    own_rows = jnp.broadcast_to(own, square)
    diag = iota(square, 0) == iota(square, 1)
    own_col = jnp.sum(jnp.where(diag, own_rows, 0), axis=1, keepdims=True)
    dev_col = jnp.right_shift(own_col, shift_bits)
    dev_row = jnp.right_shift(own_rows, shift_bits)
    same = jnp.where(dev_col == dev_row, 1, 0)
    rank_row = jnp.sum(jnp.where(iota(square, 0) < iota(square, 1), same, 0), axis=0, keepdims=True)
    rank_col = jnp.sum(jnp.where(iota(square, 1) < iota(square, 0), same, 0), axis=1, keepdims=True)
    base_chip = jnp.bitwise_xor(chip, c * half)

    def slot_of(dev, rank):
        rel = jnp.bitwise_xor(jnp.right_shift(dev, 1), base_chip)
        return rel, (rel * nc + jnp.bitwise_and(dev, 1)) * CAP + rank

    rel_col, slot_col = slot_of(dev_col, rank_col)
    turned = jnp.where(rel_col >= half, 1, 0)
    side = jnp.bitwise_xor(jnp.bitwise_xor(jnp.bitwise_and(dev_col, 1), c), turned)
    elem_col = own_col - dev_col * elems + elems * side
    _, slot_row = slot_of(jnp.right_shift(own, shift_bits), rank_row)
    count = 2 * half * quad
    pick = jnp.where(iota((count, blocks), 0) == slot_row, 1.0, 0.0)
    id_rows = jnp.broadcast_to(elem_col.astype(F32), (blocks, pts))
    get_targets.wait()
    cat = jnp.concatenate([targets_ref[:, a, :] for a in range(3)] + [id_rows], axis=1)
    packed = jnp.dot(pick, cat, precision=EXACT, preferred_element_type=F32)
    for a in range(4):
        for j in range(half):
            send[j, pl.ds(a, quad, stride=4), :] = packed[quad * j:quad * (j + 1), a * pts:(a + 1) * pts]
            give[j, pl.ds(a, quad, stride=4), :] = packed[quad * (half + j):quad * (half + j + 1), a * pts:(a + 1) * pts]
    slot_safe = jnp.minimum(jnp.maximum(slot_col, 0), count - 1)
    for k in range(blocks):
        slots[0, k] = slot_safe[k, 0]

    low_sub = iota((8, 128), 0) < 4
    low_lane = iota((8, 128), 1) < 64

    def split(e):
        high_part, low_part = [], []
        for r in range(0, fbuf.shape[1], 8):
            x = fbuf[e, r:r + 8, :]
            turned = pltpu.roll(x, 64, axis=1)
            for part in (jnp.where(low_lane, x, turned), jnp.where(low_lane, turned, x)):
                hi = part.astype(BF16).astype(F32)
                high_part.append(hi)
                low_part.append(part - hi)
        return jnp.concatenate(high_part + low_part, axis=0).astype(BF16)

    row, col = iota((24, 24), 0), iota((24, 24), 1)
    both_bits = jnp.bitwise_and(row, col) % 8
    odd = (both_bits + both_bits // 2 + both_bits // 4) % 2
    hada = jnp.where(row // 8 == col // 8, (1 - 2 * odd).astype(F32) * 0.125, 0.0)
    bits = row % 8
    sign = (1 - 2 * ((bits + bits // 2 + bits // 4) % 2)).astype(F32)
    line = iota((24, elems), 0)
    unit = jnp.where(line % 8 == jnp.right_shift(4, line // 8), 1.0, 0.0)

    def spread(side, shift):
        coefs = jnp.dot(hada * sign, shift, precision=EXACT, preferred_element_type=F32) + unit
        for e in range(elems):
            ctab[side * elems + e] = jnp.broadcast_to(coefs[:, e:e + 1], (24, pts))

    get_shift.wait()
    give[half, :, :elems] = shift_ref[:rows]
    give[half + 1, :24 - rows, :elems] = shift_ref[rows:]
    fetch.wait()
    pl.when(first)(lambda: pl.semaphore_wait(barrier, 1))
    theirs = send.at[:, pl.ds(rows, rows), :]

    def heard(count):
        pl.semaphore_wait(here, count)

    def share():
        remote(fbuf.at[pl.ds(0, elems)], fbuf.at[pl.ds(elems, elems)], sent, r_fld, sibling).start()

    corner = (b % 2) * ns + s

    def request(src, group, device):
        at = pl.multiple_of(2 * rows * group, 2 * rows)
        remote(src, recv.at[pl.ds(at, 2 * rows), :], sent, r1.at[group], device).start()

    @pl.when(c == 0)
    def _():
        remote(give, theirs, sent, r_rel, sibling).start()
        share()
        wait_for(theirs, r_rel)
        pl.when(corner < half - 1)(lambda: heard(half - 1 - corner))
        for j in reversed(range(1, half)):
            request(send.at[j], corner, near(j, 0))
        recv[pl.ds(pl.multiple_of(2 * rows * corner, 2 * rows), 2 * rows), :] = send[0]

    @pl.when(c == 1)
    def _():
        wait_for(theirs, r_rel)

        @pl.when(b == 0)
        def _():
            for j in reversed(range(1, half, ns)):
                remote(send.at[j], via.at[j // ns], sent, r_via, partner).start()

        remote(give, theirs, sent, r_rel, sibling).start()

        def pass_on(i):
            request(via.at[i], flip(s, 1), peer(ns * i, 1))

        def own(i):
            request(send.at[ns * i], corner, peer(ns * i, 1))

        columns = list(reversed(range(half // ns)))

        @pl.when(jnp.logical_and(b == 0, s == 0))
        def _():
            heard(half // ns)
            for i in columns:
                own(i)
            share()
            wait_for(via, r_via)
            for i in columns:
                pass_on(i)

        @pl.when(jnp.logical_and(b == 0, s == 1))
        def _():
            wait_for(via, r_via)
            heard(half // ns)
            for i in columns:
                pass_on(i)
                own(i)
            share()

        @pl.when(b > 0)
        def _():
            pl.when(b < top)(lambda: heard(half))
            for j in reversed(range(half)):
                request(send.at[j], corner, peer(j, 1))
            share()

    spread(0, shift_ref[...])
    spread(1, jnp.concatenate([send[half, rows:2 * rows, :elems], send[half + 1, rows:2 * rows, :elems]], axis=0)[:24])
    wait_for(fbuf.at[pl.ds(elems, elems)], r_fld)

    for g in range(half):
        base = 2 * rows * g
        z, x = g // ns, g % ns
        local = jnp.logical_and(c == 0, corner == g)

        def unless_local(body):
            pl.when(jnp.logical_not(local))(body)

        unless_local(lambda: wait_for(recv.at[pl.ds(base, 2 * rows), :], r1.at[g]))
        y = [recv[pl.ds(base + a, per, stride=4), :] for a in range(3)]
        ids = recv[pl.ds(base + 3, per, stride=4), :].astype(jnp.int32)
        ids = jnp.minimum(jnp.maximum(ids, 0), 2 * elems - 1)
        elem = [ids[k, 0] for k in range(per)]
        for k in range(per):
            for a in range(3):
                cbuf[a, 8 * k:8 * k + 8, :] = ctab[elem[k], 8 * a:8 * a + 8, :]
        coef = [[cbuf[a, pl.ds(m, per, stride=8), :] for m in range(8)] for a in range(3)]
        xi = newton(coef, y)
        for a in range(3):
            for i, value in enumerate(lagrange(xi[a])):
                lag[a, pl.ds(i, per, stride=8), :] = value
        for k in range(per):
            left = split(elem[k])
            lz = lag[2, 8 * k:8 * k + 8, :]
            w = jnp.concatenate([lag[1, 8 * k + i:8 * k + i + 1, :] * lz for i in range(8)], axis=0)
            w_hi = w.astype(BF16)
            w_lo = (w - w_hi.astype(F32)).astype(BF16)
            prod = jnp.dot(left, jnp.concatenate([w_hi, w_lo], axis=0), preferred_element_type=F32)
            prod = prod[:32] + prod[32:]
            total = None
            for q in range(4):
                i = 8 * k + 4 * (q // 2) + q % 2
                lx = jnp.where(low_sub, lag[0, i:i + 1, :], lag[0, i + 2:i + 3, :])
                term = prod[8 * q:8 * q + 8] * lx
                total = term if total is None else total + term
            res[per * g + k] = total[0:4] + total[4:8]

        slot = ns * flip(b % 2, z) + flip(s, x)

        def result(part, core, to):
            return remote(res.at[pl.ds(per * g + quad * part, quad)], ret.at[pl.ds(quad * to, quad)],
                          sent, r2, {"block": 2 * (across // 2) + z, "seg": x, "sub": core})

        result(1, other, half + slot).start()
        unless_local(lambda: result(0, c, slot).start())

        @pl.when(local)
        def _():
            ret[0:quad] = res[per * g:per * g + quad]

    pl.when(c == 0)(lambda: wait_for(ret.at[pl.ds(quad, quad * (2 * half - 1))], r2))
    pl.when(c == 1)(lambda: wait_for(ret, r2))
    for k in range(blocks):
        out_ref[k] = ret[slots[0, k]]
    wait_for(give, sent)
    wait_for(fbuf.at[pl.ds(elems, elems)], sent)

    def finish(skip):
        wait_for(recv.at[pl.ds(2 * rows * skip, 2 * rows * (half - skip)), :], sent)
        wait_for(ret.at[pl.ds(quad * skip, quad * (2 * half - skip))], sent)

    pl.when(c == 0)(lambda: finish(1))
    pl.when(c == 1)(lambda: finish(0))
    pl.when(first)(lambda: wait_for(via, sent))


def paired(sizes, old_fields, corner_shift, points, owners):
    half = sizes[0] * sizes[1] // 2
    elems, nvar, nodes = old_fields.shape
    blocks, _, pts = points.shape
    quad = sizes[2] * CAP
    rows = 4 * quad
    fields = old_fields.reshape(elems, nvar, nodes // 128, 128).transpose(0, 2, 1, 3)
    fields = fields.reshape(elems, nvar * nodes // 128, 128)
    vmem = pl.BlockSpec(memory_space=pltpu.VMEM)
    hbm = pl.BlockSpec(memory_space=pltpu.HBM)
    result = pltpu.VMEM((2 * half * quad, nvar, pts), F32)
    dma = pltpu.SemaphoreType.DMA
    return pl.pallas_call(
        functools.partial(pair_kernel, sizes),
        out_shape=jax.ShapeDtypeStruct((blocks, nvar, pts), F32),
        in_specs=[hbm] * 4,
        out_specs=vmem,
        scratch_shapes=[
            pltpu.VMEM((1, blocks), jnp.int32),
            pltpu.VMEM((blocks, 3, pts), F32),
            pltpu.VMEM((24, elems), F32),
            pltpu.VMEM((2 * elems, nvar * nodes // 128, 128), F32),
            pltpu.VMEM((2 * elems, 24, pts), F32),
            pltpu.VMEM((half + 2, 2 * rows, pts), F32),
            pltpu.VMEM((half + 2, rows, pts), F32),
            pltpu.VMEM((half // sizes[1], 2 * rows, pts), F32),
            pltpu.VMEM((2 * rows * half, pts), F32),
            pltpu.VMEM((3, 16 * quad, pts), F32),
            pltpu.VMEM((3, 16 * quad, pts), F32),
            result, result,
            pltpu.SMEM((1, blocks), jnp.int32),
            *[dma] * 5, dma((half,)), dma,
            dma, pltpu.SemaphoreType.REGULAR,
        ],
        compiler_params=pltpu.CompilerParams(
            collective_id=0, has_side_effects=True, vmem_limit_bytes=24 * 1024 * 1024),
    )(*[pltpu.with_memory_space_constraint(x, pltpu.HBM) for x in (owners.reshape(1, blocks), points, corner_shift, fields)])


def shards(sizes, old_fields, corner_shift, targets, owners):
    n = sizes[0] * sizes[1] * sizes[2]
    elems, nvar, nodes = old_fields.shape
    blocks = owners.shape[0]
    pts = targets.shape[1] // blocks
    assert n & (n - 1) == 0 and elems & (elems - 1) == 0 and nvar == 4 and nodes == 512
    group_peers = min(GROUP_PEERS, n)
    groups = n // group_peers
    wide = (CAP * n + 127) // 128
    points = targets.reshape(3, blocks, pts).transpose(1, 0, 2)
    if sizes[0] == 4 and sizes[1] == 2 and sizes[2] == 2:
        out = paired(sizes, old_fields, corner_shift, points, owners)
        return out.transpose(1, 0, 2).reshape(nvar, blocks * pts)
    vmem = pl.BlockSpec(memory_space=pltpu.VMEM)
    hbm = pl.BlockSpec(memory_space=pltpu.HBM)
    message = pltpu.VMEM((8 * n, pts), F32)
    result = pltpu.VMEM((CAP * n, nvar, pts), F32)
    out = pl.pallas_call(
        functools.partial(kernel, sizes, group_peers),
        out_shape=jax.ShapeDtypeStruct((blocks, nvar, pts), F32),
        in_specs=[hbm] * 4,
        out_specs=vmem,
        scratch_shapes=[
            pltpu.VMEM((1, blocks), jnp.int32),
            pltpu.VMEM((blocks, 3, pts), F32),
            pltpu.VMEM((24, elems), F32),
            pltpu.VMEM((elems, nvar, nodes), F32),
            pltpu.VMEM((elems, 32, 128), BF16),
            message, message, result, result,
            pltpu.VMEM((3, 8 * CAP * group_peers, pts), F32),
            pltpu.VMEM((wide, 128), jnp.int32),
            pltpu.VMEM((wide * n, 128), jnp.int32),
            pltpu.SMEM((wide * n, 128), jnp.int32),
            pltpu.VMEM((1, pts), jnp.int32),
            pltpu.SMEM((1, pts), jnp.int32),
            *[pltpu.SemaphoreType.DMA] * 6,
            pltpu.SemaphoreType.DMA, pltpu.SemaphoreType.DMA((groups,)),
            pltpu.SemaphoreType.DMA, pltpu.SemaphoreType.DMA((groups,)),
            pltpu.SemaphoreType.DMA, pltpu.SemaphoreType.DMA((groups,)),
        ],
        compiler_params=pltpu.CompilerParams(
            collective_id=0, has_side_effects=True, vmem_limit_bytes=16 * 1024 * 1024),
    )(*[pltpu.with_memory_space_constraint(x, pltpu.HBM) for x in (owners.reshape(1, blocks), points, corner_shift, old_fields)])
    return out.transpose(1, 0, 2).reshape(nvar, blocks * pts)


def solution(mesh):
    sizes = tuple(mesh.shape[a] for a in AXES)
    in_specs = (
        P(("groups", "block", "seg", "sub"), None, None),
        P(None, ("groups", "block", "seg", "sub")),
        P(None, ("groups", "block", "seg", "sub")),
        P(("groups", "block", "seg", "sub")),
    )
    out_specs = P(None, ("groups", "block", "seg", "sub"))
    return jax.shard_map(functools.partial(shards, sizes), mesh=mesh, in_specs=in_specs,
                         out_specs=out_specs, check_vma=False)
```

```python
import functools

import jax
import jax.numpy as jnp
from jax import lax
from jax.experimental import pallas as pl
from jax.experimental.pallas import tpu as pltpu
from jax.sharding import PartitionSpec as P

NEWTON = 3
CAP = 2
GROUP_PEERS = 4
AXES = ("block", "seg", "sub")

GLL_POINTS = (
    -1.0,
    -0.8717401485096066,
    -0.5917001814331423,
    -0.2092992179024789,
    0.2092992179024789,
    0.5917001814331423,
    0.8717401485096066,
    1.0,
)
WEIGHTS = []
for _n in range(8):
    _w = 1.0
    for _m in range(8):
        if _m != _n:
            _w /= GLL_POINTS[_n] - GLL_POINTS[_m]
    WEIGHTS.append(_w)

F32 = jnp.float32
BF16 = jnp.bfloat16
EXACT = lax.Precision.HIGHEST
NT = (((1,), (1,)), ((), ()))


def iota(shape, dim):
    return lax.broadcasted_iota(jnp.int32, shape, dim)


def flip(index, static):
    bit = 1
    while bit <= static:
        if static & bit:
            index = index + bit * (1 - 2 * ((index // bit) % 2))
        bit *= 2
    return index


def newton(coef, y):
    def update(xi, jac, misfit):
        m = jac
        cof = [
            [m[1][1] * m[2][2] - m[1][2] * m[2][1], m[1][2] * m[2][0] - m[1][0] * m[2][2], m[1][0] * m[2][1] - m[1][1] * m[2][0]],
            [m[0][2] * m[2][1] - m[0][1] * m[2][2], m[0][0] * m[2][2] - m[0][2] * m[2][0], m[0][1] * m[2][0] - m[0][0] * m[2][1]],
            [m[0][1] * m[1][2] - m[0][2] * m[1][1], m[0][2] * m[1][0] - m[0][0] * m[1][2], m[0][0] * m[1][1] - m[0][1] * m[1][0]],
        ]
        inv = 1.0 / (m[0][0] * cof[0][0] + m[0][1] * cof[0][1] + m[0][2] * cof[0][2])
        out = []
        for b in range(3):
            step = (cof[0][b] * misfit[0] + cof[1][b] * misfit[1] + cof[2][b] * misfit[2]) * inv
            new = -step if xi is None else xi[b] - step
            out.append(jnp.clip(new, -1.2, 1.2))
        return out

    xi = update(None, [[c[4], c[2], c[1]] for c in coef], [c[0] - t for c, t in zip(coef, y)])
    for _ in range(NEWTON - 1):
        u, v, w = xi
        uv, uw, vw = u * v, u * w, v * w
        jac, misfit = [], []
        for c, t in zip(coef, y):
            du = c[4] + c[6] * v + c[5] * w + c[7] * vw
            dv = c[2] + c[6] * u + c[3] * w + c[7] * uw
            dw = c[1] + c[5] * u + c[3] * v + c[7] * uv
            jac.append([du, dv, dw])
            misfit.append((c[0] - t) + u * du + v * (c[2] + c[3] * w) + w * c[1])
        xi = update(xi, jac, misfit)
    return xi


def lagrange(x):
    diff = [x - t for t in GLL_POINTS]
    pre = [None, diff[0]]
    for n in range(2, 8):
        pre.append(pre[-1] * diff[n - 1])
    suf = [None] * 8
    suf[6] = diff[7]
    for n in range(5, -1, -1):
        suf[n] = suf[n + 1] * diff[n + 1]
    out = []
    for n in range(8):
        value = suf[n] if n == 0 else pre[n] if n == 7 else pre[n] * suf[n]
        out.append(value * WEIGHTS[n])
    return out


def kernel(sizes, group_peers, owners_hbm, targets_hbm, shift_hbm, fields_hbm, out_ref,
           owners_ref, targets_ref, shift_ref, fbuf, table, send, recv, res, ret, lag, idsend, idrecv, ids, slotv, slots,
           osem, tsem, csem, fsem, idsem, slotsem, s0, r0, s1, r1, s2, r2):
    nb, ns, nc = sizes
    n = nb * ns * nc
    blocks = owners_ref.shape[1]
    elems = shift_ref.shape[1]
    pts = out_ref.shape[2]
    groups = n // group_peers
    lanes = idsend.shape[1]
    wide = idsend.shape[0]
    here = [lax.axis_index(a) for a in AXES]
    me = (here[0] * ns + here[1]) * nc + here[2]

    def peer(k):
        if isinstance(k, int):
            return {
                "block": flip(here[0], k // (ns * nc)),
                "seg": flip(here[1], (k // nc) % ns),
                "sub": flip(here[2], k % nc),
            }
        other = jnp.bitwise_xor(me, k)
        return {"block": other // (ns * nc), "seg": (other // nc) % ns, "sub": other % nc}

    def message(k):
        return pl.ds(8 * k if isinstance(k, int) else pl.multiple_of(8 * k, 8), 3 * CAP)

    def for_wait(first, count, ref, sem):
        part = ref.at[pl.ds(8 * first, 3 * CAP * count), :]
        pltpu.make_async_copy(part, part, sem).wait()

    def send_result(k, g):
        part = pl.ds(CAP * k, CAP)
        return pltpu.make_async_remote_copy(
            src_ref=res.at[part], dst_ref=ret.at[part], send_sem=s2, recv_sem=r2.at[g],
            device_id=peer(k), device_id_type=pl.DeviceIdType.MESH)

    get_owners = pltpu.make_async_copy(owners_hbm, owners_ref, osem)
    get_owners.start()
    get_targets = pltpu.make_async_copy(targets_hbm, targets_ref, tsem)
    get_targets.start()
    get_shift = pltpu.make_async_copy(shift_hbm, shift_ref, csem)
    get_shift.start()
    fetch = pltpu.make_async_copy(fields_hbm, fbuf, fsem)
    fetch.start()
    barrier = pltpu.get_barrier_semaphore()
    unrolled = n <= 32

    def for_peers(first, last, body):
        if unrolled:
            for k in reversed(range(first, last)):
                body(k)
        else:
            lax.fori_loop(first, last, lambda k, c: (body(k), c)[1], 0)

    for_peers(1, n, lambda k: pl.semaphore_signal(
        barrier, inc=1, device_id=peer(k), device_id_type=pl.DeviceIdType.MESH))

    shift_bits = elems.bit_length() - 1
    get_owners.wait()
    own = owners_ref[...]
    owner_dev = jnp.right_shift(own, shift_bits)
    hit = (jnp.bitwise_xor(iota((n, blocks), 0), me) == owner_dev).astype(F32)
    earlier = (iota((blocks, blocks), 0) < iota((blocks, blocks), 1)).astype(F32)
    rank = jnp.dot(hit, earlier, preferred_element_type=F32)
    match = [jnp.where(rank == float(c), hit, 0.0) for c in range(CAP)]
    both = jnp.concatenate(match, axis=0)
    get_targets.wait()
    cat = jnp.concatenate([targets_ref[:, a, :] for a in range(3)], axis=1)
    packed = jnp.dot(both, cat, precision=EXACT, preferred_element_type=F32)
    for c in range(CAP):
        part = slice(c * n, (c + 1) * n)
        for a in range(3):
            send[pl.ds(3 * c + a, n, stride=8), :] = packed[part, a * pts:(a + 1) * pts]
            recv[3 * c + a:3 * c + a + 1, :] = packed[c * n:c * n + 1, a * pts:(a + 1) * pts]
    square = (blocks, blocks)
    diag = iota(square, 0) == iota(square, 1)
    own_rows = jnp.broadcast_to(own, square)
    own_col = jnp.sum(jnp.where(diag, own_rows, 0), axis=1, keepdims=True)
    dev_col = jnp.right_shift(own_col, shift_bits)
    dev_row = jnp.right_shift(own_rows, shift_bits)
    same = jnp.where(dev_col == dev_row, 1, 0)
    rank_row = jnp.sum(jnp.where(iota(square, 0) < iota(square, 1), same, 0), axis=0, keepdims=True)
    rank_col = jnp.sum(jnp.where(iota(square, 1) < iota(square, 0), same, 0), axis=1, keepdims=True)
    place = jnp.minimum(CAP * jnp.bitwise_xor(owner_dev, me) + rank_row, CAP * n - 1)
    place = jnp.concatenate([place, jnp.zeros((1, pts - blocks), jnp.int32)], axis=1)
    elem_col = own_col - dev_col * elems
    lane_of = jnp.where(rank_col < CAP, jnp.bitwise_xor(dev_col, me) + n * rank_col, -1)
    for r in range(wide):
        here_lane = iota((blocks, lanes), 1) + lanes * r == lane_of
        row = jnp.sum(jnp.where(here_lane, elem_col, 0), axis=0, keepdims=True)
        idsend[r:r + 1, :] = row
        idrecv[r:r + 1, :] = row
    slotv[...] = place
    slot_copy = pltpu.make_async_copy(slotv, slots, slotsem)
    slot_copy.start()

    pl.semaphore_wait(barrier, n - 1)
    def send_points(k):
        g = k // group_peers
        pltpu.make_async_remote_copy(
            src_ref=idsend, dst_ref=idrecv.at[pl.ds(wide * k, wide), :], send_sem=s0, recv_sem=r0.at[g],
            device_id=peer(k), device_id_type=pl.DeviceIdType.MESH).start()
        pltpu.make_async_remote_copy(
            src_ref=send.at[message(k), :], dst_ref=recv.at[message(k), :], send_sem=s1, recv_sem=r1.at[g],
            device_id=peer(k), device_id_type=pl.DeviceIdType.MESH).start()

    for_peers(1, n, send_points)

    row, col = iota((24, 24), 0), iota((24, 24), 1)
    both_bits = jnp.bitwise_and(row, col) % 8
    odd = (both_bits + both_bits // 2 + both_bits // 4) % 2
    hada = jnp.where(row // 8 == col // 8, (1 - 2 * odd).astype(F32) * 0.125, 0.0)
    get_shift.wait()
    bits = row % 8
    sign = (1 - 2 * ((bits + bits // 2 + bits // 4) % 2)).astype(F32)
    coefs = jnp.dot(hada * sign, shift_ref[...], precision=EXACT, preferred_element_type=F32)
    c_hi = coefs.astype(BF16)
    rest = coefs - c_hi.astype(F32)
    c_mid = rest.astype(BF16)
    c_lo = (rest - c_mid.astype(F32)).astype(BF16)

    fetch.wait()
    low_sub = iota((8, 128), 0) < 4
    low_lane = iota((8, 128), 1) < 64
    keep = low_sub == low_lane

    def split(e, carry):
        parts = []
        for q in range(4):
            x = fbuf[e, :, q * 128:(q + 1) * 128]
            x = jnp.concatenate([x, x], axis=0)
            hi = x.astype(BF16).astype(F32)
            lo = x - hi
            a = jnp.where(low_sub, hi, lo)
            b = pltpu.roll(jnp.where(low_sub, lo, hi), 64, axis=1)
            parts.append(jnp.where(keep, a, b))
        table[e] = jnp.concatenate(parts, axis=0).astype(BF16)
        return carry

    lax.fori_loop(0, elems, split, 0, unroll=4)

    per = group_peers
    count = CAP * per

    def run_group(g, first):
        base = g * per
        got = per - 1 if first else per
        start = base + 1 if first else base
        for_wait(start, got, recv, r1.at[g])

        def gather(a):
            return jnp.concatenate(
                [recv[pl.ds(8 * base + 3 * c + a, per, stride=8), :] for c in range(CAP)], axis=0)

        y = [gather(a) for a in range(3)]
        taken = idrecv.at[pl.ds(wide * start, wide * got), :]
        pltpu.make_async_copy(taken, taken, r0.at[g]).wait()
        id_copy = pltpu.make_async_copy(idrecv.at[pl.ds(wide * base, wide * per), :], ids.at[pl.ds(wide * base, wide * per), :], idsem)
        id_copy.start()
        id_lane = iota((per, lanes), 1) - iota((per, lanes), 0)
        id_cols = []
        for c in range(CAP):
            at = c * n + base
            id_rows = idrecv[pl.ds(wide * base + at // lanes, per, stride=wide), :]
            id_cols.append(jnp.sum(jnp.where(id_lane == at % lanes, id_rows, 0), axis=1, keepdims=True))
        elem = jnp.concatenate(id_cols, axis=0)
        pick = jnp.where(elem == iota((count, elems), 1), 1.0, 0.0).astype(BF16)
        chosen = sum(lax.dot_general(pick, c, NT, preferred_element_type=F32) for c in (c_hi, c_mid, c_lo))
        coef = []
        for a in range(3):
            line = []
            for m in range(8):
                value = chosen[:, 8 * a + m:8 * a + m + 1]
                if m == 4 >> a:
                    value = value + 1.0
                line.append(jnp.broadcast_to(value, (count, pts)))
            coef.append(line)
        xi = newton(coef, y)
        for a in range(3):
            for i, value in enumerate(lagrange(xi[a])):
                lag[a, pl.ds(i, count, stride=8), :] = value
        id_copy.wait()
        for s in range(count):
            c, p = s // per, s % per
            e = ids[wide * (base + p) + (c * n + base) // lanes, (c * n + base) % lanes + p]
            left = table[e]
            lz = lag[2, 8 * s:8 * s + 8, :]
            w = jnp.concatenate([lag[1, 8 * s + j:8 * s + j + 1, :] * lz for j in range(8)], axis=0)
            w_hi = w.astype(BF16)
            w_lo = (w - w_hi.astype(F32)).astype(BF16)
            prod = jnp.dot(
                jnp.concatenate([left, left], axis=1),
                jnp.concatenate([w_hi, w_hi, w_lo, w_lo], axis=0),
                preferred_element_type=F32)
            total = None
            for q in range(4):
                lx = jnp.where(low_sub, lag[0, 8 * s + 2 * q:8 * s + 2 * q + 1, :],
                               lag[0, 8 * s + 2 * q + 1:8 * s + 2 * q + 2, :])
                term = prod[8 * q:8 * q + 8] * lx
                total = term if total is None else total + term
            total = total[0:4] + total[4:8]
            if first and p == 0:
                ret[c] = total
            else:
                res[CAP * (base + p) + c] = total
        for_peers_in = range(1 if first else 0, per)
        for p in for_peers_in:
            send_result(base + p, g).start()

    run_group(0, True)
    if unrolled:
        for g in range(1, groups):
            run_group(g, False)
    else:
        lax.fori_loop(1, groups, lambda g, c: (run_group(g, False), c)[1], 0)

    slot_copy.wait()
    for g in range(groups):
        start, got = (1, per - 1) if g == 0 else (g * per, per)
        back = ret.at[pl.ds(CAP * start, CAP * got)]
        pltpu.make_async_copy(back, back, r2.at[g]).wait()
    for b in range(blocks):
        out_ref[b] = ret[slots[0, b]]
    rest_ids = idrecv.at[pl.ds(wide, wide * (n - 1)), :]
    pltpu.make_async_copy(rest_ids, rest_ids, s0).wait()
    for_wait(1, n - 1, send, s1)
    left = res.at[pl.ds(CAP, CAP * (n - 1))]
    pltpu.make_async_copy(left, left, s2).wait()


def pair_kernel(sizes, owners_hbm, targets_hbm, shift_hbm, fields_hbm, out_ref,
                owners_ref, targets_ref, shift_ref, fbuf, ctab, send, give, via, recv, cbuf, lag, res, ret, slots,
                csem, fsem, sent, r_rel, r_fld, r1, r2, r_via, here):
    nb, ns, nc = sizes
    half = nb * ns // 2
    blocks = owners_ref.shape[1]
    elems = shift_ref.shape[1]
    pts = out_ref.shape[2]
    quad = nc * CAP
    rows = 4 * quad
    per = 2 * quad
    b, s, c = [lax.axis_index(a) for a in AXES]
    chip = b * ns + s
    other = 1 - c
    top = nb // 2
    across = b + c * top * (1 - 2 * ((b // top) % 2))

    def peer(j, core):
        return {"block": flip(across, j // ns), "seg": flip(s, j % ns), "sub": core}

    def near(j, core):
        return {"block": flip(b, j // ns), "seg": flip(s, j % ns), "sub": core}

    def unless_here(j, body):
        if j == 0:
            pl.when(c == 1)(body)
        else:
            body()

    def remote(src, dst, send_sem, recv_sem, device):
        return pltpu.make_async_remote_copy(
            src_ref=src, dst_ref=dst, send_sem=send_sem, recv_sem=recv_sem,
            device_id=device, device_id_type=pl.DeviceIdType.MESH)

    def wait_for(part, sem):
        pltpu.make_async_copy(part, part, sem).wait()

    get_owners = pltpu.make_async_copy(owners_hbm, owners_ref, r2)
    get_owners.start()
    get_targets = pltpu.make_async_copy(targets_hbm, targets_ref, sent)
    get_targets.start()
    barrier = pltpu.get_barrier_semaphore()

    def hello(device):
        pl.semaphore_signal(barrier, inc=1, device_id=device, device_id_type=pl.DeviceIdType.MESH)

    sibling = {"block": b, "seg": s, "sub": other}
    partner = {"block": b, "seg": flip(s, 1), "sub": 1}
    first = jnp.logical_and(c == 1, b == 0)
    high = jnp.logical_and(c == 1, b >= top)

    def above(j):
        return b % 2 == 0 if j // ns else s == 0

    def below(j):
        return b % 2 == 1 if j // ns else s == 1

    @pl.when(c == 1)
    def _():
        @pl.when(b < top)
        def _():
            for j in reversed(range(half)):
                hello(peer(j, 1))

        pl.when(b == 0)(lambda: hello(partner))
        hello(sibling)

    @pl.when(c == 0)
    def _():
        for j in reversed(range(1, half)):
            pl.when(above(j))(lambda: hello(near(j, 0)))

    get_shift = pltpu.make_async_copy(shift_hbm, shift_ref, csem)
    get_shift.start()
    fetch = pltpu.make_async_copy(fields_hbm, fbuf.at[pl.ds(0, elems)], fsem)
    fetch.start()

    pl.when(c == 0)(lambda: pl.semaphore_wait(barrier, 1 + (b % 2) * ns + s))
    pl.when(high)(lambda: pl.semaphore_wait(barrier, half))

    def answer(device):
        pl.semaphore_signal(here, inc=1, device_id=device, device_id_type=pl.DeviceIdType.MESH)

    @pl.when(high)
    def _():
        for j in reversed(range(half)):
            if j % ns:
                pl.when(flip(across, j // ns) != 0)(lambda: answer(peer(j, 1)))
            else:
                answer(peer(j, 1))

    @pl.when(c == 0)
    def _():
        for j in reversed(range(1, half)):
            pl.when(below(j))(lambda: answer(near(j, 0)))

    shift_bits = elems.bit_length() - 1
    square = (blocks, blocks)
    get_owners.wait()
    own = owners_ref[...]
    own_rows = jnp.broadcast_to(own, square)
    diag = iota(square, 0) == iota(square, 1)
    own_col = jnp.sum(jnp.where(diag, own_rows, 0), axis=1, keepdims=True)
    dev_col = jnp.right_shift(own_col, shift_bits)
    dev_row = jnp.right_shift(own_rows, shift_bits)
    same = jnp.where(dev_col == dev_row, 1, 0)
    rank_row = jnp.sum(jnp.where(iota(square, 0) < iota(square, 1), same, 0), axis=0, keepdims=True)
    rank_col = jnp.sum(jnp.where(iota(square, 1) < iota(square, 0), same, 0), axis=1, keepdims=True)
    base_chip = jnp.bitwise_xor(chip, c * half)

    def slot_of(dev, rank):
        rel = jnp.bitwise_xor(jnp.right_shift(dev, 1), base_chip)
        return rel, (rel * nc + jnp.bitwise_and(dev, 1)) * CAP + rank

    rel_col, slot_col = slot_of(dev_col, rank_col)
    turned = jnp.where(rel_col >= half, 1, 0)
    side = jnp.bitwise_xor(jnp.bitwise_xor(jnp.bitwise_and(dev_col, 1), c), turned)
    elem_col = own_col - dev_col * elems + elems * side
    _, slot_row = slot_of(jnp.right_shift(own, shift_bits), rank_row)
    count = 2 * half * quad
    pick = jnp.where(iota((count, blocks), 0) == slot_row, 1.0, 0.0)
    id_rows = jnp.broadcast_to(elem_col.astype(F32), (blocks, pts))
    get_targets.wait()
    cat = jnp.concatenate([targets_ref[:, a, :] for a in range(3)] + [id_rows], axis=1)
    packed = jnp.dot(pick, cat, precision=EXACT, preferred_element_type=F32)
    for a in range(4):
        for j in range(half):
            send[j, pl.ds(a, quad, stride=4), :] = packed[quad * j:quad * (j + 1), a * pts:(a + 1) * pts]
            give[j, pl.ds(a, quad, stride=4), :] = packed[quad * (half + j):quad * (half + j + 1), a * pts:(a + 1) * pts]
    slot_safe = jnp.minimum(jnp.maximum(slot_col, 0), count - 1)
    for k in range(blocks):
        slots[0, k] = slot_safe[k, 0]

    low_sub = iota((8, 128), 0) < 4
    low_lane = iota((8, 128), 1) < 64

    def split(e):
        high_part, low_part = [], []
        for r in range(0, fbuf.shape[1], 8):
            x = fbuf[e, r:r + 8, :]
            turned = pltpu.roll(x, 64, axis=1)
            for part in (jnp.where(low_lane, x, turned), jnp.where(low_lane, turned, x)):
                hi = part.astype(BF16).astype(F32)
                high_part.append(hi)
                low_part.append(part - hi)
        return jnp.concatenate(high_part + low_part, axis=0).astype(BF16)

    row, col = iota((24, 24), 0), iota((24, 24), 1)
    both_bits = jnp.bitwise_and(row, col) % 8
    odd = (both_bits + both_bits // 2 + both_bits // 4) % 2
    hada = jnp.where(row // 8 == col // 8, (1 - 2 * odd).astype(F32) * 0.125, 0.0)
    bits = row % 8
    sign = (1 - 2 * ((bits + bits // 2 + bits // 4) % 2)).astype(F32)
    line = iota((24, elems), 0)
    unit = jnp.where(line % 8 == jnp.right_shift(4, line // 8), 1.0, 0.0)

    def spread(side, shift):
        coefs = jnp.dot(hada * sign, shift, precision=EXACT, preferred_element_type=F32) + unit
        for e in range(elems):
            ctab[side * elems + e] = jnp.broadcast_to(coefs[:, e:e + 1], (24, pts))

    get_shift.wait()
    give[half, :, :elems] = shift_ref[:rows]
    give[half + 1, :24 - rows, :elems] = shift_ref[rows:]
    fetch.wait()
    pl.when(first)(lambda: pl.semaphore_wait(barrier, 1))
    theirs = send.at[:, pl.ds(rows, rows), :]

    def heard(count):
        pl.semaphore_wait(here, count)

    def share():
        remote(fbuf.at[pl.ds(0, elems)], fbuf.at[pl.ds(elems, elems)], sent, r_fld, sibling).start()

    corner = (b % 2) * ns + s

    def request(src, group, device):
        at = pl.multiple_of(2 * rows * group, 2 * rows)
        remote(src, recv.at[pl.ds(at, 2 * rows), :], sent, r1.at[group], device).start()

    def parted(src, device, core):
        for part, sem in ((core, 0), (1 - core, half)):
            piece = pl.ds(rows * part, rows)
            remote(src.at[piece, :], recv.at[piece, :], sent, r1.at[sem], device).start()

    def mine(src, device, core):
        pl.when(corner == 0)(lambda: parted(src, device, core))
        pl.when(corner > 0)(lambda: request(src, corner, device))

    @pl.when(c == 0)
    def _():
        remote(give, theirs, sent, r_rel, sibling).start()
        share()
        wait_for(theirs, r_rel)
        pl.when(corner < half - 1)(lambda: heard(half - 1 - corner))
        for j in reversed(range(1, half)):
            mine(send.at[j], near(j, 0), 0)
        recv[pl.ds(pl.multiple_of(2 * rows * corner, 2 * rows), 2 * rows), :] = send[0]

    @pl.when(c == 1)
    def _():
        wait_for(theirs, r_rel)

        @pl.when(b == 0)
        def _():
            for j in reversed(range(1, half, ns)):
                remote(send.at[j], via.at[j // ns], sent, r_via, partner).start()

        remote(give, theirs, sent, r_rel, sibling).start()

        columns = list(reversed(range(half // ns)))

        @pl.when(jnp.logical_and(b == 0, s == 0))
        def _():
            heard(half // ns)
            for i in columns:
                parted(send.at[ns * i], peer(ns * i, 1), 1)
            share()
            wait_for(via, r_via)
            for i in columns:
                request(via.at[i], 1, peer(ns * i, 1))

        @pl.when(jnp.logical_and(b == 0, s == 1))
        def _():
            wait_for(via, r_via)
            heard(half // ns)
            for i in columns:
                parted(via.at[i], peer(ns * i, 1), 1)
                request(send.at[ns * i], 1, peer(ns * i, 1))
            share()

        @pl.when(b > 0)
        def _():
            pl.when(b < top)(lambda: heard(half))
            for j in reversed(range(half)):
                mine(send.at[j], peer(j, 1), 1)
            share()

    spread(0, shift_ref[...])
    spread(1, jnp.concatenate([send[half, rows:2 * rows, :elems], send[half + 1, rows:2 * rows, :elems]], axis=0)[:24])
    wait_for(fbuf.at[pl.ds(elems, elems)], r_fld)

    def compute(base, count, at):
        y = [recv[pl.ds(base + a, count, stride=4), :] for a in range(3)]
        ids = recv[pl.ds(base + 3, count, stride=4), :].astype(jnp.int32)
        ids = jnp.minimum(jnp.maximum(ids, 0), 2 * elems - 1)
        elem = [ids[k, 0] for k in range(count)]
        for k in range(count):
            for a in range(3):
                cbuf[a, 8 * k:8 * k + 8, :] = ctab[elem[k], 8 * a:8 * a + 8, :]
        coef = [[cbuf[a, pl.ds(m, count, stride=8), :] for m in range(8)] for a in range(3)]
        xi = newton(coef, y)
        for a in range(3):
            for i, value in enumerate(lagrange(xi[a])):
                lag[a, per * i:per * i + count, :] = value
        for k in range(count):
            left = split(elem[k])
            lz = lag[2, pl.ds(k, 8, stride=per), :]
            w = jnp.concatenate([lag[1, per * i + k:per * i + k + 1, :] * lz for i in range(8)], axis=0)
            w_hi = w.astype(BF16)
            w_lo = (w - w_hi.astype(F32)).astype(BF16)
            prod = jnp.dot(left, jnp.concatenate([w_hi, w_lo], axis=0), preferred_element_type=F32)
            prod = prod[:32] + prod[32:]
            total = None
            for q in range(4):
                i = per * (4 * (q // 2) + q % 2) + k
                lx = jnp.where(low_sub, lag[0, i:i + 1, :], lag[0, i + 2 * per:i + 2 * per + 1, :])
                term = prod[8 * q:8 * q + 8] * lx
                total = term if total is None else total + term
            res[at + k] = total[0:4] + total[4:8]

    for g in range(half):
        base = 2 * rows * g
        z, x = g // ns, g % ns
        local = jnp.logical_and(c == 0, corner == g)

        def unless_local(body):
            pl.when(jnp.logical_not(local))(body)

        slot = ns * flip(b % 2, z) + flip(s, x)

        def result(at, to, core):
            return remote(res.at[pl.ds(at, quad)], ret.at[pl.ds(quad * to, quad)],
                          sent, r2, {"block": 2 * (across // 2) + z, "seg": x, "sub": core})

        def keep(at):
            ret[0:quad] = res[at:at + quad]

        if g == 0:
            for part, sem in ((c, 0), (other, half)):
                start = pl.multiple_of(rows * part, rows)
                unless_local(lambda: wait_for(recv.at[pl.ds(start, rows), :], r1.at[sem]))
                at = quad if sem else 0
                compute(start, quad, at)
                if sem:
                    result(at, half * other + slot, 1).start()
                else:
                    unless_local(lambda: result(at, half * c + slot, 0).start())
                    pl.when(local)(lambda: keep(at))
        else:
            unless_local(lambda: wait_for(recv.at[pl.ds(base, 2 * rows), :], r1.at[g]))
            compute(base, per, per * g)
            result(per * g + quad, half + slot, other).start()
            unless_local(lambda: result(per * g, slot, c).start())
            pl.when(local)(lambda: keep(per * g))

    pl.when(c == 0)(lambda: wait_for(ret.at[pl.ds(quad, quad * (2 * half - 1))], r2))
    pl.when(c == 1)(lambda: wait_for(ret, r2))
    for k in range(blocks):
        out_ref[k] = ret[slots[0, k]]
    wait_for(give, sent)
    wait_for(fbuf.at[pl.ds(elems, elems)], sent)

    def finish(skip):
        wait_for(recv.at[pl.ds(2 * rows * skip, 2 * rows * (half - skip)), :], sent)
        wait_for(ret.at[pl.ds(quad * skip, quad * (2 * half - skip))], sent)

    pl.when(c == 0)(lambda: finish(1))
    pl.when(c == 1)(lambda: finish(0))
    pl.when(first)(lambda: wait_for(via, sent))


def paired(sizes, old_fields, corner_shift, points, owners):
    half = sizes[0] * sizes[1] // 2
    elems, nvar, nodes = old_fields.shape
    blocks, _, pts = points.shape
    quad = sizes[2] * CAP
    rows = 4 * quad
    fields = old_fields.reshape(elems, nvar, nodes // 128, 128).transpose(0, 2, 1, 3)
    fields = fields.reshape(elems, nvar * nodes // 128, 128)
    vmem = pl.BlockSpec(memory_space=pltpu.VMEM)
    hbm = pl.BlockSpec(memory_space=pltpu.HBM)
    result = pltpu.VMEM((2 * half * quad, nvar, pts), F32)
    dma = pltpu.SemaphoreType.DMA
    return pl.pallas_call(
        functools.partial(pair_kernel, sizes),
        out_shape=jax.ShapeDtypeStruct((blocks, nvar, pts), F32),
        in_specs=[hbm] * 4,
        out_specs=vmem,
        scratch_shapes=[
            pltpu.VMEM((1, blocks), jnp.int32),
            pltpu.VMEM((blocks, 3, pts), F32),
            pltpu.VMEM((24, elems), F32),
            pltpu.VMEM((2 * elems, nvar * nodes // 128, 128), F32),
            pltpu.VMEM((2 * elems, 24, pts), F32),
            pltpu.VMEM((half + 2, 2 * rows, pts), F32),
            pltpu.VMEM((half + 2, rows, pts), F32),
            pltpu.VMEM((half // sizes[1], 2 * rows, pts), F32),
            pltpu.VMEM((2 * rows * half, pts), F32),
            pltpu.VMEM((3, 16 * quad, pts), F32),
            pltpu.VMEM((3, 16 * quad, pts), F32),
            result, result,
            pltpu.SMEM((1, blocks), jnp.int32),
            *[dma] * 5, dma((half + 1,)), dma,
            dma, pltpu.SemaphoreType.REGULAR,
        ],
        compiler_params=pltpu.CompilerParams(
            collective_id=0, has_side_effects=True, vmem_limit_bytes=24 * 1024 * 1024),
    )(*[pltpu.with_memory_space_constraint(x, pltpu.HBM) for x in (owners.reshape(1, blocks), points, corner_shift, fields)])


def shards(sizes, old_fields, corner_shift, targets, owners):
    n = sizes[0] * sizes[1] * sizes[2]
    elems, nvar, nodes = old_fields.shape
    blocks = owners.shape[0]
    pts = targets.shape[1] // blocks
    assert n & (n - 1) == 0 and elems & (elems - 1) == 0 and nvar == 4 and nodes == 512
    group_peers = min(GROUP_PEERS, n)
    groups = n // group_peers
    wide = (CAP * n + 127) // 128
    points = targets.reshape(3, blocks, pts).transpose(1, 0, 2)
    if sizes[0] == 4 and sizes[1] == 2 and sizes[2] == 2:
        out = paired(sizes, old_fields, corner_shift, points, owners)
        return out.transpose(1, 0, 2).reshape(nvar, blocks * pts)
    vmem = pl.BlockSpec(memory_space=pltpu.VMEM)
    hbm = pl.BlockSpec(memory_space=pltpu.HBM)
    message = pltpu.VMEM((8 * n, pts), F32)
    result = pltpu.VMEM((CAP * n, nvar, pts), F32)
    out = pl.pallas_call(
        functools.partial(kernel, sizes, group_peers),
        out_shape=jax.ShapeDtypeStruct((blocks, nvar, pts), F32),
        in_specs=[hbm] * 4,
        out_specs=vmem,
        scratch_shapes=[
            pltpu.VMEM((1, blocks), jnp.int32),
            pltpu.VMEM((blocks, 3, pts), F32),
            pltpu.VMEM((24, elems), F32),
            pltpu.VMEM((elems, nvar, nodes), F32),
            pltpu.VMEM((elems, 32, 128), BF16),
            message, message, result, result,
            pltpu.VMEM((3, 8 * CAP * group_peers, pts), F32),
            pltpu.VMEM((wide, 128), jnp.int32),
            pltpu.VMEM((wide * n, 128), jnp.int32),
            pltpu.SMEM((wide * n, 128), jnp.int32),
            pltpu.VMEM((1, pts), jnp.int32),
            pltpu.SMEM((1, pts), jnp.int32),
            *[pltpu.SemaphoreType.DMA] * 6,
            pltpu.SemaphoreType.DMA, pltpu.SemaphoreType.DMA((groups,)),
            pltpu.SemaphoreType.DMA, pltpu.SemaphoreType.DMA((groups,)),
            pltpu.SemaphoreType.DMA, pltpu.SemaphoreType.DMA((groups,)),
        ],
        compiler_params=pltpu.CompilerParams(
            collective_id=0, has_side_effects=True, vmem_limit_bytes=16 * 1024 * 1024),
    )(*[pltpu.with_memory_space_constraint(x, pltpu.HBM) for x in (owners.reshape(1, blocks), points, corner_shift, old_fields)])
    return out.transpose(1, 0, 2).reshape(nvar, blocks * pts)


def solution(mesh):
    sizes = tuple(mesh.shape[a] for a in AXES)
    in_specs = (
        P(("groups", "block", "seg", "sub"), None, None),
        P(None, ("groups", "block", "seg", "sub")),
        P(None, ("groups", "block", "seg", "sub")),
        P(("groups", "block", "seg", "sub")),
    )
    out_specs = P(None, ("groups", "block", "seg", "sub"))
    return jax.shard_map(functools.partial(shards, sizes), mesh=mesh, in_specs=in_specs,
                         out_specs=out_specs, check_vma=False)
```

```python
import functools

import jax
import jax.numpy as jnp
from jax import lax
from jax.experimental import pallas as pl
from jax.experimental.pallas import tpu as pltpu
from jax.sharding import PartitionSpec as P

NEWTON = 3
CAP = 2
GROUP_PEERS = 4
AXES = ("block", "seg", "sub")

GLL_POINTS = (
    -1.0,
    -0.8717401485096066,
    -0.5917001814331423,
    -0.2092992179024789,
    0.2092992179024789,
    0.5917001814331423,
    0.8717401485096066,
    1.0,
)
WEIGHTS = []
for _n in range(8):
    _w = 1.0
    for _m in range(8):
        if _m != _n:
            _w /= GLL_POINTS[_n] - GLL_POINTS[_m]
    WEIGHTS.append(_w)

F32 = jnp.float32
BF16 = jnp.bfloat16
EXACT = lax.Precision.HIGHEST
NT = (((1,), (1,)), ((), ()))


def iota(shape, dim):
    return lax.broadcasted_iota(jnp.int32, shape, dim)


def flip(index, static):
    bit = 1
    while bit <= static:
        if static & bit:
            index = index + bit * (1 - 2 * ((index // bit) % 2))
        bit *= 2
    return index


def newton(coef, y):
    def update(xi, jac, misfit):
        m = jac
        cof = [
            [m[1][1] * m[2][2] - m[1][2] * m[2][1], m[1][2] * m[2][0] - m[1][0] * m[2][2], m[1][0] * m[2][1] - m[1][1] * m[2][0]],
            [m[0][2] * m[2][1] - m[0][1] * m[2][2], m[0][0] * m[2][2] - m[0][2] * m[2][0], m[0][1] * m[2][0] - m[0][0] * m[2][1]],
            [m[0][1] * m[1][2] - m[0][2] * m[1][1], m[0][2] * m[1][0] - m[0][0] * m[1][2], m[0][0] * m[1][1] - m[0][1] * m[1][0]],
        ]
        inv = 1.0 / (m[0][0] * cof[0][0] + m[0][1] * cof[0][1] + m[0][2] * cof[0][2])
        out = []
        for b in range(3):
            step = (cof[0][b] * misfit[0] + cof[1][b] * misfit[1] + cof[2][b] * misfit[2]) * inv
            new = -step if xi is None else xi[b] - step
            out.append(jnp.clip(new, -1.2, 1.2))
        return out

    xi = update(None, [[c[4], c[2], c[1]] for c in coef], [c[0] - t for c, t in zip(coef, y)])
    for _ in range(NEWTON - 1):
        u, v, w = xi
        uv, uw, vw = u * v, u * w, v * w
        jac, misfit = [], []
        for c, t in zip(coef, y):
            du = c[4] + c[6] * v + c[5] * w + c[7] * vw
            dv = c[2] + c[6] * u + c[3] * w + c[7] * uw
            dw = c[1] + c[5] * u + c[3] * v + c[7] * uv
            jac.append([du, dv, dw])
            misfit.append((c[0] - t) + u * du + v * (c[2] + c[3] * w) + w * c[1])
        xi = update(xi, jac, misfit)
    return xi


def lagrange(x):
    diff = [x - t for t in GLL_POINTS]
    pre = [None, diff[0]]
    for n in range(2, 8):
        pre.append(pre[-1] * diff[n - 1])
    suf = [None] * 8
    suf[6] = diff[7]
    for n in range(5, -1, -1):
        suf[n] = suf[n + 1] * diff[n + 1]
    out = []
    for n in range(8):
        value = suf[n] if n == 0 else pre[n] if n == 7 else pre[n] * suf[n]
        out.append(value * WEIGHTS[n])
    return out


def kernel(sizes, group_peers, owners_hbm, targets_hbm, shift_hbm, fields_hbm, out_ref,
           owners_ref, targets_ref, shift_ref, fbuf, table, send, recv, res, ret, lag, idsend, idrecv, ids, slotv, slots,
           osem, tsem, csem, fsem, idsem, slotsem, s0, r0, s1, r1, s2, r2):
    nb, ns, nc = sizes
    n = nb * ns * nc
    blocks = owners_ref.shape[1]
    elems = shift_ref.shape[1]
    pts = out_ref.shape[2]
    groups = n // group_peers
    lanes = idsend.shape[1]
    wide = idsend.shape[0]
    here = [lax.axis_index(a) for a in AXES]
    me = (here[0] * ns + here[1]) * nc + here[2]

    def peer(k):
        if isinstance(k, int):
            return {
                "block": flip(here[0], k // (ns * nc)),
                "seg": flip(here[1], (k // nc) % ns),
                "sub": flip(here[2], k % nc),
            }
        other = jnp.bitwise_xor(me, k)
        return {"block": other // (ns * nc), "seg": (other // nc) % ns, "sub": other % nc}

    def message(k):
        return pl.ds(8 * k if isinstance(k, int) else pl.multiple_of(8 * k, 8), 3 * CAP)

    def for_wait(first, count, ref, sem):
        part = ref.at[pl.ds(8 * first, 3 * CAP * count), :]
        pltpu.make_async_copy(part, part, sem).wait()

    def send_result(k, g):
        part = pl.ds(CAP * k, CAP)
        return pltpu.make_async_remote_copy(
            src_ref=res.at[part], dst_ref=ret.at[part], send_sem=s2, recv_sem=r2.at[g],
            device_id=peer(k), device_id_type=pl.DeviceIdType.MESH)

    get_owners = pltpu.make_async_copy(owners_hbm, owners_ref, osem)
    get_owners.start()
    get_targets = pltpu.make_async_copy(targets_hbm, targets_ref, tsem)
    get_targets.start()
    get_shift = pltpu.make_async_copy(shift_hbm, shift_ref, csem)
    get_shift.start()
    fetch = pltpu.make_async_copy(fields_hbm, fbuf, fsem)
    fetch.start()
    barrier = pltpu.get_barrier_semaphore()
    unrolled = n <= 32

    def for_peers(first, last, body):
        if unrolled:
            for k in reversed(range(first, last)):
                body(k)
        else:
            lax.fori_loop(first, last, lambda k, c: (body(k), c)[1], 0)

    for_peers(1, n, lambda k: pl.semaphore_signal(
        barrier, inc=1, device_id=peer(k), device_id_type=pl.DeviceIdType.MESH))

    shift_bits = elems.bit_length() - 1
    get_owners.wait()
    own = owners_ref[...]
    owner_dev = jnp.right_shift(own, shift_bits)
    hit = (jnp.bitwise_xor(iota((n, blocks), 0), me) == owner_dev).astype(F32)
    earlier = (iota((blocks, blocks), 0) < iota((blocks, blocks), 1)).astype(F32)
    rank = jnp.dot(hit, earlier, preferred_element_type=F32)
    match = [jnp.where(rank == float(c), hit, 0.0) for c in range(CAP)]
    both = jnp.concatenate(match, axis=0)
    get_targets.wait()
    cat = jnp.concatenate([targets_ref[:, a, :] for a in range(3)], axis=1)
    packed = jnp.dot(both, cat, precision=EXACT, preferred_element_type=F32)
    for c in range(CAP):
        part = slice(c * n, (c + 1) * n)
        for a in range(3):
            send[pl.ds(3 * c + a, n, stride=8), :] = packed[part, a * pts:(a + 1) * pts]
            recv[3 * c + a:3 * c + a + 1, :] = packed[c * n:c * n + 1, a * pts:(a + 1) * pts]
    square = (blocks, blocks)
    diag = iota(square, 0) == iota(square, 1)
    own_rows = jnp.broadcast_to(own, square)
    own_col = jnp.sum(jnp.where(diag, own_rows, 0), axis=1, keepdims=True)
    dev_col = jnp.right_shift(own_col, shift_bits)
    dev_row = jnp.right_shift(own_rows, shift_bits)
    same = jnp.where(dev_col == dev_row, 1, 0)
    rank_row = jnp.sum(jnp.where(iota(square, 0) < iota(square, 1), same, 0), axis=0, keepdims=True)
    rank_col = jnp.sum(jnp.where(iota(square, 1) < iota(square, 0), same, 0), axis=1, keepdims=True)
    place = jnp.minimum(CAP * jnp.bitwise_xor(owner_dev, me) + rank_row, CAP * n - 1)
    place = jnp.concatenate([place, jnp.zeros((1, pts - blocks), jnp.int32)], axis=1)
    elem_col = own_col - dev_col * elems
    lane_of = jnp.where(rank_col < CAP, jnp.bitwise_xor(dev_col, me) + n * rank_col, -1)
    for r in range(wide):
        here_lane = iota((blocks, lanes), 1) + lanes * r == lane_of
        row = jnp.sum(jnp.where(here_lane, elem_col, 0), axis=0, keepdims=True)
        idsend[r:r + 1, :] = row
        idrecv[r:r + 1, :] = row
    slotv[...] = place
    slot_copy = pltpu.make_async_copy(slotv, slots, slotsem)
    slot_copy.start()

    pl.semaphore_wait(barrier, n - 1)
    def send_points(k):
        g = k // group_peers
        pltpu.make_async_remote_copy(
            src_ref=idsend, dst_ref=idrecv.at[pl.ds(wide * k, wide), :], send_sem=s0, recv_sem=r0.at[g],
            device_id=peer(k), device_id_type=pl.DeviceIdType.MESH).start()
        pltpu.make_async_remote_copy(
            src_ref=send.at[message(k), :], dst_ref=recv.at[message(k), :], send_sem=s1, recv_sem=r1.at[g],
            device_id=peer(k), device_id_type=pl.DeviceIdType.MESH).start()

    for_peers(1, n, send_points)

    row, col = iota((24, 24), 0), iota((24, 24), 1)
    both_bits = jnp.bitwise_and(row, col) % 8
    odd = (both_bits + both_bits // 2 + both_bits // 4) % 2
    hada = jnp.where(row // 8 == col // 8, (1 - 2 * odd).astype(F32) * 0.125, 0.0)
    get_shift.wait()
    bits = row % 8
    sign = (1 - 2 * ((bits + bits // 2 + bits // 4) % 2)).astype(F32)
    coefs = jnp.dot(hada * sign, shift_ref[...], precision=EXACT, preferred_element_type=F32)
    c_hi = coefs.astype(BF16)
    rest = coefs - c_hi.astype(F32)
    c_mid = rest.astype(BF16)
    c_lo = (rest - c_mid.astype(F32)).astype(BF16)

    fetch.wait()
    low_sub = iota((8, 128), 0) < 4
    low_lane = iota((8, 128), 1) < 64
    keep = low_sub == low_lane

    def split(e, carry):
        parts = []
        for q in range(4):
            x = fbuf[e, :, q * 128:(q + 1) * 128]
            x = jnp.concatenate([x, x], axis=0)
            hi = x.astype(BF16).astype(F32)
            lo = x - hi
            a = jnp.where(low_sub, hi, lo)
            b = pltpu.roll(jnp.where(low_sub, lo, hi), 64, axis=1)
            parts.append(jnp.where(keep, a, b))
        table[e] = jnp.concatenate(parts, axis=0).astype(BF16)
        return carry

    lax.fori_loop(0, elems, split, 0, unroll=4)

    per = group_peers
    count = CAP * per

    def run_group(g, first):
        base = g * per
        got = per - 1 if first else per
        start = base + 1 if first else base
        for_wait(start, got, recv, r1.at[g])

        def gather(a):
            return jnp.concatenate(
                [recv[pl.ds(8 * base + 3 * c + a, per, stride=8), :] for c in range(CAP)], axis=0)

        y = [gather(a) for a in range(3)]
        taken = idrecv.at[pl.ds(wide * start, wide * got), :]
        pltpu.make_async_copy(taken, taken, r0.at[g]).wait()
        id_copy = pltpu.make_async_copy(idrecv.at[pl.ds(wide * base, wide * per), :], ids.at[pl.ds(wide * base, wide * per), :], idsem)
        id_copy.start()
        id_lane = iota((per, lanes), 1) - iota((per, lanes), 0)
        id_cols = []
        for c in range(CAP):
            at = c * n + base
            id_rows = idrecv[pl.ds(wide * base + at // lanes, per, stride=wide), :]
            id_cols.append(jnp.sum(jnp.where(id_lane == at % lanes, id_rows, 0), axis=1, keepdims=True))
        elem = jnp.concatenate(id_cols, axis=0)
        pick = jnp.where(elem == iota((count, elems), 1), 1.0, 0.0).astype(BF16)
        chosen = sum(lax.dot_general(pick, c, NT, preferred_element_type=F32) for c in (c_hi, c_mid, c_lo))
        coef = []
        for a in range(3):
            line = []
            for m in range(8):
                value = chosen[:, 8 * a + m:8 * a + m + 1]
                if m == 4 >> a:
                    value = value + 1.0
                line.append(jnp.broadcast_to(value, (count, pts)))
            coef.append(line)
        xi = newton(coef, y)
        for a in range(3):
            for i, value in enumerate(lagrange(xi[a])):
                lag[a, pl.ds(i, count, stride=8), :] = value
        id_copy.wait()
        for s in range(count):
            c, p = s // per, s % per
            e = ids[wide * (base + p) + (c * n + base) // lanes, (c * n + base) % lanes + p]
            left = table[e]
            lz = lag[2, 8 * s:8 * s + 8, :]
            w = jnp.concatenate([lag[1, 8 * s + j:8 * s + j + 1, :] * lz for j in range(8)], axis=0)
            w_hi = w.astype(BF16)
            w_lo = (w - w_hi.astype(F32)).astype(BF16)
            prod = jnp.dot(
                jnp.concatenate([left, left], axis=1),
                jnp.concatenate([w_hi, w_hi, w_lo, w_lo], axis=0),
                preferred_element_type=F32)
            total = None
            for q in range(4):
                lx = jnp.where(low_sub, lag[0, 8 * s + 2 * q:8 * s + 2 * q + 1, :],
                               lag[0, 8 * s + 2 * q + 1:8 * s + 2 * q + 2, :])
                term = prod[8 * q:8 * q + 8] * lx
                total = term if total is None else total + term
            total = total[0:4] + total[4:8]
            if first and p == 0:
                ret[c] = total
            else:
                res[CAP * (base + p) + c] = total
        for_peers_in = range(1 if first else 0, per)
        for p in for_peers_in:
            send_result(base + p, g).start()

    run_group(0, True)
    if unrolled:
        for g in range(1, groups):
            run_group(g, False)
    else:
        lax.fori_loop(1, groups, lambda g, c: (run_group(g, False), c)[1], 0)

    slot_copy.wait()
    for g in range(groups):
        start, got = (1, per - 1) if g == 0 else (g * per, per)
        back = ret.at[pl.ds(CAP * start, CAP * got)]
        pltpu.make_async_copy(back, back, r2.at[g]).wait()
    for b in range(blocks):
        out_ref[b] = ret[slots[0, b]]
    rest_ids = idrecv.at[pl.ds(wide, wide * (n - 1)), :]
    pltpu.make_async_copy(rest_ids, rest_ids, s0).wait()
    for_wait(1, n - 1, send, s1)
    left = res.at[pl.ds(CAP, CAP * (n - 1))]
    pltpu.make_async_copy(left, left, s2).wait()


def pair_kernel(sizes, owners_hbm, targets_hbm, shift_hbm, fields_hbm, out_ref,
                owners_ref, targets_ref, shift_ref, fbuf, ctab, send, give, via, recv, cbuf, lag, res, ret, slots,
                csem, fsem, sent, r_rel, r_fld, r1, r2, r_via, here):
    nb, ns, nc = sizes
    half = nb * ns // 2
    blocks = owners_ref.shape[1]
    elems = shift_ref.shape[1]
    pts = out_ref.shape[2]
    quad = nc * CAP
    rows = 4 * quad
    per = 2 * quad
    b, s, c = [lax.axis_index(a) for a in AXES]
    chip = b * ns + s
    other = 1 - c
    top = nb // 2
    across = b + c * top * (1 - 2 * ((b // top) % 2))

    def peer(j, core):
        return {"block": flip(across, j // ns), "seg": flip(s, j % ns), "sub": core}

    def near(j, core):
        return {"block": flip(b, j // ns), "seg": flip(s, j % ns), "sub": core}

    def unless_here(j, body):
        if j == 0:
            pl.when(c == 1)(body)
        else:
            body()

    def remote(src, dst, send_sem, recv_sem, device):
        return pltpu.make_async_remote_copy(
            src_ref=src, dst_ref=dst, send_sem=send_sem, recv_sem=recv_sem,
            device_id=device, device_id_type=pl.DeviceIdType.MESH)

    def wait_for(part, sem):
        pltpu.make_async_copy(part, part, sem).wait()

    get_owners = pltpu.make_async_copy(owners_hbm, owners_ref, r2)
    get_owners.start()
    get_targets = pltpu.make_async_copy(targets_hbm, targets_ref, sent)
    get_targets.start()
    barrier = pltpu.get_barrier_semaphore()

    def hello(device):
        pl.semaphore_signal(barrier, inc=1, device_id=device, device_id_type=pl.DeviceIdType.MESH)

    sibling = {"block": b, "seg": s, "sub": other}
    partner = {"block": b, "seg": flip(s, 1), "sub": 1}
    first = jnp.logical_and(c == 1, b == 0)
    high = jnp.logical_and(c == 1, b >= top)

    def above(j):
        return b % 2 == 0 if j // ns else s == 0

    def below(j):
        return b % 2 == 1 if j // ns else s == 1

    @pl.when(c == 1)
    def _():
        @pl.when(b < top)
        def _():
            for j in reversed(range(half)):
                if j % ns:
                    pl.when(s == 0)(lambda: hello(peer(j, 1)))
                else:
                    hello(peer(j, 1))

        @pl.when(jnp.logical_and(b >= top, s == 0))
        def _():
            for j in reversed(range(1, half, ns)):
                pl.when(flip(across, j // ns) != 0)(lambda: hello(peer(j, 1)))

        pl.when(b == 0)(lambda: hello(partner))
        hello(sibling)

    @pl.when(c == 0)
    def _():
        for j in reversed(range(1, half)):
            pl.when(above(j))(lambda: hello(near(j, 0)))

    get_shift = pltpu.make_async_copy(shift_hbm, shift_ref, csem)
    get_shift.start()
    fetch = pltpu.make_async_copy(fields_hbm, fbuf.at[pl.ds(0, elems)], fsem)
    fetch.start()

    pl.when(c == 0)(lambda: pl.semaphore_wait(barrier, 1 + (b % 2) * ns + s))
    pl.when(high)(lambda: pl.semaphore_wait(barrier, half // ns * (1 + s)))

    def answer(device):
        pl.semaphore_signal(here, inc=1, device_id=device, device_id_type=pl.DeviceIdType.MESH)

    @pl.when(high)
    def _():
        for j in reversed(range(half)):
            if j % ns:
                pl.when(jnp.logical_and(flip(across, j // ns) != 0, s == 1))(lambda: answer(peer(j, 1)))
            else:
                answer(peer(j, 1))

    @pl.when(c == 0)
    def _():
        for j in reversed(range(1, half)):
            pl.when(below(j))(lambda: answer(near(j, 0)))

    shift_bits = elems.bit_length() - 1
    square = (blocks, blocks)
    get_owners.wait()
    own = owners_ref[...]
    own_rows = jnp.broadcast_to(own, square)
    diag = iota(square, 0) == iota(square, 1)
    own_col = jnp.sum(jnp.where(diag, own_rows, 0), axis=1, keepdims=True)
    dev_col = jnp.right_shift(own_col, shift_bits)
    dev_row = jnp.right_shift(own_rows, shift_bits)
    same = jnp.where(dev_col == dev_row, 1, 0)
    rank_row = jnp.sum(jnp.where(iota(square, 0) < iota(square, 1), same, 0), axis=0, keepdims=True)
    rank_col = jnp.sum(jnp.where(iota(square, 1) < iota(square, 0), same, 0), axis=1, keepdims=True)
    base_chip = jnp.bitwise_xor(chip, c * half)

    def slot_of(dev, rank):
        rel = jnp.bitwise_xor(jnp.right_shift(dev, 1), base_chip)
        return rel, (rel * nc + jnp.bitwise_and(dev, 1)) * CAP + rank

    rel_col, slot_col = slot_of(dev_col, rank_col)
    turned = jnp.where(rel_col >= half, 1, 0)
    side = jnp.bitwise_xor(jnp.bitwise_xor(jnp.bitwise_and(dev_col, 1), c), turned)
    elem_col = own_col - dev_col * elems + elems * side
    _, slot_row = slot_of(jnp.right_shift(own, shift_bits), rank_row)
    count = 2 * half * quad
    pick = jnp.where(iota((count, blocks), 0) == slot_row, 1.0, 0.0)
    id_rows = jnp.broadcast_to(elem_col.astype(F32), (blocks, pts))
    get_targets.wait()
    cat = jnp.concatenate([targets_ref[:, a, :] for a in range(3)] + [id_rows], axis=1)
    packed = jnp.dot(pick, cat, precision=EXACT, preferred_element_type=F32)
    for a in range(4):
        for j in range(half):
            send[j, pl.ds(a, quad, stride=4), :] = packed[quad * j:quad * (j + 1), a * pts:(a + 1) * pts]
            give[j, pl.ds(a, quad, stride=4), :] = packed[quad * (half + j):quad * (half + j + 1), a * pts:(a + 1) * pts]
    slot_safe = jnp.minimum(jnp.maximum(slot_col, 0), count - 1)
    for k in range(blocks):
        slots[0, k] = slot_safe[k, 0]

    low_sub = iota((8, 128), 0) < 4
    low_lane = iota((8, 128), 1) < 64

    def split(e):
        high_part, low_part = [], []
        for r in range(0, fbuf.shape[1], 8):
            x = fbuf[e, r:r + 8, :]
            turned = pltpu.roll(x, 64, axis=1)
            for part in (jnp.where(low_lane, x, turned), jnp.where(low_lane, turned, x)):
                hi = part.astype(BF16).astype(F32)
                high_part.append(hi)
                low_part.append(part - hi)
        return jnp.concatenate(high_part + low_part, axis=0).astype(BF16)

    row, col = iota((24, 24), 0), iota((24, 24), 1)
    both_bits = jnp.bitwise_and(row, col) % 8
    odd = (both_bits + both_bits // 2 + both_bits // 4) % 2
    hada = jnp.where(row // 8 == col // 8, (1 - 2 * odd).astype(F32) * 0.125, 0.0)
    bits = row % 8
    sign = (1 - 2 * ((bits + bits // 2 + bits // 4) % 2)).astype(F32)
    line = iota((24, elems), 0)
    unit = jnp.where(line % 8 == jnp.right_shift(4, line // 8), 1.0, 0.0)

    def spread(side, shift):
        coefs = jnp.dot(hada * sign, shift, precision=EXACT, preferred_element_type=F32) + unit
        for e in range(elems):
            ctab[side * elems + e] = jnp.broadcast_to(coefs[:, e:e + 1], (24, pts))

    get_shift.wait()
    give[half, :, :elems] = shift_ref[:rows]
    give[half + 1, :24 - rows, :elems] = shift_ref[rows:]
    fetch.wait()
    pl.when(first)(lambda: pl.semaphore_wait(barrier, 1))

    @pl.when(jnp.logical_and(c == 1, jnp.logical_and(jnp.logical_and(b > 0, b < top), s == 1)))
    def _():
        pl.semaphore_wait(barrier, half // ns)
        for j in reversed(range(1, half, ns)):
            answer(peer(j, 1))

    theirs = send.at[:, pl.ds(rows, rows), :]

    def heard(count):
        pl.semaphore_wait(here, count)

    def share():
        remote(fbuf.at[pl.ds(0, elems)], fbuf.at[pl.ds(elems, elems)], sent, r_fld, sibling).start()

    corner = (b % 2) * ns + s

    def request(src, group, device):
        at = pl.multiple_of(2 * rows * group, 2 * rows)
        remote(src, recv.at[pl.ds(at, 2 * rows), :], sent, r1.at[group], device).start()

    def parted(src, device, core):
        for part, sem in ((core, 0), (1 - core, half)):
            piece = pl.ds(rows * part, rows)
            remote(src.at[piece, :], recv.at[piece, :], sent, r1.at[sem], device).start()

    def mine(src, device, core):
        pl.when(corner == 0)(lambda: parted(src, device, core))
        pl.when(corner > 0)(lambda: request(src, corner, device))

    @pl.when(c == 0)
    def _():
        remote(give, theirs, sent, r_rel, sibling).start()
        share()
        wait_for(theirs, r_rel)
        pl.when(corner < half - 1)(lambda: heard(half - 1 - corner))
        for j in reversed(range(1, half)):
            mine(send.at[j], near(j, 0), 0)
        recv[pl.ds(pl.multiple_of(2 * rows * corner, 2 * rows), 2 * rows), :] = send[0]

    @pl.when(c == 1)
    def _():
        wait_for(theirs, r_rel)

        @pl.when(b == 0)
        def _():
            for j in reversed(range(1, half, ns)):
                remote(send.at[j], via.at[j // ns], sent, r_via, partner).start()

        remote(give, theirs, sent, r_rel, sibling).start()

        columns = list(reversed(range(half // ns)))

        @pl.when(jnp.logical_and(b == 0, s == 0))
        def _():
            heard(half // ns)
            for i in columns:
                parted(send.at[ns * i], peer(ns * i, 1), 1)
            for i in columns:
                answer(peer(ns * i, 1))
            share()
            wait_for(via, r_via)
            for i in columns:
                request(via.at[i], 1, peer(ns * i, 1))

        @pl.when(jnp.logical_and(b == 0, s == 1))
        def _():
            wait_for(via, r_via)
            heard(half // ns)
            for i in columns:
                parted(via.at[i], peer(ns * i, 1), 1)
                request(send.at[ns * i], 1, peer(ns * i, 1))
            share()

        @pl.when(b > 0)
        def _():
            pl.when(b < top)(lambda: heard(half // ns * (2 - s)))
            pl.when(jnp.logical_and(b >= top, s == 0))(lambda: heard(ns))
            for j in reversed(range(half)):
                mine(send.at[j], peer(j, 1), 1)
            share()

    spread(0, shift_ref[...])
    spread(1, jnp.concatenate([send[half, rows:2 * rows, :elems], send[half + 1, rows:2 * rows, :elems]], axis=0)[:24])
    wait_for(fbuf.at[pl.ds(elems, elems)], r_fld)

    def compute(base, count, at):
        y = [recv[pl.ds(base + a, count, stride=4), :] for a in range(3)]
        ids = recv[pl.ds(base + 3, count, stride=4), :].astype(jnp.int32)
        ids = jnp.minimum(jnp.maximum(ids, 0), 2 * elems - 1)
        elem = [ids[k, 0] for k in range(count)]
        for k in range(count):
            for a in range(3):
                cbuf[a, 8 * k:8 * k + 8, :] = ctab[elem[k], 8 * a:8 * a + 8, :]
        coef = [[cbuf[a, pl.ds(m, count, stride=8), :] for m in range(8)] for a in range(3)]
        xi = newton(coef, y)
        for a in range(3):
            for i, value in enumerate(lagrange(xi[a])):
                lag[a, per * i:per * i + count, :] = value
        for k in range(count):
            left = split(elem[k])
            lz = lag[2, pl.ds(k, 8, stride=per), :]
            w = jnp.concatenate([lag[1, per * i + k:per * i + k + 1, :] * lz for i in range(8)], axis=0)
            w_hi = w.astype(BF16)
            w_lo = (w - w_hi.astype(F32)).astype(BF16)
            prod = jnp.dot(left, jnp.concatenate([w_hi, w_lo], axis=0), preferred_element_type=F32)
            prod = prod[:32] + prod[32:]
            total = None
            for q in range(4):
                i = per * (4 * (q // 2) + q % 2) + k
                lx = jnp.where(low_sub, lag[0, i:i + 1, :], lag[0, i + 2 * per:i + 2 * per + 1, :])
                term = prod[8 * q:8 * q + 8] * lx
                total = term if total is None else total + term
            res[at + k] = total[0:4] + total[4:8]

    for g in range(half):
        base = 2 * rows * g
        z, x = g // ns, g % ns
        local = jnp.logical_and(c == 0, corner == g)

        def unless_local(body):
            pl.when(jnp.logical_not(local))(body)

        slot = ns * flip(b % 2, z) + flip(s, x)

        def result(at, to, core):
            return remote(res.at[pl.ds(at, quad)], ret.at[pl.ds(quad * to, quad)],
                          sent, r2, {"block": 2 * (across // 2) + z, "seg": x, "sub": core})

        def keep(at):
            ret[0:quad] = res[at:at + quad]

        if g == 0:
            for part, sem in ((c, 0), (other, half)):
                start = pl.multiple_of(rows * part, rows)
                unless_local(lambda: wait_for(recv.at[pl.ds(start, rows), :], r1.at[sem]))
                at = quad if sem else 0
                compute(start, quad, at)
                if sem:
                    result(at, half * other + slot, 1).start()
                else:
                    unless_local(lambda: result(at, half * c + slot, 0).start())
                    pl.when(local)(lambda: keep(at))
        else:
            unless_local(lambda: wait_for(recv.at[pl.ds(base, 2 * rows), :], r1.at[g]))
            compute(base, per, per * g)
            result(per * g + quad, half + slot, other).start()
            unless_local(lambda: result(per * g, slot, c).start())
            pl.when(local)(lambda: keep(per * g))

    pl.when(c == 0)(lambda: wait_for(ret.at[pl.ds(quad, quad * (2 * half - 1))], r2))
    pl.when(c == 1)(lambda: wait_for(ret, r2))
    for k in range(blocks):
        out_ref[k] = ret[slots[0, k]]
    wait_for(give, sent)
    wait_for(fbuf.at[pl.ds(elems, elems)], sent)

    def finish(skip):
        wait_for(recv.at[pl.ds(2 * rows * skip, 2 * rows * (half - skip)), :], sent)
        wait_for(ret.at[pl.ds(quad * skip, quad * (2 * half - skip))], sent)

    pl.when(c == 0)(lambda: finish(1))
    pl.when(c == 1)(lambda: finish(0))
    pl.when(first)(lambda: wait_for(via, sent))


def paired(sizes, old_fields, corner_shift, points, owners):
    half = sizes[0] * sizes[1] // 2
    elems, nvar, nodes = old_fields.shape
    blocks, _, pts = points.shape
    quad = sizes[2] * CAP
    rows = 4 * quad
    fields = old_fields.reshape(elems, nvar, nodes // 128, 128).transpose(0, 2, 1, 3)
    fields = fields.reshape(elems, nvar * nodes // 128, 128)
    vmem = pl.BlockSpec(memory_space=pltpu.VMEM)
    hbm = pl.BlockSpec(memory_space=pltpu.HBM)
    result = pltpu.VMEM((2 * half * quad, nvar, pts), F32)
    dma = pltpu.SemaphoreType.DMA
    return pl.pallas_call(
        functools.partial(pair_kernel, sizes),
        out_shape=jax.ShapeDtypeStruct((blocks, nvar, pts), F32),
        in_specs=[hbm] * 4,
        out_specs=vmem,
        scratch_shapes=[
            pltpu.VMEM((1, blocks), jnp.int32),
            pltpu.VMEM((blocks, 3, pts), F32),
            pltpu.VMEM((24, elems), F32),
            pltpu.VMEM((2 * elems, nvar * nodes // 128, 128), F32),
            pltpu.VMEM((2 * elems, 24, pts), F32),
            pltpu.VMEM((half + 2, 2 * rows, pts), F32),
            pltpu.VMEM((half + 2, rows, pts), F32),
            pltpu.VMEM((half // sizes[1], 2 * rows, pts), F32),
            pltpu.VMEM((2 * rows * half, pts), F32),
            pltpu.VMEM((3, 16 * quad, pts), F32),
            pltpu.VMEM((3, 16 * quad, pts), F32),
            result, result,
            pltpu.SMEM((1, blocks), jnp.int32),
            *[dma] * 5, dma((half + 1,)), dma,
            dma, pltpu.SemaphoreType.REGULAR,
        ],
        compiler_params=pltpu.CompilerParams(
            collective_id=0, has_side_effects=True, vmem_limit_bytes=24 * 1024 * 1024),
    )(*[pltpu.with_memory_space_constraint(x, pltpu.HBM) for x in (owners.reshape(1, blocks), points, corner_shift, fields)])


def shards(sizes, old_fields, corner_shift, targets, owners):
    n = sizes[0] * sizes[1] * sizes[2]
    elems, nvar, nodes = old_fields.shape
    blocks = owners.shape[0]
    pts = targets.shape[1] // blocks
    assert n & (n - 1) == 0 and elems & (elems - 1) == 0 and nvar == 4 and nodes == 512
    group_peers = min(GROUP_PEERS, n)
    groups = n // group_peers
    wide = (CAP * n + 127) // 128
    points = targets.reshape(3, blocks, pts).transpose(1, 0, 2)
    if sizes[0] == 4 and sizes[1] == 2 and sizes[2] == 2:
        out = paired(sizes, old_fields, corner_shift, points, owners)
        return out.transpose(1, 0, 2).reshape(nvar, blocks * pts)
    vmem = pl.BlockSpec(memory_space=pltpu.VMEM)
    hbm = pl.BlockSpec(memory_space=pltpu.HBM)
    message = pltpu.VMEM((8 * n, pts), F32)
    result = pltpu.VMEM((CAP * n, nvar, pts), F32)
    out = pl.pallas_call(
        functools.partial(kernel, sizes, group_peers),
        out_shape=jax.ShapeDtypeStruct((blocks, nvar, pts), F32),
        in_specs=[hbm] * 4,
        out_specs=vmem,
        scratch_shapes=[
            pltpu.VMEM((1, blocks), jnp.int32),
            pltpu.VMEM((blocks, 3, pts), F32),
            pltpu.VMEM((24, elems), F32),
            pltpu.VMEM((elems, nvar, nodes), F32),
            pltpu.VMEM((elems, 32, 128), BF16),
            message, message, result, result,
            pltpu.VMEM((3, 8 * CAP * group_peers, pts), F32),
            pltpu.VMEM((wide, 128), jnp.int32),
            pltpu.VMEM((wide * n, 128), jnp.int32),
            pltpu.SMEM((wide * n, 128), jnp.int32),
            pltpu.VMEM((1, pts), jnp.int32),
            pltpu.SMEM((1, pts), jnp.int32),
            *[pltpu.SemaphoreType.DMA] * 6,
            pltpu.SemaphoreType.DMA, pltpu.SemaphoreType.DMA((groups,)),
            pltpu.SemaphoreType.DMA, pltpu.SemaphoreType.DMA((groups,)),
            pltpu.SemaphoreType.DMA, pltpu.SemaphoreType.DMA((groups,)),
        ],
        compiler_params=pltpu.CompilerParams(
            collective_id=0, has_side_effects=True, vmem_limit_bytes=16 * 1024 * 1024),
    )(*[pltpu.with_memory_space_constraint(x, pltpu.HBM) for x in (owners.reshape(1, blocks), points, corner_shift, old_fields)])
    return out.transpose(1, 0, 2).reshape(nvar, blocks * pts)


def solution(mesh):
    sizes = tuple(mesh.shape[a] for a in AXES)
    in_specs = (
        P(("groups", "block", "seg", "sub"), None, None),
        P(None, ("groups", "block", "seg", "sub")),
        P(None, ("groups", "block", "seg", "sub")),
        P(("groups", "block", "seg", "sub")),
    )
    out_specs = P(None, ("groups", "block", "seg", "sub"))
    return jax.shard_map(functools.partial(shards, sizes), mesh=mesh, in_specs=in_specs,
                         out_specs=out_specs, check_vma=False)
```

```python
import functools

import jax
import jax.numpy as jnp
from jax import lax
from jax.experimental import pallas as pl
from jax.experimental.pallas import tpu as pltpu
from jax.sharding import PartitionSpec as P

NEWTON = 3
CAP = 2
GROUP_PEERS = 4
AXES = ("block", "seg", "sub")

GLL_POINTS = (
    -1.0,
    -0.8717401485096066,
    -0.5917001814331423,
    -0.2092992179024789,
    0.2092992179024789,
    0.5917001814331423,
    0.8717401485096066,
    1.0,
)
WEIGHTS = []
for _n in range(8):
    _w = 1.0
    for _m in range(8):
        if _m != _n:
            _w /= GLL_POINTS[_n] - GLL_POINTS[_m]
    WEIGHTS.append(_w)

F32 = jnp.float32
BF16 = jnp.bfloat16
EXACT = lax.Precision.HIGHEST
NT = (((1,), (1,)), ((), ()))


def iota(shape, dim):
    return lax.broadcasted_iota(jnp.int32, shape, dim)


def flip(index, static):
    bit = 1
    while bit <= static:
        if static & bit:
            index = index + bit * (1 - 2 * ((index // bit) % 2))
        bit *= 2
    return index


def newton(coef, y):
    def update(xi, jac, misfit):
        m = jac
        cof = [
            [m[1][1] * m[2][2] - m[1][2] * m[2][1], m[1][2] * m[2][0] - m[1][0] * m[2][2], m[1][0] * m[2][1] - m[1][1] * m[2][0]],
            [m[0][2] * m[2][1] - m[0][1] * m[2][2], m[0][0] * m[2][2] - m[0][2] * m[2][0], m[0][1] * m[2][0] - m[0][0] * m[2][1]],
            [m[0][1] * m[1][2] - m[0][2] * m[1][1], m[0][2] * m[1][0] - m[0][0] * m[1][2], m[0][0] * m[1][1] - m[0][1] * m[1][0]],
        ]
        inv = 1.0 / (m[0][0] * cof[0][0] + m[0][1] * cof[0][1] + m[0][2] * cof[0][2])
        out = []
        for b in range(3):
            step = (cof[0][b] * misfit[0] + cof[1][b] * misfit[1] + cof[2][b] * misfit[2]) * inv
            new = -step if xi is None else xi[b] - step
            out.append(jnp.clip(new, -1.2, 1.2))
        return out

    xi = update(None, [[c[4], c[2], c[1]] for c in coef], [c[0] - t for c, t in zip(coef, y)])
    for _ in range(NEWTON - 1):
        u, v, w = xi
        uv, uw, vw = u * v, u * w, v * w
        jac, misfit = [], []
        for c, t in zip(coef, y):
            du = c[4] + c[6] * v + c[5] * w + c[7] * vw
            dv = c[2] + c[6] * u + c[3] * w + c[7] * uw
            dw = c[1] + c[5] * u + c[3] * v + c[7] * uv
            jac.append([du, dv, dw])
            misfit.append((c[0] - t) + u * du + v * (c[2] + c[3] * w) + w * c[1])
        xi = update(xi, jac, misfit)
    return xi


def lagrange(x):
    diff = [x - t for t in GLL_POINTS]
    pre = [None, diff[0]]
    for n in range(2, 8):
        pre.append(pre[-1] * diff[n - 1])
    suf = [None] * 8
    suf[6] = diff[7]
    for n in range(5, -1, -1):
        suf[n] = suf[n + 1] * diff[n + 1]
    out = []
    for n in range(8):
        value = suf[n] if n == 0 else pre[n] if n == 7 else pre[n] * suf[n]
        out.append(value * WEIGHTS[n])
    return out


def kernel(sizes, group_peers, owners_hbm, targets_hbm, shift_hbm, fields_hbm, out_ref,
           owners_ref, targets_ref, shift_ref, fbuf, table, send, recv, res, ret, lag, idsend, idrecv, ids, slotv, slots,
           osem, tsem, csem, fsem, idsem, slotsem, s0, r0, s1, r1, s2, r2):
    nb, ns, nc = sizes
    n = nb * ns * nc
    blocks = owners_ref.shape[1]
    elems = shift_ref.shape[1]
    pts = out_ref.shape[2]
    groups = n // group_peers
    lanes = idsend.shape[1]
    wide = idsend.shape[0]
    here = [lax.axis_index(a) for a in AXES]
    me = (here[0] * ns + here[1]) * nc + here[2]

    def peer(k):
        if isinstance(k, int):
            return {
                "block": flip(here[0], k // (ns * nc)),
                "seg": flip(here[1], (k // nc) % ns),
                "sub": flip(here[2], k % nc),
            }
        other = jnp.bitwise_xor(me, k)
        return {"block": other // (ns * nc), "seg": (other // nc) % ns, "sub": other % nc}

    def message(k):
        return pl.ds(8 * k if isinstance(k, int) else pl.multiple_of(8 * k, 8), 3 * CAP)

    def for_wait(first, count, ref, sem):
        part = ref.at[pl.ds(8 * first, 3 * CAP * count), :]
        pltpu.make_async_copy(part, part, sem).wait()

    def send_result(k, g):
        part = pl.ds(CAP * k, CAP)
        return pltpu.make_async_remote_copy(
            src_ref=res.at[part], dst_ref=ret.at[part], send_sem=s2, recv_sem=r2.at[g],
            device_id=peer(k), device_id_type=pl.DeviceIdType.MESH)

    get_owners = pltpu.make_async_copy(owners_hbm, owners_ref, osem)
    get_owners.start()
    get_targets = pltpu.make_async_copy(targets_hbm, targets_ref, tsem)
    get_targets.start()
    get_shift = pltpu.make_async_copy(shift_hbm, shift_ref, csem)
    get_shift.start()
    fetch = pltpu.make_async_copy(fields_hbm, fbuf, fsem)
    fetch.start()
    barrier = pltpu.get_barrier_semaphore()
    unrolled = n <= 32

    def for_peers(first, last, body):
        if unrolled:
            for k in reversed(range(first, last)):
                body(k)
        else:
            lax.fori_loop(first, last, lambda k, c: (body(k), c)[1], 0)

    for_peers(1, n, lambda k: pl.semaphore_signal(
        barrier, inc=1, device_id=peer(k), device_id_type=pl.DeviceIdType.MESH))

    shift_bits = elems.bit_length() - 1
    get_owners.wait()
    own = owners_ref[...]
    owner_dev = jnp.right_shift(own, shift_bits)
    hit = (jnp.bitwise_xor(iota((n, blocks), 0), me) == owner_dev).astype(F32)
    earlier = (iota((blocks, blocks), 0) < iota((blocks, blocks), 1)).astype(F32)
    rank = jnp.dot(hit, earlier, preferred_element_type=F32)
    match = [jnp.where(rank == float(c), hit, 0.0) for c in range(CAP)]
    both = jnp.concatenate(match, axis=0)
    get_targets.wait()
    cat = jnp.concatenate([targets_ref[:, a, :] for a in range(3)], axis=1)
    packed = jnp.dot(both, cat, precision=EXACT, preferred_element_type=F32)
    for c in range(CAP):
        part = slice(c * n, (c + 1) * n)
        for a in range(3):
            send[pl.ds(3 * c + a, n, stride=8), :] = packed[part, a * pts:(a + 1) * pts]
            recv[3 * c + a:3 * c + a + 1, :] = packed[c * n:c * n + 1, a * pts:(a + 1) * pts]
    square = (blocks, blocks)
    diag = iota(square, 0) == iota(square, 1)
    own_rows = jnp.broadcast_to(own, square)
    own_col = jnp.sum(jnp.where(diag, own_rows, 0), axis=1, keepdims=True)
    dev_col = jnp.right_shift(own_col, shift_bits)
    dev_row = jnp.right_shift(own_rows, shift_bits)
    same = jnp.where(dev_col == dev_row, 1, 0)
    rank_row = jnp.sum(jnp.where(iota(square, 0) < iota(square, 1), same, 0), axis=0, keepdims=True)
    rank_col = jnp.sum(jnp.where(iota(square, 1) < iota(square, 0), same, 0), axis=1, keepdims=True)
    place = jnp.minimum(CAP * jnp.bitwise_xor(owner_dev, me) + rank_row, CAP * n - 1)
    place = jnp.concatenate([place, jnp.zeros((1, pts - blocks), jnp.int32)], axis=1)
    elem_col = own_col - dev_col * elems
    lane_of = jnp.where(rank_col < CAP, jnp.bitwise_xor(dev_col, me) + n * rank_col, -1)
    for r in range(wide):
        here_lane = iota((blocks, lanes), 1) + lanes * r == lane_of
        row = jnp.sum(jnp.where(here_lane, elem_col, 0), axis=0, keepdims=True)
        idsend[r:r + 1, :] = row
        idrecv[r:r + 1, :] = row
    slotv[...] = place
    slot_copy = pltpu.make_async_copy(slotv, slots, slotsem)
    slot_copy.start()

    pl.semaphore_wait(barrier, n - 1)
    def send_points(k):
        g = k // group_peers
        pltpu.make_async_remote_copy(
            src_ref=idsend, dst_ref=idrecv.at[pl.ds(wide * k, wide), :], send_sem=s0, recv_sem=r0.at[g],
            device_id=peer(k), device_id_type=pl.DeviceIdType.MESH).start()
        pltpu.make_async_remote_copy(
            src_ref=send.at[message(k), :], dst_ref=recv.at[message(k), :], send_sem=s1, recv_sem=r1.at[g],
            device_id=peer(k), device_id_type=pl.DeviceIdType.MESH).start()

    for_peers(1, n, send_points)

    row, col = iota((24, 24), 0), iota((24, 24), 1)
    both_bits = jnp.bitwise_and(row, col) % 8
    odd = (both_bits + both_bits // 2 + both_bits // 4) % 2
    hada = jnp.where(row // 8 == col // 8, (1 - 2 * odd).astype(F32) * 0.125, 0.0)
    get_shift.wait()
    bits = row % 8
    sign = (1 - 2 * ((bits + bits // 2 + bits // 4) % 2)).astype(F32)
    coefs = jnp.dot(hada * sign, shift_ref[...], precision=EXACT, preferred_element_type=F32)
    c_hi = coefs.astype(BF16)
    rest = coefs - c_hi.astype(F32)
    c_mid = rest.astype(BF16)
    c_lo = (rest - c_mid.astype(F32)).astype(BF16)

    fetch.wait()
    low_sub = iota((8, 128), 0) < 4
    low_lane = iota((8, 128), 1) < 64
    keep = low_sub == low_lane

    def split(e, carry):
        parts = []
        for q in range(4):
            x = fbuf[e, :, q * 128:(q + 1) * 128]
            x = jnp.concatenate([x, x], axis=0)
            hi = x.astype(BF16).astype(F32)
            lo = x - hi
            a = jnp.where(low_sub, hi, lo)
            b = pltpu.roll(jnp.where(low_sub, lo, hi), 64, axis=1)
            parts.append(jnp.where(keep, a, b))
        table[e] = jnp.concatenate(parts, axis=0).astype(BF16)
        return carry

    lax.fori_loop(0, elems, split, 0, unroll=4)

    per = group_peers
    count = CAP * per

    def run_group(g, first):
        base = g * per
        got = per - 1 if first else per
        start = base + 1 if first else base
        for_wait(start, got, recv, r1.at[g])

        def gather(a):
            return jnp.concatenate(
                [recv[pl.ds(8 * base + 3 * c + a, per, stride=8), :] for c in range(CAP)], axis=0)

        y = [gather(a) for a in range(3)]
        taken = idrecv.at[pl.ds(wide * start, wide * got), :]
        pltpu.make_async_copy(taken, taken, r0.at[g]).wait()
        id_copy = pltpu.make_async_copy(idrecv.at[pl.ds(wide * base, wide * per), :], ids.at[pl.ds(wide * base, wide * per), :], idsem)
        id_copy.start()
        id_lane = iota((per, lanes), 1) - iota((per, lanes), 0)
        id_cols = []
        for c in range(CAP):
            at = c * n + base
            id_rows = idrecv[pl.ds(wide * base + at // lanes, per, stride=wide), :]
            id_cols.append(jnp.sum(jnp.where(id_lane == at % lanes, id_rows, 0), axis=1, keepdims=True))
        elem = jnp.concatenate(id_cols, axis=0)
        pick = jnp.where(elem == iota((count, elems), 1), 1.0, 0.0).astype(BF16)
        chosen = sum(lax.dot_general(pick, c, NT, preferred_element_type=F32) for c in (c_hi, c_mid, c_lo))
        coef = []
        for a in range(3):
            line = []
            for m in range(8):
                value = chosen[:, 8 * a + m:8 * a + m + 1]
                if m == 4 >> a:
                    value = value + 1.0
                line.append(jnp.broadcast_to(value, (count, pts)))
            coef.append(line)
        xi = newton(coef, y)
        for a in range(3):
            for i, value in enumerate(lagrange(xi[a])):
                lag[a, pl.ds(i, count, stride=8), :] = value
        id_copy.wait()
        for s in range(count):
            c, p = s // per, s % per
            e = ids[wide * (base + p) + (c * n + base) // lanes, (c * n + base) % lanes + p]
            left = table[e]
            lz = lag[2, 8 * s:8 * s + 8, :]
            w = jnp.concatenate([lag[1, 8 * s + j:8 * s + j + 1, :] * lz for j in range(8)], axis=0)
            w_hi = w.astype(BF16)
            w_lo = (w - w_hi.astype(F32)).astype(BF16)
            prod = jnp.dot(
                jnp.concatenate([left, left], axis=1),
                jnp.concatenate([w_hi, w_hi, w_lo, w_lo], axis=0),
                preferred_element_type=F32)
            total = None
            for q in range(4):
                lx = jnp.where(low_sub, lag[0, 8 * s + 2 * q:8 * s + 2 * q + 1, :],
                               lag[0, 8 * s + 2 * q + 1:8 * s + 2 * q + 2, :])
                term = prod[8 * q:8 * q + 8] * lx
                total = term if total is None else total + term
            total = total[0:4] + total[4:8]
            if first and p == 0:
                ret[c] = total
            else:
                res[CAP * (base + p) + c] = total
        for_peers_in = range(1 if first else 0, per)
        for p in for_peers_in:
            send_result(base + p, g).start()

    run_group(0, True)
    if unrolled:
        for g in range(1, groups):
            run_group(g, False)
    else:
        lax.fori_loop(1, groups, lambda g, c: (run_group(g, False), c)[1], 0)

    slot_copy.wait()
    for g in range(groups):
        start, got = (1, per - 1) if g == 0 else (g * per, per)
        back = ret.at[pl.ds(CAP * start, CAP * got)]
        pltpu.make_async_copy(back, back, r2.at[g]).wait()
    for b in range(blocks):
        out_ref[b] = ret[slots[0, b]]
    rest_ids = idrecv.at[pl.ds(wide, wide * (n - 1)), :]
    pltpu.make_async_copy(rest_ids, rest_ids, s0).wait()
    for_wait(1, n - 1, send, s1)
    left = res.at[pl.ds(CAP, CAP * (n - 1))]
    pltpu.make_async_copy(left, left, s2).wait()


def pair_kernel(sizes, owners_hbm, targets_hbm, shift_hbm, fields_hbm, out_ref,
                owners_ref, targets_ref, shift_ref, fbuf, ctab, send, give, via, recv, cbuf, lag, res, ret, slots,
                csem, fsem, sent, r_rel, r_fld, r1, r2, r_via, here):
    nb, ns, nc = sizes
    half = nb * ns // 2
    blocks = owners_ref.shape[1]
    elems = shift_ref.shape[1]
    pts = out_ref.shape[2]
    quad = nc * CAP
    rows = 4 * quad
    per = 2 * quad
    b, s, c = [lax.axis_index(a) for a in AXES]
    chip = b * ns + s
    other = 1 - c
    top = nb // 2
    across = b + c * top * (1 - 2 * ((b // top) % 2))

    def peer(j, core):
        return {"block": flip(across, j // ns), "seg": flip(s, j % ns), "sub": core}

    def near(j, core):
        return {"block": flip(b, j // ns), "seg": flip(s, j % ns), "sub": core}

    def unless_here(j, body):
        if j == 0:
            pl.when(c == 1)(body)
        else:
            body()

    def remote(src, dst, send_sem, recv_sem, device):
        return pltpu.make_async_remote_copy(
            src_ref=src, dst_ref=dst, send_sem=send_sem, recv_sem=recv_sem,
            device_id=device, device_id_type=pl.DeviceIdType.MESH)

    def wait_for(part, sem):
        pltpu.make_async_copy(part, part, sem).wait()

    get_owners = pltpu.make_async_copy(owners_hbm, owners_ref, r2)
    get_owners.start()
    get_targets = pltpu.make_async_copy(targets_hbm, targets_ref, sent)
    get_targets.start()
    barrier = pltpu.get_barrier_semaphore()

    def hello(device):
        pl.semaphore_signal(barrier, inc=1, device_id=device, device_id_type=pl.DeviceIdType.MESH)

    sibling = {"block": b, "seg": s, "sub": other}
    partner = {"block": b, "seg": flip(s, 1), "sub": 1}
    first = jnp.logical_and(c == 1, b == 0)
    high = jnp.logical_and(c == 1, b >= top)

    def above(j):
        return b % 2 == 0 if j // ns else s == 0

    def below(j):
        return b % 2 == 1 if j // ns else s == 1

    @pl.when(c == 1)
    def _():
        @pl.when(b < top)
        def _():
            for j in reversed(range(half)):
                if j % ns:
                    pl.when(s == 0)(lambda: hello(peer(j, 1)))
                else:
                    hello(peer(j, 1))

        @pl.when(jnp.logical_and(b >= top, s == 0))
        def _():
            for j in reversed(range(1, half, ns)):
                pl.when(flip(across, j // ns) != 0)(lambda: hello(peer(j, 1)))

        pl.when(b == 0)(lambda: hello(partner))
        hello(sibling)

    @pl.when(c == 0)
    def _():
        for j in reversed(range(1, half)):
            pl.when(above(j))(lambda: hello(near(j, 0)))

    get_shift = pltpu.make_async_copy(shift_hbm, shift_ref, csem)
    get_shift.start()
    fetch = pltpu.make_async_copy(fields_hbm, fbuf.at[pl.ds(0, elems)], fsem)
    fetch.start()

    pl.when(c == 0)(lambda: pl.semaphore_wait(barrier, 1 + (b % 2) * ns + s))
    pl.when(high)(lambda: pl.semaphore_wait(barrier, half // ns * (1 + s)))

    def answer(device):
        pl.semaphore_signal(here, inc=1, device_id=device, device_id_type=pl.DeviceIdType.MESH)

    @pl.when(high)
    def _():
        for j in reversed(range(half)):
            if j % ns:
                pl.when(jnp.logical_and(flip(across, j // ns) != 0, s == 1))(lambda: answer(peer(j, 1)))
            else:
                answer(peer(j, 1))

    @pl.when(c == 0)
    def _():
        for j in reversed(range(1, half)):
            pl.when(below(j))(lambda: answer(near(j, 0)))

    shift_bits = elems.bit_length() - 1
    square = (blocks, blocks)
    get_owners.wait()
    own = owners_ref[...]
    own_rows = jnp.broadcast_to(own, square)
    diag = iota(square, 0) == iota(square, 1)
    own_col = jnp.sum(jnp.where(diag, own_rows, 0), axis=1, keepdims=True)
    dev_col = jnp.right_shift(own_col, shift_bits)
    dev_row = jnp.right_shift(own_rows, shift_bits)
    same = jnp.where(dev_col == dev_row, 1, 0)
    rank_row = jnp.sum(jnp.where(iota(square, 0) < iota(square, 1), same, 0), axis=0, keepdims=True)
    rank_col = jnp.sum(jnp.where(iota(square, 1) < iota(square, 0), same, 0), axis=1, keepdims=True)
    base_chip = jnp.bitwise_xor(chip, c * half)

    def slot_of(dev, rank):
        rel = jnp.bitwise_xor(jnp.right_shift(dev, 1), base_chip)
        return rel, (rel * nc + jnp.bitwise_and(dev, 1)) * CAP + rank

    rel_col, slot_col = slot_of(dev_col, rank_col)
    turned = jnp.where(rel_col >= half, 1, 0)
    side = jnp.bitwise_xor(jnp.bitwise_xor(jnp.bitwise_and(dev_col, 1), c), turned)
    elem_col = own_col - dev_col * elems + elems * side
    _, slot_row = slot_of(jnp.right_shift(own, shift_bits), rank_row)
    count = 2 * half * quad
    pick = jnp.where(iota((count, blocks), 0) == slot_row, 1.0, 0.0)
    id_rows = jnp.broadcast_to(elem_col.astype(F32), (blocks, pts))
    get_targets.wait()
    cat = jnp.concatenate([targets_ref[:, a, :] for a in range(3)] + [id_rows], axis=1)
    packed = jnp.dot(pick, cat, precision=EXACT, preferred_element_type=F32)
    for a in range(4):
        for j in range(half):
            send[j, pl.ds(a, quad, stride=4), :] = packed[quad * j:quad * (j + 1), a * pts:(a + 1) * pts]
            give[j, pl.ds(a, quad, stride=4), :] = packed[quad * (half + j):quad * (half + j + 1), a * pts:(a + 1) * pts]
    slot_safe = jnp.minimum(jnp.maximum(slot_col, 0), count - 1)
    for k in range(blocks):
        slots[0, k] = slot_safe[k, 0]

    low_sub = iota((8, 128), 0) < 4
    low_lane = iota((8, 128), 1) < 64

    def split(e):
        high_part, low_part = [], []
        for r in range(0, fbuf.shape[1], 8):
            x = fbuf[e, r:r + 8, :]
            turned = pltpu.roll(x, 64, axis=1)
            for part in (jnp.where(low_lane, x, turned), jnp.where(low_lane, turned, x)):
                hi = part.astype(BF16).astype(F32)
                high_part.append(hi)
                low_part.append(part - hi)
        return jnp.concatenate(high_part + low_part, axis=0).astype(BF16)

    row, col = iota((24, 24), 0), iota((24, 24), 1)
    both_bits = jnp.bitwise_and(row, col) % 8
    odd = (both_bits + both_bits // 2 + both_bits // 4) % 2
    hada = jnp.where(row // 8 == col // 8, (1 - 2 * odd).astype(F32) * 0.125, 0.0)
    bits = row % 8
    sign = (1 - 2 * ((bits + bits // 2 + bits // 4) % 2)).astype(F32)
    line = iota((24, elems), 0)
    unit = jnp.where(line % 8 == jnp.right_shift(4, line // 8), 1.0, 0.0)

    def spread(side, shift):
        coefs = jnp.dot(hada * sign, shift, precision=EXACT, preferred_element_type=F32) + unit
        for e in range(elems):
            ctab[side * elems + e] = jnp.broadcast_to(coefs[:, e:e + 1], (24, pts))

    get_shift.wait()
    give[half, :, :elems] = shift_ref[:rows]
    give[half + 1, :24 - rows, :elems] = shift_ref[rows:]
    fetch.wait()
    pl.when(first)(lambda: pl.semaphore_wait(barrier, 1))

    @pl.when(jnp.logical_and(c == 1, jnp.logical_and(jnp.logical_and(b > 0, b < top), s == 1)))
    def _():
        pl.semaphore_wait(barrier, half // ns)
        for j in reversed(range(1, half, ns)):
            answer(peer(j, 1))

    theirs = send.at[:, pl.ds(rows, rows), :]

    def heard(count):
        pl.semaphore_wait(here, count)

    def share():
        remote(fbuf.at[pl.ds(0, elems)], fbuf.at[pl.ds(elems, elems)], sent, r_fld, sibling).start()

    corner = (b % 2) * ns + s

    def request(src, group, device):
        at = pl.multiple_of(2 * rows * group, 2 * rows)
        remote(src, recv.at[pl.ds(at, 2 * rows), :], sent, r1.at[group], device).start()

    def parted(src, device, core):
        for part, sem in ((core, 0), (1 - core, half)):
            piece = pl.ds(rows * part, rows)
            remote(src.at[piece, :], recv.at[piece, :], sent, r1.at[sem], device).start()

    def mine(src, device, core):
        pl.when(corner == 0)(lambda: parted(src, device, core))
        pl.when(corner > 0)(lambda: request(src, corner, device))

    @pl.when(c == 0)
    def _():
        remote(give, theirs, sent, r_rel, sibling).start()
        share()
        wait_for(theirs, r_rel)
        pl.when(corner < half - 1)(lambda: heard(half - 1 - corner))
        for j in reversed(range(1, half)):
            mine(send.at[j], near(j, 0), 0)
        recv[pl.ds(pl.multiple_of(2 * rows * corner, 2 * rows), 2 * rows), :] = send[0]

    @pl.when(c == 1)
    def _():
        wait_for(theirs, r_rel)

        @pl.when(b == 0)
        def _():
            for j in reversed(range(1, half, ns)):
                remote(send.at[j], via.at[j // ns], sent, r_via, partner).start()

        remote(give, theirs, sent, r_rel, sibling).start()

        columns = list(reversed(range(half // ns)))

        @pl.when(jnp.logical_and(b == 0, s == 0))
        def _():
            heard(half // ns)
            for i in columns:
                parted(send.at[ns * i], peer(ns * i, 1), 1)
            for i in columns:
                answer(peer(ns * i, 1))
            share()
            wait_for(via, r_via)
            for i in columns:
                request(via.at[i], 1, peer(ns * i, 1))

        @pl.when(jnp.logical_and(b == 0, s == 1))
        def _():
            wait_for(via, r_via)
            heard(half // ns)
            for i in columns:
                parted(via.at[i], peer(ns * i, 1), 1)
            for i in columns:
                request(send.at[ns * i], 1, peer(ns * i, 1))
            share()

        @pl.when(b > 0)
        def _():
            pl.when(b < top)(lambda: heard(half // ns * (2 - s)))
            pl.when(jnp.logical_and(b >= top, s == 0))(lambda: heard(ns))
            for j in reversed(range(half)):
                mine(send.at[j], peer(j, 1), 1)
            share()

    spread(0, shift_ref[...])
    spread(1, jnp.concatenate([send[half, rows:2 * rows, :elems], send[half + 1, rows:2 * rows, :elems]], axis=0)[:24])
    wait_for(fbuf.at[pl.ds(elems, elems)], r_fld)

    def compute(base, count, at):
        y = [recv[pl.ds(base + a, count, stride=4), :] for a in range(3)]
        ids = recv[pl.ds(base + 3, count, stride=4), :].astype(jnp.int32)
        ids = jnp.minimum(jnp.maximum(ids, 0), 2 * elems - 1)
        elem = [ids[k, 0] for k in range(count)]
        for k in range(count):
            for a in range(3):
                cbuf[a, 8 * k:8 * k + 8, :] = ctab[elem[k], 8 * a:8 * a + 8, :]
        coef = [[cbuf[a, pl.ds(m, count, stride=8), :] for m in range(8)] for a in range(3)]
        xi = newton(coef, y)
        for a in range(3):
            for i, value in enumerate(lagrange(xi[a])):
                lag[a, per * i:per * i + count, :] = value
        for k in range(count):
            left = split(elem[k])
            lz = lag[2, pl.ds(k, 8, stride=per), :]
            w = jnp.concatenate([lag[1, per * i + k:per * i + k + 1, :] * lz for i in range(8)], axis=0)
            w_hi = w.astype(BF16)
            w_lo = (w - w_hi.astype(F32)).astype(BF16)
            prod = jnp.dot(left, jnp.concatenate([w_hi, w_lo], axis=0), preferred_element_type=F32)
            prod = prod[:32] + prod[32:]
            total = None
            for q in range(4):
                i = per * (4 * (q // 2) + q % 2) + k
                lx = jnp.where(low_sub, lag[0, i:i + 1, :], lag[0, i + 2 * per:i + 2 * per + 1, :])
                term = prod[8 * q:8 * q + 8] * lx
                total = term if total is None else total + term
            res[at + k] = total[0:4] + total[4:8]

    for g in range(half):
        base = 2 * rows * g
        z, x = g // ns, g % ns
        local = jnp.logical_and(c == 0, corner == g)

        def unless_local(body):
            pl.when(jnp.logical_not(local))(body)

        slot = ns * flip(b % 2, z) + flip(s, x)

        def result(at, to, core):
            return remote(res.at[pl.ds(at, quad)], ret.at[pl.ds(quad * to, quad)],
                          sent, r2, {"block": 2 * (across // 2) + z, "seg": x, "sub": core})

        def keep(at):
            ret[0:quad] = res[at:at + quad]

        if g == 0:
            for part, sem in ((c, 0), (other, half)):
                start = pl.multiple_of(rows * part, rows)
                unless_local(lambda: wait_for(recv.at[pl.ds(start, rows), :], r1.at[sem]))
                at = quad if sem else 0
                compute(start, quad, at)
                if sem:
                    result(at, half * other + slot, 1).start()
                else:
                    unless_local(lambda: result(at, half * c + slot, 0).start())
                    pl.when(local)(lambda: keep(at))
        else:
            unless_local(lambda: wait_for(recv.at[pl.ds(base, 2 * rows), :], r1.at[g]))
            compute(base, per, per * g)
            result(per * g + quad, half + slot, other).start()
            unless_local(lambda: result(per * g, slot, c).start())
            pl.when(local)(lambda: keep(per * g))

    pl.when(c == 0)(lambda: wait_for(ret.at[pl.ds(quad, quad * (2 * half - 1))], r2))
    pl.when(c == 1)(lambda: wait_for(ret, r2))
    for k in range(blocks):
        out_ref[k] = ret[slots[0, k]]
    wait_for(give, sent)
    wait_for(fbuf.at[pl.ds(elems, elems)], sent)

    def finish(skip):
        wait_for(recv.at[pl.ds(2 * rows * skip, 2 * rows * (half - skip)), :], sent)
        wait_for(ret.at[pl.ds(quad * skip, quad * (2 * half - skip))], sent)

    pl.when(c == 0)(lambda: finish(1))
    pl.when(c == 1)(lambda: finish(0))
    pl.when(first)(lambda: wait_for(via, sent))


def paired(sizes, old_fields, corner_shift, points, owners):
    half = sizes[0] * sizes[1] // 2
    elems, nvar, nodes = old_fields.shape
    blocks, _, pts = points.shape
    quad = sizes[2] * CAP
    rows = 4 * quad
    fields = old_fields.reshape(elems, nvar, nodes // 128, 128).transpose(0, 2, 1, 3)
    fields = fields.reshape(elems, nvar * nodes // 128, 128)
    vmem = pl.BlockSpec(memory_space=pltpu.VMEM)
    hbm = pl.BlockSpec(memory_space=pltpu.HBM)
    result = pltpu.VMEM((2 * half * quad, nvar, pts), F32)
    dma = pltpu.SemaphoreType.DMA
    return pl.pallas_call(
        functools.partial(pair_kernel, sizes),
        out_shape=jax.ShapeDtypeStruct((blocks, nvar, pts), F32),
        in_specs=[hbm] * 4,
        out_specs=vmem,
        scratch_shapes=[
            pltpu.VMEM((1, blocks), jnp.int32),
            pltpu.VMEM((blocks, 3, pts), F32),
            pltpu.VMEM((24, elems), F32),
            pltpu.VMEM((2 * elems, nvar * nodes // 128, 128), F32),
            pltpu.VMEM((2 * elems, 24, pts), F32),
            pltpu.VMEM((half + 2, 2 * rows, pts), F32),
            pltpu.VMEM((half + 2, rows, pts), F32),
            pltpu.VMEM((half // sizes[1], 2 * rows, pts), F32),
            pltpu.VMEM((2 * rows * half, pts), F32),
            pltpu.VMEM((3, 16 * quad, pts), F32),
            pltpu.VMEM((3, 16 * quad, pts), F32),
            result, result,
            pltpu.SMEM((1, blocks), jnp.int32),
            *[dma] * 5, dma((half + 1,)), dma,
            dma, pltpu.SemaphoreType.REGULAR,
        ],
        compiler_params=pltpu.CompilerParams(
            collective_id=0, has_side_effects=True, vmem_limit_bytes=24 * 1024 * 1024),
    )(*[pltpu.with_memory_space_constraint(x, pltpu.HBM) for x in (owners.reshape(1, blocks), points, corner_shift, fields)])


def shards(sizes, old_fields, corner_shift, targets, owners):
    n = sizes[0] * sizes[1] * sizes[2]
    elems, nvar, nodes = old_fields.shape
    blocks = owners.shape[0]
    pts = targets.shape[1] // blocks
    assert n & (n - 1) == 0 and elems & (elems - 1) == 0 and nvar == 4 and nodes == 512
    group_peers = min(GROUP_PEERS, n)
    groups = n // group_peers
    wide = (CAP * n + 127) // 128
    points = targets.reshape(3, blocks, pts).transpose(1, 0, 2)
    if sizes[0] == 4 and sizes[1] == 2 and sizes[2] == 2:
        out = paired(sizes, old_fields, corner_shift, points, owners)
        return out.transpose(1, 0, 2).reshape(nvar, blocks * pts)
    vmem = pl.BlockSpec(memory_space=pltpu.VMEM)
    hbm = pl.BlockSpec(memory_space=pltpu.HBM)
    message = pltpu.VMEM((8 * n, pts), F32)
    result = pltpu.VMEM((CAP * n, nvar, pts), F32)
    out = pl.pallas_call(
        functools.partial(kernel, sizes, group_peers),
        out_shape=jax.ShapeDtypeStruct((blocks, nvar, pts), F32),
        in_specs=[hbm] * 4,
        out_specs=vmem,
        scratch_shapes=[
            pltpu.VMEM((1, blocks), jnp.int32),
            pltpu.VMEM((blocks, 3, pts), F32),
            pltpu.VMEM((24, elems), F32),
            pltpu.VMEM((elems, nvar, nodes), F32),
            pltpu.VMEM((elems, 32, 128), BF16),
            message, message, result, result,
            pltpu.VMEM((3, 8 * CAP * group_peers, pts), F32),
            pltpu.VMEM((wide, 128), jnp.int32),
            pltpu.VMEM((wide * n, 128), jnp.int32),
            pltpu.SMEM((wide * n, 128), jnp.int32),
            pltpu.VMEM((1, pts), jnp.int32),
            pltpu.SMEM((1, pts), jnp.int32),
            *[pltpu.SemaphoreType.DMA] * 6,
            pltpu.SemaphoreType.DMA, pltpu.SemaphoreType.DMA((groups,)),
            pltpu.SemaphoreType.DMA, pltpu.SemaphoreType.DMA((groups,)),
            pltpu.SemaphoreType.DMA, pltpu.SemaphoreType.DMA((groups,)),
        ],
        compiler_params=pltpu.CompilerParams(
            collective_id=0, has_side_effects=True, vmem_limit_bytes=16 * 1024 * 1024),
    )(*[pltpu.with_memory_space_constraint(x, pltpu.HBM) for x in (owners.reshape(1, blocks), points, corner_shift, old_fields)])
    return out.transpose(1, 0, 2).reshape(nvar, blocks * pts)


def solution(mesh):
    sizes = tuple(mesh.shape[a] for a in AXES)
    in_specs = (
        P(("groups", "block", "seg", "sub"), None, None),
        P(None, ("groups", "block", "seg", "sub")),
        P(None, ("groups", "block", "seg", "sub")),
        P(("groups", "block", "seg", "sub")),
    )
    out_specs = P(None, ("groups", "block", "seg", "sub"))
    return jax.shard_map(functools.partial(shards, sizes), mesh=mesh, in_specs=in_specs,
                         out_specs=out_specs, check_vma=False)
```
